8 devices in a mesh: dp: 2 (over z, y), ep: 4 (over x, core).
Axes of the slice: x: 2, y: 2, z: 1, core: 2. Of those that a mesh axis runs over, the one named last changes fastest.
Arguments:
- tokens: bfloat16 [2048, 1024], P(('dp', 'ep'))
- w_router: bfloat16 [1024, 32], replicated
- w_gate: bfloat16 [32, 1024, 512], P('ep')
- w_up: bfloat16 [32, 1024, 512], P('ep')
- w_down: bfloat16 [32, 512, 1024], P('ep')
- top_ids: int32 [2048, 8], P(('dp', 'ep'))
- r_proj: bfloat16 [2048, 1024], P(('dp', 'ep'))
Outputs:
- output 1: float32 [2048, 1024], P(('dp', 'ep'))
- output 2: float32 [2048, 1024], P(('dp', 'ep'))
- output 3: float32 [32, 1024, 512], P('ep')
- output 4: float32 [32, 1024, 512], P('ep')
- output 5: float32 [32, 512, 1024], P('ep')
- output 6: float32 [1024, 32], replicated
All inputs are finite; a program needn't handle non-finite values.
Results may differ from the reference program's by a relative error of at most 0.00173.
Values are sent between devices in bfloat16 or wider.
A program may use at most 1 GiB of HBM per device.

```python
import jax
import jax.numpy as jnp
from jax import lax

D = 1024
FF = 512
EXPERTS = 32
TOP = 8
N_TOK = 2048
BLK = 64
ASSIGN = N_TOK * TOP
NBLK = (ASSIGN + BLK - 1) // BLK + EXPERTS
ROWS = NBLK * BLK


def draw_routing(rng_key):
    key_rank, key_noise = jax.random.split(rng_key)
    expert_rank = jax.random.permutation(key_rank, EXPERTS)
    popular = 2000 // (expert_rank + 2)
    rand_noise = jax.random.randint(key_noise, (N_TOK, EXPERTS), 0, 1000)
    int_score = (popular[None, :] + rand_noise) * EXPERTS + jnp.arange(EXPERTS)[None, :]
    return lax.top_k(int_score, TOP)[1].astype(jnp.int32)


def setup_inputs(seed: int = 0) -> dict:
    key_list = jax.random.split(jax.random.key(seed), 7)
    tokens = jax.random.normal(key_list[0], (N_TOK, D), jnp.float32).astype(jnp.bfloat16)
    w_router = (jax.random.normal(key_list[1], (D, EXPERTS), jnp.float32) * D ** -0.5).astype(jnp.bfloat16)
    w_gate = (jax.random.normal(key_list[2], (EXPERTS, D, FF), jnp.float32) * D ** -0.5).astype(jnp.bfloat16)
    w_up = (jax.random.normal(key_list[3], (EXPERTS, D, FF), jnp.float32) * D ** -0.5).astype(jnp.bfloat16)
    w_down = (jax.random.normal(key_list[4], (EXPERTS, FF, D), jnp.float32) * FF ** -0.5).astype(jnp.bfloat16)
    top_ids = draw_routing(key_list[5])
    r_proj = jax.random.normal(key_list[6], (N_TOK, D), jnp.float32).astype(jnp.bfloat16)
    return {'tokens': tokens, 'w_router': w_router, 'w_gate': w_gate, 'w_up': w_up, 'w_down': w_down, 'top_ids': top_ids, 'r_proj': r_proj}


def reference(tokens, w_router, w_gate, w_up, w_down, top_ids, r_proj):
    logits = jnp.dot(tokens, w_router, preferred_element_type=jnp.float32)
    gate_prob = jax.nn.softmax(jnp.take_along_axis(logits, top_ids, axis=1), axis=-1)
    exp_flat = top_ids.reshape(-1)
    sort_idx = jnp.argsort(exp_flat, stable=True).astype(jnp.int32)
    sorted_exp = exp_flat[sort_idx]
    exp_count = jnp.bincount(exp_flat, length=EXPERTS).astype(jnp.int32)
    pad_count = (exp_count + BLK - 1) // BLK * BLK
    pad_end = jnp.cumsum(pad_count)
    pad_start = pad_end - pad_count
    cnt_start = jnp.cumsum(exp_count) - exp_count
    row_pos = pad_start[sorted_exp] + jnp.arange(ASSIGN, dtype=jnp.int32) - cnt_start[sorted_exp]
    slot_asg = jnp.full((ROWS,), ASSIGN, jnp.int32).at[row_pos].set(sort_idx)
    pos_asg = jnp.zeros((ASSIGN,), jnp.int32).at[sort_idx].set(row_pos)
    blk_start = jnp.arange(NBLK, dtype=jnp.int32) * BLK
    blk_exp = jnp.minimum(jnp.sum((pad_end[None, :] <= blk_start[:, None]).astype(jnp.int32), axis=1), EXPERTS - 1)
    row_valid = (slot_asg < ASSIGN)[:, None]
    safe_asg = jnp.minimum(slot_asg, ASSIGN - 1)
    tok_rows = jnp.where(row_valid, tokens[safe_asg // TOP], 0).reshape(NBLK, BLK, D)
    contract_rows = (((0,), (0,)), ((), ()))
    contract_cols = (((1,), (1,)), ((), ()))

    def fwd_block(blk_args):
        x_blk, expert = blk_args
        h_gate = jnp.dot(x_blk, w_gate[expert], preferred_element_type=jnp.float32)
        h_up = jnp.dot(x_blk, w_up[expert], preferred_element_type=jnp.float32)
        act_rows = (jax.nn.silu(h_gate) * h_up).astype(jnp.bfloat16)
        return jnp.dot(act_rows, w_down[expert], preferred_element_type=jnp.float32).astype(jnp.bfloat16)

    out_pad = lax.map(fwd_block, (tok_rows, blk_exp)).reshape(ROWS, D)
    out_asg = out_pad[pos_asg].reshape(N_TOK, TOP, D).astype(jnp.float32)
    y_out = tokens.astype(jnp.float32) + jnp.einsum('tkh,tk->th', out_asg, gate_prob)

    d_y = r_proj.astype(jnp.float32)
    d_gates = jnp.einsum('tkh,th->tk', out_asg, d_y)
    d_sel = gate_prob * (d_gates - jnp.sum(gate_prob * d_gates, axis=-1, keepdims=True))
    onehot = (top_ids[:, :, None] == jnp.arange(EXPERTS)[None, None, :]).astype(jnp.float32)
    d_logit = jnp.einsum('tk,tke->te', d_sel, onehot).astype(jnp.bfloat16)
    grad_router = lax.dot_general(tokens, d_logit, contract_rows, preferred_element_type=jnp.float32)
    dx_router = lax.dot_general(d_logit, w_router, contract_cols, preferred_element_type=jnp.float32)
    d_out = (gate_prob[:, :, None] * d_y[:, None, :]).astype(jnp.bfloat16).reshape(ASSIGN, D)
    d_pad = jnp.where(row_valid, d_out[safe_asg], 0).reshape(NBLK, BLK, D)

    def bwd_block(grad_acc, blk_args):
        g_gate, g_up, g_down = grad_acc
        x_blk, d_blk, expert = blk_args
        h_gate = jnp.dot(x_blk, w_gate[expert], preferred_element_type=jnp.float32)
        h_up = jnp.dot(x_blk, w_up[expert], preferred_element_type=jnp.float32)
        sig_gate = jax.nn.sigmoid(h_gate)
        silu_gate = h_gate * sig_gate
        act_rows = (silu_gate * h_up).astype(jnp.bfloat16)
        d_act = lax.dot_general(d_blk, w_down[expert], contract_cols, preferred_element_type=jnp.float32)
        d_hgate = (d_act * h_up * sig_gate * (1.0 + h_gate * (1.0 - sig_gate))).astype(jnp.bfloat16)
        d_hup = (d_act * silu_gate).astype(jnp.bfloat16)
        g_gate = g_gate.at[expert].add(lax.dot_general(x_blk, d_hgate, contract_rows, preferred_element_type=jnp.float32))
        g_up = g_up.at[expert].add(lax.dot_general(x_blk, d_hup, contract_rows, preferred_element_type=jnp.float32))
        g_down = g_down.at[expert].add(lax.dot_general(act_rows, d_blk, contract_rows, preferred_element_type=jnp.float32))
        d_rows = lax.dot_general(d_hgate, w_gate[expert], contract_cols, preferred_element_type=jnp.float32) + lax.dot_general(d_hup, w_up[expert], contract_cols, preferred_element_type=jnp.float32)
        return (g_gate, g_up, g_down), d_rows.astype(jnp.bfloat16)

    zero_in = jnp.zeros((EXPERTS, D, FF), jnp.float32)
    zero_out = jnp.zeros((EXPERTS, FF, D), jnp.float32)
    grads, d_rows = lax.scan(bwd_block, (zero_in, zero_in, zero_out), (tok_rows, d_pad, blk_exp))
    d_expert = jnp.sum(d_rows.reshape(ROWS, D)[pos_asg].reshape(N_TOK, TOP, D).astype(jnp.float32), axis=1)
    grad_tokens = d_y + dx_router + d_expert
    return y_out, grad_tokens, grads[0], grads[1], grads[2], grad_router
```

```python
import functools

import jax
import jax.numpy as jnp
from jax import lax
from jax.experimental import pallas as pl
from jax.experimental.pallas import tpu as pltpu
from jax.sharding import PartitionSpec as P

F32 = jnp.float32
BF16 = jnp.bfloat16
MESH = pl.DeviceIdType.MESH
VMEM_MAX = 63 * 1024 * 1024
T = 256
NB = 256
HALF = 1024
D = 1024
FF = 512
NE = 8
S = 8
L = 128
Q = 4
RB = 1032
R1 = 8256
R2 = 16448


def dot(a, b, ca=1, cb=0):
    return lax.dot_general(a, b, (((ca,), (cb,)), ((), ())), preferred_element_type=F32)


def vspec():
    return pl.BlockSpec(memory_space=pltpu.VMEM)


def aspec():
    return pl.BlockSpec(memory_space=pl.ANY)


def sspec():
    return pl.BlockSpec(memory_space=pltpu.SMEM)


def barrier_all(dp, ep):
    bar = pltpu.get_barrier_semaphore()
    for k in range(1, S):
        pl.semaphore_signal(bar, inc=1, device_id=((dp + k // Q) % 2, (ep + k % Q) % Q), device_id_type=MESH)
    pl.semaphore_wait(bar, 7)


def gather_kernel(x_ref, r_ref, ids_ref, wr_ref,
                  xon, xof, ron, rof, xqn, rqn, gt_out, idx_out, gat_out, cnt_out,
                  gt_s, pos_s, v_s, ssem, rsem, lsem, gsend, grecv):
    dp = lax.axis_index('dp')
    ep = lax.axis_index('ep')
    c = ep % 2
    xc = ep // 2
    me = dp * Q + ep
    mate = (dp, xc * 2 + 1 - c)
    xnb = (dp, (1 - xc) * 2 + c)
    ynb = (1 - dp, ep)
    barrier_all(dp, ep)

    def rcopy(src, dst, k, dev):
        return pltpu.make_async_remote_copy(src_ref=src, dst_ref=dst, send_sem=ssem.at[k], recv_sem=rsem.at[k], device_id=dev, device_id_type=MESH)

    direct = [
        rcopy(x_ref, xof.at[c], 0, xnb), rcopy(x_ref, xqn.at[c], 1, ynb),
        rcopy(r_ref, rof.at[c], 2, xnb), rcopy(r_ref, rqn.at[c], 3, ynb),
        rcopy(x_ref, xon.at[c], Q, mate), rcopy(r_ref, ron.at[c], 5, mate)]
    for cp in direct:
        cp.start()
    local = [pltpu.make_async_copy(x_ref, xon.at[c], lsem.at[0]), pltpu.make_async_copy(r_ref, ron.at[c], lsem.at[1])]
    for cp in local:
        cp.start()

    zt = dot(wr_ref[...], x_ref[...], 1, 1)
    eio = lax.broadcasted_iota(jnp.int32, (32, NB), 0)
    sel = eio == ids_ref[0:1, :]
    for j in range(1, S):
        sel = sel | (eio == ids_ref[j:j + 1, :])
    zm = jnp.max(jnp.where(sel, zt, -jnp.inf), axis=0, keepdims=True)
    pe = jnp.where(sel, jnp.exp(zt - zm), 0.0)
    gt_s[me] = jnp.where(sel, pe / jnp.sum(pe, axis=0, keepdims=True), -1.0)
    gcopies = []
    for k in range(1, S):
        dev = ((dp + k // Q) % 2, (ep + k % Q) % Q)
        cp = pltpu.make_async_remote_copy(src_ref=gt_s.at[me], dst_ref=gt_s.at[me], send_sem=gsend.at[k - 1], recv_sem=grecv.at[k - 1], device_id=dev, device_id_type=MESH)
        cp.start()
        gcopies.append(cp)
    for cp in gcopies:
        cp.wait()

    tri = (lax.broadcasted_iota(jnp.int32, (NB, NB), 0) < lax.broadcasted_iota(jnp.int32, (NB, NB), 1)).astype(BF16)
    srow = lax.broadcasted_iota(jnp.int32, (S, NB), 0)
    tlan = lax.broadcasted_iota(jnp.int32, (S, NB), 1).astype(F32)
    for half in range(2):
        base = jnp.zeros((S, 1), F32)
        for k in range(Q):
            hd = dp if half == 0 else 1 - dp
            xx = xc if k < 2 else 1 - xc
            g = gt_s[hd * Q + xx * 2 + k % 2, pl.ds(pl.multiple_of(ep * S, S), S), :]
            m = g >= 0.0
            mf = m.astype(F32)
            pos = dot(mf.astype(BF16), tri) + base
            pos_s[half * Q + k] = jnp.where(m, pos, -1.0)
            base = base + jnp.sum(mf, axis=1, keepdims=True)
            g = jnp.where(m, g, 0.0)
            g1 = g.astype(BF16)
            e1 = g - g1.astype(F32)
            g2 = e1.astype(BF16)
            g3 = (e1 - g2.astype(F32)).astype(BF16)
            head = jnp.where(srow == 0, tlan, jnp.where(srow == 1, float(k), 0.0))
            v_s[half * Q + k] = jnp.concatenate([head, g1.astype(F32), g2.astype(F32), g3.astype(F32)], axis=0).astype(BF16)
        cnt_out[half] = jnp.broadcast_to(base, (S, L)).astype(jnp.int32)

    pio = lax.broadcasted_iota(jnp.int32, (NB, NB), 0).astype(F32)
    rio = lax.broadcasted_iota(jnp.int32, (32, NB), 0)
    lio = lax.broadcasted_iota(jnp.int32, (1, NB), 1)

    def list_body(he, carry):
        half = he // S
        e = he % S
        cnt_e = cnt_out[half, pl.ds(e, 1), 0:1]
        for pt in range(Q):
            acc = jnp.zeros((32, NB), F32)
            for k in range(pt, Q):
                prow = pos_s[half * Q + k, pl.ds(e, 1), :] - float(256 * pt)
                oh = (pio == prow).astype(F32).astype(BF16)
                acc = acc + dot(v_s[half * Q + k], oh, 1, 1)
            ids = (acc[0:1, :] + 256.0 * acc[1:2, :]).astype(jnp.int32)
            ids = jnp.where(lio + 256 * pt < cnt_e, ids, HALF)
            gv = jnp.sum(jnp.where((rio >= S) & (rio % S == e), acc, 0.0), axis=0, keepdims=True)
            for q in range(2):
                idx_out[he, 2 * pt + q:2 * pt + q + 1, :] = ids[:, L * q:L * (q + 1)]
                gat_out[he, 2 * pt + q:2 * pt + q + 1, :] = gv[:, L * q:L * (q + 1)]
        return carry

    lax.fori_loop(0, 16, list_body, 0)
    gt_out[...] = gt_s[...]

    fwd = [
        rcopy(xof.at[c], xof.at[c], 6, mate), rcopy(xqn.at[c], xqn.at[c], 7, mate),
        rcopy(rof.at[c], rof.at[c], S, mate), rcopy(rqn.at[c], rqn.at[c], 9, mate)]
    for k in range(Q):
        direct[k].wait_recv()
        fwd[k].start()
    for cp in local:
        cp.wait()
    direct[Q].wait_recv()
    direct[5].wait_recv()
    for cp in direct:
        cp.wait_send()
    for cp in fwd:
        cp.wait()


def load_rows(srcs, dst2, tmp, sem):
    copies = [pltpu.make_async_copy(s, tmp.at[i % 2], sem.at[i % 2]) for i, s in enumerate(srcs)]
    copies[0].start()
    for i in range(len(srcs)):
        if i + 1 < len(srcs):
            copies[i + 1].start()
        copies[i].wait()

        def body(b, carry, i=i):
            r0 = pl.multiple_of(b * 64, 64)
            for s in range(S):
                dst2[pl.ds((i * NB + r0) * S + s, 64, stride=S), :] = tmp[i % 2, pl.ds(r0, 64), L * s:L * (s + 1)].astype(F32)
            return carry

        lax.fori_loop(0, NB // 64, body, 0)


def rows2d(ref2, base):
    return [ref2[pl.ds(base * S + s, T, stride=S), :] for s in range(S)]


def zero_rows(ref2, n):
    def body(i, carry):
        ref2[pl.ds(pl.multiple_of(i * 64, 64), 64), :] = jnp.zeros((64, L), F32)
        return carry
    lax.fori_loop(0, n // 64, body, 0)


def row8(t):
    return pl.ds(pl.multiple_of(t * S, S), S)


def own_kernel(cnt, idx, gat, pid, xn, xf, rn, rf, w1, w3, w2,
               y_out, dx_out, dgt_out,
               x2, r2, u2, rr2, gb, o2, d2, dgs, dgd, tmp, sem):
    e = pl.program_id(0)

    @pl.when(e == 0)
    def _():
        zero_rows(y_out, R1)
        zero_rows(dx_out, R1)
        zero_rows(u2, 1024 * S + 64)
        zero_rows(rr2, 1024 * S + 64)
        dgd[...] = jnp.zeros_like(dgd)
        x2[8192:8256, :] = jnp.zeros((64, L), F32)
        r2[8192:8256, :] = jnp.zeros((64, L), F32)
        load_rows([xn.at[0], xn.at[1], xf.at[0], xf.at[1]], x2, tmp, sem)
        load_rows([rn.at[0], rn.at[1], rf.at[0], rf.at[1]], r2, tmp, sem)

    n = cnt[0, e, 0]
    sio = lax.broadcasted_iota(jnp.int32, (S, L), 0)

    def gather_body(c, carry):
        ih = c // 16
        il = (c % 16) * S
        ts = [idx[e, ih, il + j] for j in range(S)]
        gs = [gat[e, ih, il + j] for j in range(S)]
        xs = [x2[row8(t), :] for t in ts]
        rs = [r2[row8(t), :] for t in ts]
        gv = jnp.full((S, L), gs[0], F32)
        for j in range(1, S):
            gv = jnp.where(sio == j, gs[j], gv)
        for j in range(S):
            u2[row8(c * S + j), :] = xs[j]
            rr2[row8(c * S + j), :] = rs[j]
        gb[row8(c), :] = gv
        return carry

    lax.fori_loop(0, (n + 7) // S, gather_body, 0)

    lane = lax.broadcasted_iota(jnp.int32, (T, L), 1)
    rown = lax.broadcasted_iota(jnp.int32, (T, L), 0)

    def tile_body(k, carry):
        base = k * T
        u = jnp.concatenate([p.astype(BF16) for p in rows2d(u2, base)], axis=1)
        gcol = jnp.where(rown + base < n, gb[pl.ds(pl.multiple_of(base, T), T), :], 0.0)
        do = jnp.concatenate([(p * gcol).astype(BF16) for p in rows2d(rr2, base)], axis=1)
        h1 = dot(u, w1[0])
        h3 = dot(u, w3[0])
        sg = jax.nn.sigmoid(h1)
        sl = h1 * sg
        a = (sl * h3).astype(BF16)
        o = dot(a, w2[0]).astype(BF16).astype(F32)
        da = dot(do, w2[0], 1, 1)
        dh1 = (da * h3 * sg * (1.0 + h1 * (1.0 - sg))).astype(BF16)
        dh3 = (da * sl).astype(BF16)
        dr = (dot(dh1, w1[0], 1, 1) + dot(dh3, w3[0], 1, 1)).astype(BF16).astype(F32)
        acc = jnp.zeros((T, L), F32)
        rp = rows2d(rr2, base)
        for s in range(S):
            os = o[:, L * s:L * (s + 1)]
            o2[pl.ds(s, T, stride=S), :] = os
            d2[pl.ds(s, T, stride=S), :] = dr[:, L * s:L * (s + 1)]
            acc = acc + os * rp[s]
        dgc = jnp.sum(acc, axis=1, keepdims=True)
        dgs[...] = jnp.where(lane == e, dgc, 0.0)

        def scat_body(c, carry2):
            cc = c + base // S
            ih = cc // 16
            il = (cc % 16) * S
            ts = [idx[e, ih, il + j] for j in range(S)]
            gs = [gat[e, ih, il + j] for j in range(S)]
            ys = [y_out[row8(ts[j]), :] + gs[j] * o2[row8(c * S + j), :] for j in range(S)]
            ds = [dx_out[row8(ts[j]), :] + d2[row8(c * S + j), :] for j in range(S)]
            dg8 = dgs[row8(c), :]
            gd = [dgd[pl.ds(ts[j], 1), :] + dg8[j:j + 1, :] for j in range(S)]
            for j in range(S):
                y_out[row8(ts[j]), :] = ys[j]
                dx_out[row8(ts[j]), :] = ds[j]
                dgd[pl.ds(ts[j], 1), :] = gd[j]
            return carry2

        lax.fori_loop(0, (jnp.minimum(n - base, T) + 7) // S, scat_body, 0)
        return carry

    lax.fori_loop(0, (n + T - 1) // T, tile_body, 0)

    @pl.when(e == NE - 1)
    def _():
        xc = pid[1] // 2
        tr = jnp.transpose(dgd[0:HALF, :])
        dgt_out[:, pl.ds(pl.multiple_of(xc * 512, 512), 512)] = tr[0:S, 0:512]
        dgt_out[:, pl.ds(pl.multiple_of(512 - xc * 512, 512), 512)] = tr[0:S, 512:1024]


def pair_kernel(yp, dxp, dgt, ynear, yfar, dnear, dfar, dg_out, rbuf, obuf, dgb, ssem, rsem, lsem, gsend, grecv):
    dp = lax.axis_index('dp')
    ep = lax.axis_index('ep')
    c = ep % 2
    me = dp * Q + ep
    mate = (dp, (ep // 2) * 2 + 1 - c)
    barrier_all(dp, ep)
    parts = [(yp, 4096), (dxp, 4096), (yp, 0), (dxp, 0)]
    outs = [yfar, dfar, ynear, dnear]
    sends, loads = [], []
    for i, (src, base) in enumerate(parts):
        cp = pltpu.make_async_remote_copy(
            src_ref=src.at[pl.ds(pl.multiple_of(base + (1 - c) * 2048, 2048), 2048)], dst_ref=rbuf.at[i],
            send_sem=ssem.at[i], recv_sem=rsem.at[i], device_id=mate, device_id_type=MESH)
        cp.start()
        sends.append(cp)
        ld = pltpu.make_async_copy(src.at[pl.ds(pl.multiple_of(base + c * 2048, 2048), 2048)], obuf.at[i], lsem.at[i])
        ld.start()
        loads.append(ld)
    gcopies = []
    for k in range(1, S):
        dev = ((dp + k // Q) % 2, (ep + k % Q) % Q)
        cp = pltpu.make_async_remote_copy(src_ref=dgt, dst_ref=dgb.at[me], send_sem=gsend.at[k - 1], recv_sem=grecv.at[k - 1], device_id=dev, device_id_type=MESH)
        cp.start()
        gcopies.append(cp)
    for i in range(Q):
        loads[i].wait()
        sends[i].wait_recv()

        def body(b, carry, i=i):
            s = pl.ds(pl.multiple_of(b * L, L), L)
            outs[i][s, :] = obuf[i, s, :] + rbuf[i, s, :]
            return carry

        lax.fori_loop(0, 16, body, 0)
    for cp in gcopies:
        cp.wait()
    for cp in sends:
        cp.wait_send()
    dgb[me] = dgt[...]
    dg_out[...] = dgb[...]


def grad_kernel(cnt, idx, gat, xon, xof, xqn, xqf, ron, rof, rqn, rqf, w1, w3, w2,
                g1, g3, g2, x2, r2, u2, d2, tmp, sem):
    e = pl.program_id(0)

    @pl.when(e == 0)
    def _():
        zero_rows(u2, 2048 * S + 64)
        zero_rows(d2, 2048 * S + 64)
        x2[16384:16448, :] = jnp.zeros((64, L), F32)
        r2[16384:16448, :] = jnp.zeros((64, L), F32)
        load_rows([a.at[i] for a in (xon, xof, xqn, xqf) for i in range(2)], x2, tmp, sem)
        load_rows([a.at[i] for a in (ron, rof, rqn, rqf) for i in range(2)], r2, tmp, sem)

    n0 = cnt[0, e, 0]
    n = n0 + cnt[1, e, 0]

    def gather_half(h):
        def body(c, carry):
            ih = c // 16
            il = (c % 16) * S
            ts = [idx[h * S + e, ih, il + j] + h * HALF for j in range(S)]
            gs = [gat[h * S + e, ih, il + j] for j in range(S)]
            xs = [x2[row8(t), :] for t in ts]
            rs = [r2[row8(t), :] * g for t, g in zip(ts, gs)]
            for j in range(S):
                u2[row8(h * n0 + c * S + j), :] = xs[j]
                d2[row8(h * n0 + c * S + j), :] = rs[j]
            return carry
        lax.fori_loop(0, (cnt[h, e, 0] + 7) // S, body, 0)

    gather_half(0)
    gather_half(1)
    rown = lax.broadcasted_iota(jnp.int32, (T, L), 0)

    def tile(k, first):
        base = k * T
        u = jnp.concatenate([p.astype(BF16) for p in rows2d(u2, base)], axis=1)
        live = rown + base < n
        do = jnp.concatenate([jnp.where(live, p, 0.0).astype(BF16) for p in rows2d(d2, base)], axis=1)
        h1 = dot(u, w1[0])
        h3 = dot(u, w3[0])
        sg = jax.nn.sigmoid(h1)
        sl = h1 * sg
        a = (sl * h3).astype(BF16)
        da = dot(do, w2[0], 1, 1)
        dh1 = (da * h3 * sg * (1.0 + h1 * (1.0 - sg))).astype(BF16)
        dh3 = (da * sl).astype(BF16)
        if first:
            g1[0] = dot(u, dh1, 0, 0)
            g3[0] = dot(u, dh3, 0, 0)
            g2[0] = dot(a, do, 0, 0)
        else:
            g1[0] += dot(u, dh1, 0, 0)
            g3[0] += dot(u, dh3, 0, 0)
            g2[0] += dot(a, do, 0, 0)

    tile(0, True)

    def tile_body(k, carry):
        tile(k, False)
        return carry

    lax.fori_loop(1, (n + T - 1) // T, tile_body, 0)


def final_kernel(pid, x, r, ynear, dnear, yrec, drec, dg, gt, wr, xon, xof, xqn, xqf,
                 y_out, dx_out, dw_out, dz_s):
    dp = pid[0]
    ep = pid[1]
    xc = ep // 2
    for b in range(S):
        gm = jnp.maximum(gt[b], 0.0)
        dgv = dg[32 * (b // Q):32 * (b // Q + 1), NB * (b % Q):NB * (b % Q + 1)]
        s = jnp.sum(gm * dgv, axis=0, keepdims=True)
        dz_s[b] = (gm * (dgv - s)).astype(BF16)
    acc = jnp.zeros((32, D), F32)
    for h, arrs in enumerate(((xon, xof), (xqn, xqf))):
        hd = dp if h == 0 else 1 - dp
        for f, arr in enumerate(arrs):
            xx = xc if f == 0 else 1 - xc
            for c in range(2):
                acc = acc + dot(dz_s[hd * Q + xx * 2 + c], arr[c])
    dw_out[...] = acc
    dxr = dot(dz_s[dp * Q + ep], wr[...], 0, 0)
    for s in range(S):
        cs = slice(L * s, L * (s + 1))
        rows = pl.ds(s, NB, stride=S)
        y_out[:, cs] = x[:, cs].astype(F32) + (ynear[rows, :] + yrec[rows, :])
        dx_out[:, cs] = r[:, cs].astype(F32) + dxr[:, cs] + (dnear[rows, :] + drec[rows, :])


def solution(mesh):
    axes = ('dp', 'ep')
    sds = jax.ShapeDtypeStruct

    def local_step(tokens, w_router, w_gate, w_up, w_down, top_ids, r_proj):
        pid = jnp.stack([lax.axis_index('dp'), lax.axis_index('ep')]).astype(jnp.int32)
        near = sds((2, NB, D), BF16)
        dma = pltpu.SemaphoreType.DMA
        xon, xof, ron, rof, xqn, rqn, gt, idx, gat, cnt = pl.pallas_call(
            gather_kernel,
            out_shape=[near] * 6 + [sds((S, 32, NB), F32), sds((16, S, L), jnp.int32), sds((16, S, L), F32), sds((2, S, L), jnp.int32)],
            in_specs=[vspec()] * Q,
            out_specs=[aspec()] * 6 + [vspec()] * Q,
            scratch_shapes=[pltpu.VMEM((S, 32, NB), F32), pltpu.VMEM((S, S, NB), F32), pltpu.VMEM((S, 32, NB), BF16),
                            dma((10,)), dma((10,)), dma((2,)), dma((7,)), dma((7,))],
            compiler_params=pltpu.CompilerParams(collective_id=0, has_side_effects=True),
            name='k0_gather',
        )(tokens, r_proj, top_ids.T, w_router.T)

        xswap = [(0, 2), (2, 0), (1, 3), (3, 1)]
        xqf = lax.ppermute(xqn, 'ep', xswap)
        rqf = lax.ppermute(rof, 'dp', [(0, 1), (1, 0)])

        wspec = [pl.BlockSpec((1, D, FF), lambda e: (e, 0, 0)), pl.BlockSpec((1, D, FF), lambda e: (e, 0, 0)), pl.BlockSpec((1, FF, D), lambda e: (e, 0, 0))]
        part = sds((R1, L), F32)
        pspec = pl.BlockSpec((R1, L), lambda e: (0, 0))
        yp, dxp, dgt = pl.pallas_call(
            own_kernel,
            grid=(NE,),
            out_shape=[part, part, sds((S, HALF), F32)],
            in_specs=[sspec()] * Q + [aspec()] * Q + wspec,
            out_specs=[pspec, pspec, pl.BlockSpec((S, HALF), lambda e: (0, 0))],
            scratch_shapes=[pltpu.VMEM((R1, L), F32), pltpu.VMEM((R1, L), F32),
                            pltpu.VMEM((R1, L), F32), pltpu.VMEM((R1, L), F32),
                            pltpu.VMEM((RB, L), F32),
                            pltpu.VMEM((T * S, L), F32), pltpu.VMEM((T * S, L), F32),
                            pltpu.VMEM((T, L), F32), pltpu.VMEM((RB, L), F32),
                            pltpu.VMEM((2, NB, D), BF16), dma((2,))],
            compiler_params=pltpu.CompilerParams(vmem_limit_bytes=VMEM_MAX, dimension_semantics=('arbitrary',)),
            cost_estimate=pl.CostEstimate(flops=20 * 10 ** 9, bytes_accessed=40 * 10 ** 6, transcendentals=0),
            name='k1_own',
        )(cnt, idx, gat, pid, xon, xof, ron, rof, w_gate, w_up, w_down)

        quarter = sds((NB * S, L), F32)
        ynear, yfar, dnear, dfar, dg = pl.pallas_call(
            pair_kernel,
            out_shape=[quarter] * Q + [sds((S, S, HALF), F32)],
            in_specs=[aspec(), aspec(), vspec()],
            out_specs=[vspec()] * 5,
            scratch_shapes=[pltpu.VMEM((Q, NB * S, L), F32), pltpu.VMEM((Q, NB * S, L), F32), pltpu.VMEM((S, S, HALF), F32),
                            dma((Q,)), dma((Q,)), dma((Q,)), dma((7,)), dma((7,))],
            compiler_params=pltpu.CompilerParams(collective_id=1, has_side_effects=True),
            name='k2_pair',
        )(yp, dxp, dgt)

        yrec = lax.ppermute(yfar, 'ep', xswap)
        drec = lax.ppermute(dfar, 'ep', xswap)

        gspec = [pl.BlockSpec((1, D, FF), lambda e: (e, 0, 0)), pl.BlockSpec((1, D, FF), lambda e: (e, 0, 0)), pl.BlockSpec((1, FF, D), lambda e: (e, 0, 0))]
        grad_gate, grad_up, grad_down = pl.pallas_call(
            grad_kernel,
            grid=(NE,),
            out_shape=[sds((NE, D, FF), F32), sds((NE, D, FF), F32), sds((NE, FF, D), F32)],
            in_specs=[sspec()] * 3 + [aspec()] * S + wspec,
            out_specs=gspec,
            scratch_shapes=[pltpu.VMEM((R2, L), F32), pltpu.VMEM((R2, L), F32),
                            pltpu.VMEM((R2, L), F32), pltpu.VMEM((R2, L), F32),
                            pltpu.VMEM((2, NB, D), BF16), dma((2,))],
            compiler_params=pltpu.CompilerParams(vmem_limit_bytes=VMEM_MAX, dimension_semantics=('arbitrary',)),
            cost_estimate=pl.CostEstimate(flops=30 * 10 ** 9, bytes_accessed=90 * 10 ** 6, transcendentals=0),
            name='k3_grad',
        )(cnt, idx, gat, xon, xof, xqn, xqf, ron, rof, rqn, rqf, w_gate, w_up, w_down)

        y, dx, dwt = pl.pallas_call(
            final_kernel,
            out_shape=[sds((NB, D), F32), sds((NB, D), F32), sds((32, D), F32)],
            in_specs=[sspec()] + [vspec()] * 13,
            out_specs=[vspec()] * 3,
            scratch_shapes=[pltpu.VMEM((S, 32, NB), BF16)],
            compiler_params=pltpu.CompilerParams(vmem_limit_bytes=VMEM_MAX),
            name='k4_final',
        )(pid, tokens, r_proj, ynear, dnear, yrec, drec, dg.reshape(64, HALF), gt, w_router.T, xon, xof, xqn, xqf)
        return y, dx, grad_gate, grad_up, grad_down, dwt.T

    tok_spec = P(axes, None)
    exp_spec = P('ep', None, None)
    return jax.shard_map(local_step, mesh=mesh, in_specs=(tok_spec, P(), exp_spec, exp_spec, exp_spec, tok_spec, tok_spec), out_specs=(tok_spec, tok_spec, exp_spec, exp_spec, exp_spec, P()), check_vma=False)
```

```python
import functools

import jax
import jax.numpy as jnp
from jax import lax
from jax.experimental import pallas as pl
from jax.experimental.pallas import tpu as pltpu
from jax.sharding import PartitionSpec as P

F32 = jnp.float32
BF16 = jnp.bfloat16
MESH = pl.DeviceIdType.MESH
VMEM_MAX = 63 * 1024 * 1024
T = 256
NB = 256
HALF = 1024
D = 1024
FF = 512
NE = 8
NL = 17
SLOTS = 4
S = 8
L = 128
Q = 4
RB = 1032
R1 = 8256
R2 = 16448


def dot(a, b, ca=1, cb=0):
    return lax.dot_general(a, b, (((ca,), (cb,)), ((), ())), preferred_element_type=F32)


def vspec():
    return pl.BlockSpec(memory_space=pltpu.VMEM)


def aspec():
    return pl.BlockSpec(memory_space=pl.ANY)


def sspec():
    return pl.BlockSpec(memory_space=pltpu.SMEM)


def barrier_all(dp, ep):
    bar = pltpu.get_barrier_semaphore()
    for k in range(1, S):
        pl.semaphore_signal(bar, inc=1, device_id=((dp + k // Q) % 2, (ep + k % Q) % Q), device_id_type=MESH)
    pl.semaphore_wait(bar, 7)


def gather_kernel(x_ref, r_ref, ids_ref, wr_ref,
                  xon, xof, ron, rof, xqn, rqn, gt_out, idx_out, gat_out, cnt_out,
                  gt_s, pos_s, v_s, ssem, rsem, lsem, gsend, grecv):
    dp = lax.axis_index('dp')
    ep = lax.axis_index('ep')
    c = ep % 2
    xc = ep // 2
    me = dp * Q + ep
    mate = (dp, xc * 2 + 1 - c)
    xnb = (dp, (1 - xc) * 2 + c)
    ynb = (1 - dp, ep)
    barrier_all(dp, ep)

    def rcopy(src, dst, k, dev):
        return pltpu.make_async_remote_copy(src_ref=src, dst_ref=dst, send_sem=ssem.at[k], recv_sem=rsem.at[k], device_id=dev, device_id_type=MESH)

    zt = dot(wr_ref[...], x_ref[...], 1, 1)
    eio = lax.broadcasted_iota(jnp.int32, (32, NB), 0)
    sel = eio == ids_ref[0:1, :]
    for j in range(1, S):
        sel = sel | (eio == ids_ref[j:j + 1, :])
    zm = jnp.max(jnp.where(sel, zt, -jnp.inf), axis=0, keepdims=True)
    pe = jnp.where(sel, jnp.exp(zt - zm), 0.0)
    gt_out[...] = jnp.where(sel, pe / jnp.sum(pe, axis=0, keepdims=True), -1.0)
    gt_s[me] = gt_out[pl.ds(pl.multiple_of(ep * S, S), S), :]
    gcopies = []
    for k in range(1, S):
        dev = ((dp + k // Q) % 2, (ep + k % Q) % Q)
        cp = pltpu.make_async_remote_copy(src_ref=gt_out.at[pl.ds(pl.multiple_of(dev[1] * S, S), S)], dst_ref=gt_s.at[me], send_sem=gsend.at[k - 1], recv_sem=grecv.at[k - 1], device_id=dev, device_id_type=MESH)
        cp.start()
        gcopies.append(cp)
    direct = [
        rcopy(x_ref, xof.at[c], 0, xnb), rcopy(x_ref, xqn.at[c], 1, ynb),
        rcopy(r_ref, rof.at[c], 2, xnb), rcopy(r_ref, rqn.at[c], 3, ynb),
        rcopy(x_ref, xon.at[c], Q, mate), rcopy(r_ref, ron.at[c], 5, mate)]
    for cp in direct:
        cp.start()
    local = [pltpu.make_async_copy(x_ref, xon.at[c], lsem.at[0]), pltpu.make_async_copy(r_ref, ron.at[c], lsem.at[1])]
    for cp in local:
        cp.start()
    for cp in gcopies:
        cp.wait()

    tri = (lax.broadcasted_iota(jnp.int32, (NB, NB), 0) < lax.broadcasted_iota(jnp.int32, (NB, NB), 1)).astype(BF16)
    srow = lax.broadcasted_iota(jnp.int32, (S, NB), 0)
    tlan = lax.broadcasted_iota(jnp.int32, (S, NB), 1).astype(F32)
    for half in range(2):
        base = jnp.zeros((S, 1), F32)
        for k in range(Q):
            hd = dp if half == 0 else 1 - dp
            xx = xc if k < 2 else 1 - xc
            g = gt_s[hd * Q + xx * 2 + k % 2]
            m = g >= 0.0
            mf = m.astype(F32)
            pos = dot(mf.astype(BF16), tri) + base
            pos_s[half * Q + k] = jnp.where(m, pos, -1.0)
            base = base + jnp.sum(mf, axis=1, keepdims=True)
            g = jnp.where(m, g, 0.0)
            g1 = g.astype(BF16)
            e1 = g - g1.astype(F32)
            g2 = e1.astype(BF16)
            g3 = (e1 - g2.astype(F32)).astype(BF16)
            head = jnp.where(srow == 0, tlan, jnp.where(srow == 1, float(k), 0.0))
            v_s[half * Q + k] = jnp.concatenate([head, g1.astype(F32), g2.astype(F32), g3.astype(F32)], axis=0).astype(BF16)
        cnt_out[half] = jnp.broadcast_to(base, (S, L)).astype(jnp.int32)

    pio = lax.broadcasted_iota(jnp.int32, (NB, NB), 0).astype(F32)
    rio = lax.broadcasted_iota(jnp.int32, (32, NB), 0)
    lio = lax.broadcasted_iota(jnp.int32, (1, NB), 1)

    def list_body(he, carry):
        half = he // S
        e = he % S
        cnt_e = cnt_out[half, pl.ds(e, 1), 0:1]
        for pt in range(Q):
            acc = jnp.zeros((32, NB), F32)
            for k in range(pt, Q):
                prow = pos_s[half * Q + k, pl.ds(e, 1), :] - float(256 * pt)
                oh = (pio == prow).astype(F32).astype(BF16)
                acc = acc + dot(v_s[half * Q + k], oh, 1, 1)
            ids = (acc[0:1, :] + 256.0 * acc[1:2, :]).astype(jnp.int32)
            ids = jnp.where(lio + NB * pt < cnt_e, ids, HALF) + half * HALF
            gv = jnp.sum(jnp.where((rio >= S) & (rio % S == e), acc, 0.0), axis=0, keepdims=True)
            for q in range(2):
                idx_out[he, 2 * pt + q:2 * pt + q + 1, :] = ids[:, L * q:L * (q + 1)]
                gat_out[he, 2 * pt + q:2 * pt + q + 1, :] = gv[:, L * q:L * (q + 1)]
        return carry

    lax.fori_loop(0, 2 * S, list_body, 0)
    idx_out[2 * S] = jnp.zeros((S, L), jnp.int32)
    gat_out[2 * S] = jnp.zeros((S, L), F32)

    fwd = [
        rcopy(xof.at[c], xof.at[c], 6, mate), rcopy(xqn.at[c], xqn.at[c], 7, mate),
        rcopy(rof.at[c], rof.at[c], S, mate), rcopy(rqn.at[c], rqn.at[c], 9, mate)]
    for k in range(Q):
        direct[k].wait_recv()
        fwd[k].start()
    for cp in local:
        cp.wait()
    direct[Q].wait_recv()
    direct[5].wait_recv()
    for cp in direct:
        cp.wait_send()
    for cp in fwd:
        cp.wait()


def load_rows(srcs, tmp, sem):
    copies = [pltpu.make_async_copy(src, tmp.at[i % SLOTS], sem.at[i % SLOTS]) for i, (src, _, _) in enumerate(srcs)]
    for i in range(SLOTS):
        copies[i].start()
    for i, (_, dst2, row) in enumerate(srcs):
        copies[i].wait()

        def body(b, carry, i=i, dst2=dst2, row=row):
            r0 = pl.multiple_of(b * 64, 64)
            for s in range(S):
                dst2[pl.ds((row + r0) * S + s, 64, stride=S), :] = tmp[i % SLOTS, pl.ds(r0, 64), L * s:L * (s + 1)].astype(F32)
            return carry

        lax.fori_loop(0, NB // 64, body, 0)
        if i + SLOTS < len(srcs):
            copies[i + SLOTS].start()


def load_tokens(pairs, x2, r2, tmp, sem):
    srcs = []
    for i, (xa, ra) in enumerate(pairs):
        for c in range(2):
            srcs.append((xa.at[c], x2, (2 * i + c) * NB))
            srcs.append((ra.at[c], r2, (2 * i + c) * NB))
    load_rows(srcs, tmp, sem)
    for ref in (x2, r2):
        ref[pl.ds(2 * len(pairs) * NB * S, 64), :] = jnp.zeros((64, L), F32)


def strided(ref2, s):
    return ref2[pl.ds(s, T, stride=S), :]


def zero_rows(ref2, n):
    def body(i, carry):
        ref2[pl.ds(pl.multiple_of(i * 64, 64), 64), :] = jnp.zeros((64, L), F32)
        return carry
    lax.fori_loop(0, n // 64, body, 0)


def row8(t):
    return pl.ds(pl.multiple_of(t * S, S), S)


def own_kernel(cnt, idx, gat, pid, gatv, xn, xf, rn, rf, w1, w3, w2,
               y_out, dx_out, dgt_out,
               x2, r2, ust, rst, us, rs, ds, o2, d2, dgs, dgd, tmp, prev, sem):
    e = pl.program_id(0)

    def gather(base, r0, n):
        for r in range(n):
            t = row8(idx[base + r])
            ust[row8(r0 + r), :] = x2[t, :]
            rst[row8(r0 + r), :] = r2[t, :]

    def scatter(base, r0, n):
        for c in range(0, n, S):
            ts = [idx[base + c + j] for j in range(S)]
            gs = [gat[base + c + j] for j in range(S)]
            ys = [y_out[row8(ts[j]), :] + gs[j] * o2[row8(r0 + c + j), :] for j in range(S)]
            dl = [dx_out[row8(ts[j]), :] + d2[row8(r0 + c + j), :] for j in range(S)]
            gd = [dgd[pl.ds(ts[j], 1), :] + dgs[pl.ds(r0 + c + j, 1), :] for j in range(S)]
            for j in range(S):
                y_out[row8(ts[j]), :] = ys[j]
                dx_out[row8(ts[j]), :] = dl[j]
                dgd[pl.ds(ts[j], 1), :] = gd[j]

    @pl.when(e == 0)
    def _():
        load_tokens([(xn, rn), (xf, rf)], x2, r2, tmp, sem)
        zero_rows(y_out, R1)
        zero_rows(dx_out, R1)
        zero_rows(o2, T * S)
        zero_rows(d2, T * S)
        dgd[...] = jnp.zeros_like(dgd)
        dgs[...] = jnp.zeros_like(dgs)
        prev[0] = 0

        def first(c, carry):
            gather(c * S, c * S, S)
            return carry
        lax.fori_loop(0, T // S, first, 0)

    n = cnt[0, e, 0]
    lane = lax.broadcasted_iota(jnp.int32, (T, L), 1)

    def tile_body(k, carry):
        base = k * T
        gcol = jnp.concatenate([jnp.transpose(jnp.broadcast_to(gatv[pl.ds(e * S + 2 * k + q, 1), :], (L, L))) for q in range(2)], axis=0)
        for s in range(S):
            cs = slice(L * s, L * (s + 1))
            us[:, cs] = strided(ust, s).astype(BF16)
            rv = strided(rst, s)
            rs[:, cs] = rv.astype(BF16)
            ds[:, cs] = (rv * gcol).astype(BF16)
        more = base + T < n
        gather(jnp.where(more, e * HALF + base + T, jnp.minimum(e + 1, NE - 1) * HALF), 0, T)
        scatter(prev[0], 0, T)
        u = us[...]
        h1 = dot(u, w1[0])
        h3 = dot(u, w3[0])
        sg = jax.nn.sigmoid(h1)
        sl = h1 * sg
        a = (sl * h3).astype(BF16)
        o = dot(a, w2[0]).astype(BF16).astype(F32)
        da = dot(ds[...], w2[0], 1, 1)
        dh1 = (da * h3 * sg * (1.0 + h1 * (1.0 - sg))).astype(BF16)
        dh3 = (da * sl).astype(BF16)
        dr = (dot(dh1, w1[0], 1, 1) + dot(dh3, w3[0], 1, 1)).astype(BF16).astype(F32)
        acc = jnp.zeros((T, L), F32)
        for s in range(S):
            cs = slice(L * s, L * (s + 1))
            o2[pl.ds(s, T, stride=S), :] = o[:, cs]
            d2[pl.ds(s, T, stride=S), :] = dr[:, cs]
            acc = acc + o[:, cs] * rs[:, cs].astype(F32)
        dgc = jnp.sum(acc, axis=1, keepdims=True)
        dgs[...] = jnp.where(lane == e, dgc, 0.0)
        prev[0] = e * HALF + base
        return carry

    lax.fori_loop(0, jnp.maximum((n + T - 1) // T, 1), tile_body, 0)

    @pl.when(e == NE - 1)
    def _():
        def last(c, carry):
            scatter(prev[0] + c * S, c * S, S)
            return carry
        lax.fori_loop(0, T // S, last, 0)
        xc = pid[1] // 2
        tr = jnp.transpose(dgd[0:HALF, :])
        dgt_out[:, pl.ds(pl.multiple_of(xc * FF, FF), FF)] = tr[0:S, 0:FF]
        dgt_out[:, pl.ds(pl.multiple_of(FF - xc * FF, FF), FF)] = tr[0:S, FF:HALF]


def pair_kernel(yp, dxp, dgt, gt, ynear, yfar, dnear, dfar, dg_out, gt_out, rbuf, obuf, dgb, gtb, ssem, rsem, lsem, gsend, grecv):
    dp = lax.axis_index('dp')
    ep = lax.axis_index('ep')
    c = ep % 2
    me = dp * Q + ep
    mate = (dp, (ep // 2) * 2 + 1 - c)
    barrier_all(dp, ep)
    parts = [(yp, 4096), (dxp, 4096), (yp, 0), (dxp, 0)]
    outs = [yfar, dfar, ynear, dnear]
    sends, loads = [], []
    for i, (src, base) in enumerate(parts):
        cp = pltpu.make_async_remote_copy(
            src_ref=src.at[pl.ds(pl.multiple_of(base + (1 - c) * 2048, 2048), 2048)], dst_ref=rbuf.at[i],
            send_sem=ssem.at[i], recv_sem=rsem.at[i], device_id=mate, device_id_type=MESH)
        cp.start()
        sends.append(cp)
        ld = pltpu.make_async_copy(src.at[pl.ds(pl.multiple_of(base + c * 2048, 2048), 2048)], obuf.at[i], lsem.at[i])
        ld.start()
        loads.append(ld)
    gcopies = []
    for k in range(1, S):
        dev = ((dp + k // Q) % 2, (ep + k % Q) % Q)
        for q, (src, dst) in enumerate(((dgt, dgb), (gt, gtb))):
            cp = pltpu.make_async_remote_copy(src_ref=src, dst_ref=dst.at[me], send_sem=gsend.at[q, k - 1], recv_sem=grecv.at[q, k - 1], device_id=dev, device_id_type=MESH)
            cp.start()
            gcopies.append(cp)
    for i in range(Q):
        loads[i].wait()
        sends[i].wait_recv()

        def body(b, carry, i=i):
            s = pl.ds(pl.multiple_of(b * L, L), L)
            outs[i][s, :] = obuf[i, s, :] + rbuf[i, s, :]
            return carry

        lax.fori_loop(0, 16, body, 0)
    for cp in gcopies:
        cp.wait()
    for cp in sends:
        cp.wait_send()
    dgb[me] = dgt[...]
    dg_out[...] = dgb[...]
    gtb[me] = gt[...]
    gt_out[...] = gtb[...]


def grad_kernel(cnt, idx, gat, xon, xof, xqn, xqf, ron, rof, rqn, rqf, w1, w3, w2,
                g1, g3, g2, x2, r2, ust, dst, us, ds, tmp, sem):
    e = pl.program_id(0)

    def gather(ne, nb, r0, n):
        n0 = cnt[0, ne, 0]
        a0 = ne * HALF
        a1 = NE * HALF + a0 - n0
        for r in range(n):
            q = nb + r
            q = q + jnp.where(q < n0, a0, a1)
            t = row8(idx[q])
            ust[row8(r0 + r), :] = x2[t, :]
            dst[row8(r0 + r), :] = r2[t, :] * gat[q]

    @pl.when(e == 0)
    def _():
        load_tokens([(xon, ron), (xof, rof), (xqn, rqn), (xqf, rqf)], x2, r2, tmp, sem)

        def first(c, carry):
            gather(0, c * S, c * S, S)
            return carry
        lax.fori_loop(0, T // S, first, 0)

    n = cnt[0, e, 0] + cnt[1, e, 0]
    rown = lax.broadcasted_iota(jnp.int32, (T, L), 0)

    def tile(k, first):
        base = k * T
        live = rown + base < n
        for s in range(S):
            cs = slice(L * s, L * (s + 1))
            us[:, cs] = strided(ust, s).astype(BF16)
            ds[:, cs] = jnp.where(live, strided(dst, s), 0.0).astype(BF16)
        more = base + T < n
        gather(jnp.where(more, e, jnp.minimum(e + 1, NE - 1)), jnp.where(more, base + T, 0), 0, T)
        u = us[...]
        do = ds[...]
        h1 = dot(u, w1[0])
        h3 = dot(u, w3[0])
        sg = jax.nn.sigmoid(h1)
        sl = h1 * sg
        a = (sl * h3).astype(BF16)
        da = dot(do, w2[0], 1, 1)
        dh1 = (da * h3 * sg * (1.0 + h1 * (1.0 - sg))).astype(BF16)
        dh3 = (da * sl).astype(BF16)
        if first:
            g1[0] = dot(u, dh1, 0, 0)
            g3[0] = dot(u, dh3, 0, 0)
            g2[0] = dot(a, do, 0, 0)
        else:
            g1[0] += dot(u, dh1, 0, 0)
            g3[0] += dot(u, dh3, 0, 0)
            g2[0] += dot(a, do, 0, 0)

    tile(0, True)

    def tile_body(k, carry):
        tile(k, False)
        return carry

    lax.fori_loop(1, (n + T - 1) // T, tile_body, 0)


def final_kernel(pid, x, r, ynear, dnear, yrec, drec, dg, gt, wr, xon, xof, xqn, xqf,
                 y_out, dx_out, dw_out, dz_s):
    dp = pid[0]
    ep = pid[1]
    xc = ep // 2
    for b in range(S):
        gm = jnp.maximum(gt[b], 0.0)
        dgv = dg[32 * (b // Q):32 * (b // Q + 1), NB * (b % Q):NB * (b % Q + 1)]
        s = jnp.sum(gm * dgv, axis=0, keepdims=True)
        dz_s[b] = (gm * (dgv - s)).astype(BF16)
    acc = jnp.zeros((32, D), F32)
    for h, arrs in enumerate(((xon, xof), (xqn, xqf))):
        hd = dp if h == 0 else 1 - dp
        for f, arr in enumerate(arrs):
            xx = xc if f == 0 else 1 - xc
            for c in range(2):
                acc = acc + dot(dz_s[hd * Q + xx * 2 + c], arr[c])
    dw_out[...] = acc
    dxr = dot(dz_s[dp * Q + ep], wr[...], 0, 0)
    for s in range(S):
        cs = slice(L * s, L * (s + 1))
        rows = pl.ds(s, NB, stride=S)
        y_out[:, cs] = x[:, cs].astype(F32) + (ynear[rows, :] + yrec[rows, :])
        dx_out[:, cs] = r[:, cs].astype(F32) + dxr[:, cs] + (dnear[rows, :] + drec[rows, :])


def solution(mesh):
    axes = ('dp', 'ep')
    sds = jax.ShapeDtypeStruct

    def local_step(tokens, w_router, w_gate, w_up, w_down, top_ids, r_proj):
        pid = jnp.stack([lax.axis_index('dp'), lax.axis_index('ep')]).astype(jnp.int32)
        near = sds((2, NB, D), BF16)
        dma = pltpu.SemaphoreType.DMA
        xon, xof, ron, rof, xqn, rqn, gto, idx, gat, cnt = pl.pallas_call(
            gather_kernel,
            out_shape=[near] * 6 + [sds((32, NB), F32), sds((NL, S, L), jnp.int32), sds((NL, S, L), F32), sds((2, S, L), jnp.int32)],
            in_specs=[vspec()] * Q,
            out_specs=[aspec()] * 6 + [vspec()] * Q,
            scratch_shapes=[pltpu.VMEM((S, S, NB), F32), pltpu.VMEM((S, S, NB), F32), pltpu.VMEM((S, 32, NB), BF16),
                            dma((10,)), dma((10,)), dma((2,)), dma((7,)), dma((7,))],
            compiler_params=pltpu.CompilerParams(collective_id=0, has_side_effects=True),
            name='k0_gather',
        )(tokens, r_proj, top_ids.T, w_router.T)

        idx1 = idx.reshape(-1)
        gat1 = gat.reshape(-1)
        xswap = [(0, 2), (2, 0), (1, 3), (3, 1)]
        xqf = lax.ppermute(xqn, 'ep', xswap)
        rqf = lax.ppermute(rof, 'dp', [(0, 1), (1, 0)])

        wspec = [pl.BlockSpec((1, D, FF), lambda e: (e, 0, 0)), pl.BlockSpec((1, D, FF), lambda e: (e, 0, 0)), pl.BlockSpec((1, FF, D), lambda e: (e, 0, 0))]
        part = sds((R1, L), F32)
        pspec = pl.BlockSpec((R1, L), lambda e: (0, 0))
        yp, dxp, dgt = pl.pallas_call(
            own_kernel,
            grid=(NE,),
            out_shape=[part, part, sds((S, HALF), F32)],
            in_specs=[sspec()] * Q + [vspec()] + [aspec()] * Q + wspec,
            out_specs=[pspec, pspec, pl.BlockSpec((S, HALF), lambda e: (0, 0))],
            scratch_shapes=[pltpu.VMEM((R1, L), F32)] * 2 + [pltpu.VMEM((T * S, L), F32)] * 2 + [pltpu.VMEM((T, D), BF16)] * 3
            + [pltpu.VMEM((T * S, L), F32)] * 2 + [pltpu.VMEM((T, L), F32), pltpu.VMEM((RB, L), F32),
               pltpu.VMEM((SLOTS, NB, D), BF16), pltpu.SMEM((1,), jnp.int32), dma((SLOTS,))],
            compiler_params=pltpu.CompilerParams(vmem_limit_bytes=VMEM_MAX, dimension_semantics=('arbitrary',)),
            cost_estimate=pl.CostEstimate(flops=20 * 10 ** 9, bytes_accessed=40 * 10 ** 6, transcendentals=0),
            name='k1_own',
        )(cnt, idx1, gat1, pid, gat.reshape(NL * S, L), xon, xof, ron, rof, w_gate, w_up, w_down)

        quarter = sds((NB * S, L), F32)
        ynear, yfar, dnear, dfar, dg, gt = pl.pallas_call(
            pair_kernel,
            out_shape=[quarter] * Q + [sds((S, S, HALF), F32), sds((S, 32, NB), F32)],
            in_specs=[aspec(), aspec(), vspec(), vspec()],
            out_specs=[vspec()] * 6,
            scratch_shapes=[pltpu.VMEM((Q, NB * S, L), F32), pltpu.VMEM((Q, NB * S, L), F32), pltpu.VMEM((S, S, HALF), F32), pltpu.VMEM((S, 32, NB), F32),
                            dma((Q,)), dma((Q,)), dma((Q,)), dma((2, 7)), dma((2, 7))],
            compiler_params=pltpu.CompilerParams(collective_id=1, has_side_effects=True),
            name='k2_pair',
        )(yp, dxp, dgt, gto)

        yrec = lax.ppermute(yfar, 'ep', xswap)
        drec = lax.ppermute(dfar, 'ep', xswap)

        gspec = [pl.BlockSpec((1, D, FF), lambda e: (e, 0, 0)), pl.BlockSpec((1, D, FF), lambda e: (e, 0, 0)), pl.BlockSpec((1, FF, D), lambda e: (e, 0, 0))]
        grad_gate, grad_up, grad_down = pl.pallas_call(
            grad_kernel,
            grid=(NE,),
            out_shape=[sds((NE, D, FF), F32), sds((NE, D, FF), F32), sds((NE, FF, D), F32)],
            in_specs=[sspec()] * 3 + [aspec()] * S + wspec,
            out_specs=gspec,
            scratch_shapes=[pltpu.VMEM((R2, L), F32)] * 2 + [pltpu.VMEM((T * S, L), F32)] * 2 + [pltpu.VMEM((T, D), BF16)] * 2
            + [pltpu.VMEM((SLOTS, NB, D), BF16), dma((SLOTS,))],
            compiler_params=pltpu.CompilerParams(vmem_limit_bytes=VMEM_MAX, dimension_semantics=('arbitrary',)),
            cost_estimate=pl.CostEstimate(flops=30 * 10 ** 9, bytes_accessed=90 * 10 ** 6, transcendentals=0),
            name='k3_grad',
        )(cnt, idx1, gat1, xon, xof, xqn, xqf, ron, rof, rqn, rqf, w_gate, w_up, w_down)

        y, dx, dwt = pl.pallas_call(
            final_kernel,
            out_shape=[sds((NB, D), F32), sds((NB, D), F32), sds((32, D), F32)],
            in_specs=[sspec()] + [vspec()] * 13,
            out_specs=[vspec()] * 3,
            scratch_shapes=[pltpu.VMEM((S, 32, NB), BF16)],
            compiler_params=pltpu.CompilerParams(vmem_limit_bytes=VMEM_MAX),
            name='k4_final',
        )(pid, tokens, r_proj, ynear, dnear, yrec, drec, dg.reshape(64, HALF), gt, w_router.T, xon, xof, xqn, xqf)
        return y, dx, grad_gate, grad_up, grad_down, dwt.T

    tok_spec = P(axes, None)
    exp_spec = P('ep', None, None)
    return jax.shard_map(local_step, mesh=mesh, in_specs=(tok_spec, P(), exp_spec, exp_spec, exp_spec, tok_spec, tok_spec), out_specs=(tok_spec, tok_spec, exp_spec, exp_spec, exp_spec, P()), check_vma=False)
```

```python
import functools

import jax
import jax.numpy as jnp
from jax import lax
from jax.experimental import pallas as pl
from jax.experimental.pallas import tpu as pltpu
from jax.sharding import PartitionSpec as P

F32 = jnp.float32
BF16 = jnp.bfloat16
MESH = pl.DeviceIdType.MESH
VMEM_MAX = 63 * 1024 * 1024
T = 256
NB = 256
HALF = 1024
D = 1024
FF = 512
NE = 8
NL = 17
SLOTS = 4
PT = 9
S = 8
L = 128
Q = 4
RB = 1032
R1 = 8256
R2 = 16448
X1 = 9288
X2 = 18504
XT = 2304


def dot(a, b, ca=1, cb=0):
    return lax.dot_general(a, b, (((ca,), (cb,)), ((), ())), preferred_element_type=F32)


def vspec():
    return pl.BlockSpec(memory_space=pltpu.VMEM)


def aspec():
    return pl.BlockSpec(memory_space=pl.ANY)


def sspec():
    return pl.BlockSpec(memory_space=pltpu.SMEM)


def barrier_all(dp, ep):
    bar = pltpu.get_barrier_semaphore()
    for k in range(1, S):
        pl.semaphore_signal(bar, inc=1, device_id=((dp + k // Q) % 2, (ep + k % Q) % Q), device_id_type=MESH)
    pl.semaphore_wait(bar, 7)


def gather_kernel(x_ref, r_ref, ids_ref, wr_ref,
                  xon, xof, ron, rof, xqn, rqn, gt_out, idx_out, gat_out, cnt_out,
                  gt_s, pos_s, v_s, ssem, rsem, lsem, gsend, grecv):
    dp = lax.axis_index('dp')
    ep = lax.axis_index('ep')
    c = ep % 2
    xc = ep // 2
    me = dp * Q + ep
    mate = (dp, xc * 2 + 1 - c)
    xnb = (dp, (1 - xc) * 2 + c)
    ynb = (1 - dp, ep)
    barrier_all(dp, ep)

    def rcopy(src, dst, k, dev):
        return pltpu.make_async_remote_copy(src_ref=src, dst_ref=dst, send_sem=ssem.at[k], recv_sem=rsem.at[k], device_id=dev, device_id_type=MESH)

    zt = dot(wr_ref[...], x_ref[...], 1, 1)
    eio = lax.broadcasted_iota(jnp.int32, (32, NB), 0)
    sel = eio == ids_ref[0:1, :]
    for j in range(1, S):
        sel = sel | (eio == ids_ref[j:j + 1, :])
    zm = jnp.max(jnp.where(sel, zt, -jnp.inf), axis=0, keepdims=True)
    pe = jnp.where(sel, jnp.exp(zt - zm), 0.0)
    gt_out[...] = jnp.where(sel, pe / jnp.sum(pe, axis=0, keepdims=True), -1.0)
    gt_s[me] = gt_out[pl.ds(pl.multiple_of(ep * S, S), S), :]
    gcopies = []
    for k in range(1, S):
        dev = ((dp + k // Q) % 2, (ep + k % Q) % Q)
        cp = pltpu.make_async_remote_copy(src_ref=gt_out.at[pl.ds(pl.multiple_of(dev[1] * S, S), S)], dst_ref=gt_s.at[me], send_sem=gsend.at[k - 1], recv_sem=grecv.at[k - 1], device_id=dev, device_id_type=MESH)
        cp.start()
        gcopies.append(cp)
    direct = [
        rcopy(x_ref, xof.at[c], 0, xnb), rcopy(x_ref, xqn.at[c], 1, ynb),
        rcopy(r_ref, rof.at[c], 2, xnb), rcopy(r_ref, rqn.at[c], 3, ynb),
        rcopy(x_ref, xon.at[c], Q, mate), rcopy(r_ref, ron.at[c], 5, mate)]
    for cp in direct:
        cp.start()
    local = [pltpu.make_async_copy(x_ref, xon.at[c], lsem.at[0]), pltpu.make_async_copy(r_ref, ron.at[c], lsem.at[1])]
    for cp in local:
        cp.start()
    for cp in gcopies:
        cp.wait()

    tri = (lax.broadcasted_iota(jnp.int32, (NB, NB), 0) < lax.broadcasted_iota(jnp.int32, (NB, NB), 1)).astype(BF16)
    srow = lax.broadcasted_iota(jnp.int32, (S, NB), 0)
    tlan = lax.broadcasted_iota(jnp.int32, (S, NB), 1).astype(F32)
    for half in range(2):
        base = jnp.zeros((S, 1), F32)
        for k in range(Q):
            hd = dp if half == 0 else 1 - dp
            xx = xc if k < 2 else 1 - xc
            g = gt_s[hd * Q + xx * 2 + k % 2]
            m = g >= 0.0
            mf = m.astype(F32)
            pos = dot(mf.astype(BF16), tri) + base
            pos_s[half * Q + k] = jnp.where(m, pos, -1.0)
            base = base + jnp.sum(mf, axis=1, keepdims=True)
            g = jnp.where(m, g, 0.0)
            g1 = g.astype(BF16)
            e1 = g - g1.astype(F32)
            g2 = e1.astype(BF16)
            g3 = (e1 - g2.astype(F32)).astype(BF16)
            head = jnp.where(srow == 0, tlan, jnp.where(srow == 1, float(k), 0.0))
            v_s[half * Q + k] = jnp.concatenate([head, g1.astype(F32), g2.astype(F32), g3.astype(F32)], axis=0).astype(BF16)
        cnt_out[half] = jnp.broadcast_to(base, (S, L)).astype(jnp.int32)

    pio = lax.broadcasted_iota(jnp.int32, (NB, NB), 0).astype(F32)
    rio = lax.broadcasted_iota(jnp.int32, (32, NB), 0)
    lio = lax.broadcasted_iota(jnp.int32, (1, NB), 1)

    def list_body(he, carry):
        half = he // S
        e = he % S
        cnt_e = cnt_out[half, pl.ds(e, 1), 0:1]
        for pt in range(Q):
            acc = jnp.zeros((32, NB), F32)
            for k in range(pt, Q):
                prow = pos_s[half * Q + k, pl.ds(e, 1), :] - float(256 * pt)
                oh = (pio == prow).astype(F32).astype(BF16)
                acc = acc + dot(v_s[half * Q + k], oh, 1, 1)
            ids = (acc[0:1, :] + 256.0 * acc[1:2, :]).astype(jnp.int32)
            ids = jnp.where(lio + NB * pt < cnt_e, ids, HALF) + half * HALF
            gv = jnp.sum(jnp.where((rio >= S) & (rio % S == e), acc, 0.0), axis=0, keepdims=True)
            for q in range(2):
                idx_out[he, 2 * pt + q:2 * pt + q + 1, :] = ids[:, L * q:L * (q + 1)]
                gat_out[he, 2 * pt + q:2 * pt + q + 1, :] = gv[:, L * q:L * (q + 1)]
        return carry

    lax.fori_loop(0, 2 * S, list_body, 0)
    idx_out[2 * S] = jnp.zeros((S, L), jnp.int32)
    gat_out[2 * S] = jnp.zeros((S, L), F32)

    fwd = [
        rcopy(xof.at[c], xof.at[c], 6, mate), rcopy(xqn.at[c], xqn.at[c], 7, mate),
        rcopy(rof.at[c], rof.at[c], S, mate), rcopy(rqn.at[c], rqn.at[c], 9, mate)]
    for k in range(Q):
        direct[k].wait_recv()
        fwd[k].start()
    for cp in local:
        cp.wait()
    direct[Q].wait_recv()
    direct[5].wait_recv()
    for cp in direct:
        cp.wait_send()
    for cp in fwd:
        cp.wait()


def load_rows(srcs, tmp, sem):
    copies = [pltpu.make_async_copy(src, tmp.at[i % SLOTS], sem.at[i % SLOTS]) for i, (src, _, _) in enumerate(srcs)]
    for i in range(SLOTS):
        copies[i].start()
    for i, (_, dst2, row) in enumerate(srcs):
        copies[i].wait()

        def body(b, carry, i=i, dst2=dst2, row=row):
            r0 = pl.multiple_of(b * 64, 64)
            for s in range(S):
                dst2[pl.ds((row + r0) * PT + s, 64, stride=PT), :] = tmp[i % SLOTS, pl.ds(r0, 64), L * s:L * (s + 1)].astype(F32)
            return carry

        lax.fori_loop(0, NB // 64, body, 0)
        if i + SLOTS < len(srcs):
            copies[i + SLOTS].start()


def load_tokens(pairs, x2, r2, tmp, sem):
    srcs = []
    for i, (xa, ra) in enumerate(pairs):
        for c in range(2):
            srcs.append((xa.at[c], x2, (2 * i + c) * NB))
            srcs.append((ra.at[c], r2, (2 * i + c) * NB))
    load_rows(srcs, tmp, sem)
    for ref in (x2, r2):
        ref[row9(2 * len(pairs) * NB), :] = jnp.zeros((S, L), F32)


def strided(ref2, s):
    return ref2[pl.ds(s, T, stride=PT), :]


def zero_rows(ref2, n):
    def body(i, carry):
        ref2[pl.ds(pl.multiple_of(i * 64, 64), 64), :] = jnp.zeros((64, L), F32)
        return carry
    lax.fori_loop(0, n // 64, body, 0)


def row9(t):
    return pl.ds(t * PT, S)


def row8(t):
    return pl.ds(pl.multiple_of(t * S, S), S)


def own_kernel(cnt, idx, pid, gatv, xn, xf, rn, rf, w1, w3, w2,
               y_out, dx_out, dgt_out,
               x2, r2, ust, rst, us, rs, ds, o2, d2, dgs, dgd, tmp, prev, sem):
    e = pl.program_id(0)

    def gather(base, r0, n):
        for r in range(n):
            t = row9(idx[base + r])
            ust[row9(r0 + r), :] = x2[t, :]
            rst[row9(r0 + r), :] = r2[t, :]

    def scatter(base, r0, n):
        for c in range(0, n, S):
            ts = [idx[base + c + j] for j in range(S)]
            ys = [y_out[row8(ts[j]), :] + o2[row9(r0 + c + j), :] for j in range(S)]
            dl = [dx_out[row8(ts[j]), :] + d2[row9(r0 + c + j), :] for j in range(S)]
            gd = [dgd[pl.ds(ts[j], 1), :] + dgs[pl.ds(r0 + c + j, 1), :] for j in range(S)]
            for j in range(S):
                y_out[row8(ts[j]), :] = ys[j]
                dx_out[row8(ts[j]), :] = dl[j]
                dgd[pl.ds(ts[j], 1), :] = gd[j]

    @pl.when(e == 0)
    def _():
        load_tokens([(xn, rn), (xf, rf)], x2, r2, tmp, sem)
        zero_rows(y_out, R1)
        zero_rows(dx_out, R1)
        zero_rows(o2, XT)
        zero_rows(d2, XT)
        dgd[...] = jnp.zeros_like(dgd)
        dgs[...] = jnp.zeros_like(dgs)
        prev[0] = 0

        def first(c, carry):
            gather(c * S, c * S, S)
            return carry
        lax.fori_loop(0, T // S, first, 0)

    n = cnt[0, e, 0]
    lane = lax.broadcasted_iota(jnp.int32, (T, L), 1)

    def tile_body(k, carry):
        base = k * T
        gcol = jnp.concatenate([jnp.transpose(jnp.broadcast_to(gatv[pl.ds(e * S + 2 * k + q, 1), :], (L, L))) for q in range(2)], axis=0)
        for s in range(S):
            cs = slice(L * s, L * (s + 1))
            us[:, cs] = strided(ust, s).astype(BF16)
            rv = strided(rst, s)
            rs[:, cs] = rv.astype(BF16)
            ds[:, cs] = (rv * gcol).astype(BF16)
        more = base + T < n
        gather(jnp.where(more, e * HALF + base + T, jnp.minimum(e + 1, NE - 1) * HALF), 0, T)
        scatter(prev[0], 0, T)
        u = us[...]
        h1 = dot(u, w1[0])
        h3 = dot(u, w3[0])
        sg = jax.nn.sigmoid(h1)
        sl = h1 * sg
        a = (sl * h3).astype(BF16)
        da = dot(ds[...], w2[0], 1, 1)
        o = dot(a, w2[0]).astype(BF16).astype(F32)
        dh1 = (da * h3 * sg * (1.0 + h1 * (1.0 - sg))).astype(BF16)
        dh3 = (da * sl).astype(BF16)
        dr = (dot(dh1, w1[0], 1, 1) + dot(dh3, w3[0], 1, 1)).astype(BF16).astype(F32)
        acc = jnp.zeros((T, L), F32)
        for s in range(S):
            cs = slice(L * s, L * (s + 1))
            o2[pl.ds(s, T, stride=PT), :] = o[:, cs] * gcol
            d2[pl.ds(s, T, stride=PT), :] = dr[:, cs]
            acc = acc + o[:, cs] * rs[:, cs].astype(F32)
        dgc = jnp.sum(acc, axis=1, keepdims=True)
        dgs[...] = jnp.where(lane == e, dgc, 0.0)
        prev[0] = e * HALF + base
        return carry

    lax.fori_loop(0, jnp.maximum((n + T - 1) // T, 1), tile_body, 0)

    @pl.when(e == NE - 1)
    def _():
        def last(c, carry):
            scatter(prev[0] + c * S, c * S, S)
            return carry
        lax.fori_loop(0, T // S, last, 0)
        xc = pid[1] // 2
        tr = jnp.transpose(dgd[0:HALF, :])
        dgt_out[:, pl.ds(pl.multiple_of(xc * FF, FF), FF)] = tr[0:S, 0:FF]
        dgt_out[:, pl.ds(pl.multiple_of(FF - xc * FF, FF), FF)] = tr[0:S, FF:HALF]


def pair_kernel(yp, dxp, dgt, gt, ynear, yfar, dnear, dfar, dg_out, gt_out, rbuf, obuf, dgb, gtb, ssem, rsem, lsem, gsend, grecv):
    dp = lax.axis_index('dp')
    ep = lax.axis_index('ep')
    c = ep % 2
    me = dp * Q + ep
    mate = (dp, (ep // 2) * 2 + 1 - c)
    barrier_all(dp, ep)
    parts = [(yp, 4096), (dxp, 4096), (yp, 0), (dxp, 0)]
    outs = [yfar, dfar, ynear, dnear]
    sends, loads = [], []
    for i, (src, base) in enumerate(parts):
        cp = pltpu.make_async_remote_copy(
            src_ref=src.at[pl.ds(pl.multiple_of(base + (1 - c) * 2048, 2048), 2048)], dst_ref=rbuf.at[i],
            send_sem=ssem.at[i], recv_sem=rsem.at[i], device_id=mate, device_id_type=MESH)
        cp.start()
        sends.append(cp)
        ld = pltpu.make_async_copy(src.at[pl.ds(pl.multiple_of(base + c * 2048, 2048), 2048)], obuf.at[i], lsem.at[i])
        ld.start()
        loads.append(ld)
    gcopies = []
    for k in range(1, S):
        dev = ((dp + k // Q) % 2, (ep + k % Q) % Q)
        for q, (src, dst) in enumerate(((dgt, dgb), (gt, gtb))):
            cp = pltpu.make_async_remote_copy(src_ref=src, dst_ref=dst.at[me], send_sem=gsend.at[q, k - 1], recv_sem=grecv.at[q, k - 1], device_id=dev, device_id_type=MESH)
            cp.start()
            gcopies.append(cp)
    for i in range(Q):
        loads[i].wait()
        sends[i].wait_recv()

        def body(b, carry, i=i):
            s = pl.ds(pl.multiple_of(b * L, L), L)
            outs[i][s, :] = obuf[i, s, :] + rbuf[i, s, :]
            return carry

        lax.fori_loop(0, 16, body, 0)
    for cp in gcopies:
        cp.wait()
    for cp in sends:
        cp.wait_send()
    dgb[me] = dgt[...]
    dg_out[...] = dgb[...]
    gtb[me] = gt[...]
    gt_out[...] = gtb[...]


def grad_kernel(cnt, idx, gat, xon, xof, xqn, xqf, ron, rof, rqn, rqf, w1, w3, w2,
                g1, g3, g2, x2, r2, ust, dst, us, ds, tmp, sem):
    e = pl.program_id(0)

    def gather(ne, nb, r0, n):
        n0 = cnt[0, ne, 0]
        a0 = ne * HALF
        a1 = NE * HALF + a0 - n0
        for r in range(n):
            q = nb + r
            q = q + jnp.where(q < n0, a0, a1)
            t = row9(idx[q])
            ust[row9(r0 + r), :] = x2[t, :]
            dst[row9(r0 + r), :] = r2[t, :] * gat[q]

    @pl.when(e == 0)
    def _():
        load_tokens([(xon, ron), (xof, rof), (xqn, rqn), (xqf, rqf)], x2, r2, tmp, sem)

        def first(c, carry):
            gather(0, c * S, c * S, S)
            return carry
        lax.fori_loop(0, T // S, first, 0)

    n = cnt[0, e, 0] + cnt[1, e, 0]
    rown = lax.broadcasted_iota(jnp.int32, (T, L), 0)

    def tile(k, first):
        base = k * T
        live = rown + base < n
        for s in range(S):
            cs = slice(L * s, L * (s + 1))
            us[:, cs] = strided(ust, s).astype(BF16)
            ds[:, cs] = jnp.where(live, strided(dst, s), 0.0).astype(BF16)
        more = base + T < n
        gather(jnp.where(more, e, jnp.minimum(e + 1, NE - 1)), jnp.where(more, base + T, 0), 0, T)
        u = us[...]
        do = ds[...]
        h1 = dot(u, w1[0])
        h3 = dot(u, w3[0])
        sg = jax.nn.sigmoid(h1)
        sl = h1 * sg
        a = (sl * h3).astype(BF16)
        da = dot(do, w2[0], 1, 1)
        dh1 = (da * h3 * sg * (1.0 + h1 * (1.0 - sg))).astype(BF16)
        dh3 = (da * sl).astype(BF16)
        if first:
            g2[0] = dot(a, do, 0, 0)
            g1[0] = dot(u, dh1, 0, 0)
            g3[0] = dot(u, dh3, 0, 0)
        else:
            g2[0] += dot(a, do, 0, 0)
            g1[0] += dot(u, dh1, 0, 0)
            g3[0] += dot(u, dh3, 0, 0)

    tile(0, True)

    def tile_body(k, carry):
        tile(k, False)
        return carry

    lax.fori_loop(1, (n + T - 1) // T, tile_body, 0)


def final_kernel(pid, x, r, ynear, dnear, yrec, drec, dg, gt, wr, xon, xof, xqn, xqf,
                 y_out, dx_out, dw_out, dz_s):
    dp = pid[0]
    ep = pid[1]
    xc = ep // 2
    for b in range(S):
        gm = jnp.maximum(gt[b], 0.0)
        dgv = dg[32 * (b // Q):32 * (b // Q + 1), NB * (b % Q):NB * (b % Q + 1)]
        s = jnp.sum(gm * dgv, axis=0, keepdims=True)
        dz_s[b] = (gm * (dgv - s)).astype(BF16)
    acc = jnp.zeros((32, D), F32)
    for h, arrs in enumerate(((xon, xof), (xqn, xqf))):
        hd = dp if h == 0 else 1 - dp
        for f, arr in enumerate(arrs):
            xx = xc if f == 0 else 1 - xc
            for c in range(2):
                acc = acc + dot(dz_s[hd * Q + xx * 2 + c], arr[c])
    dw_out[...] = acc
    dxr = dot(dz_s[dp * Q + ep], wr[...], 0, 0)
    for s in range(S):
        cs = slice(L * s, L * (s + 1))
        rows = pl.ds(s, NB, stride=S)
        y_out[:, cs] = x[:, cs].astype(F32) + (ynear[rows, :] + yrec[rows, :])
        dx_out[:, cs] = r[:, cs].astype(F32) + dxr[:, cs] + (dnear[rows, :] + drec[rows, :])


def solution(mesh):
    axes = ('dp', 'ep')
    sds = jax.ShapeDtypeStruct

    def local_step(tokens, w_router, w_gate, w_up, w_down, top_ids, r_proj):
        pid = jnp.stack([lax.axis_index('dp'), lax.axis_index('ep')]).astype(jnp.int32)
        near = sds((2, NB, D), BF16)
        dma = pltpu.SemaphoreType.DMA
        xon, xof, ron, rof, xqn, rqn, gto, idx, gat, cnt = pl.pallas_call(
            gather_kernel,
            out_shape=[near] * 6 + [sds((32, NB), F32), sds((NL, S, L), jnp.int32), sds((NL, S, L), F32), sds((2, S, L), jnp.int32)],
            in_specs=[vspec()] * Q,
            out_specs=[aspec()] * 6 + [vspec()] * Q,
            scratch_shapes=[pltpu.VMEM((S, S, NB), F32), pltpu.VMEM((S, S, NB), F32), pltpu.VMEM((S, 32, NB), BF16),
                            dma((10,)), dma((10,)), dma((2,)), dma((7,)), dma((7,))],
            compiler_params=pltpu.CompilerParams(collective_id=0, has_side_effects=True),
            name='k0_gather',
        )(tokens, r_proj, top_ids.T, w_router.T)

        idx1 = idx.reshape(-1)
        gat1 = gat.reshape(-1)
        xswap = [(0, 2), (2, 0), (1, 3), (3, 1)]
        xqf = lax.ppermute(xqn, 'ep', xswap)
        rqf = lax.ppermute(rof, 'dp', [(0, 1), (1, 0)])

        wspec = [pl.BlockSpec((1, D, FF), lambda e: (e, 0, 0)), pl.BlockSpec((1, D, FF), lambda e: (e, 0, 0)), pl.BlockSpec((1, FF, D), lambda e: (e, 0, 0))]
        part = sds((R1, L), F32)
        pspec = pl.BlockSpec((R1, L), lambda e: (0, 0))
        yp, dxp, dgt = pl.pallas_call(
            own_kernel,
            grid=(NE,),
            out_shape=[part, part, sds((S, HALF), F32)],
            in_specs=[sspec()] * 3 + [vspec()] + [aspec()] * Q + wspec,
            out_specs=[pspec, pspec, pl.BlockSpec((S, HALF), lambda e: (0, 0))],
            scratch_shapes=[pltpu.VMEM((X1, L), F32)] * 2 + [pltpu.VMEM((XT, L), F32)] * 2 + [pltpu.VMEM((T, D), BF16)] * 3
            + [pltpu.VMEM((XT, L), F32)] * 2 + [pltpu.VMEM((T, L), F32), pltpu.VMEM((RB, L), F32),
               pltpu.VMEM((SLOTS, NB, D), BF16), pltpu.SMEM((1,), jnp.int32), dma((SLOTS,))],
            compiler_params=pltpu.CompilerParams(vmem_limit_bytes=VMEM_MAX, dimension_semantics=('arbitrary',)),
            cost_estimate=pl.CostEstimate(flops=20 * 10 ** 9, bytes_accessed=40 * 10 ** 6, transcendentals=0),
            name='k1_own',
        )(cnt, idx1, pid, gat.reshape(NL * S, L), xon, xof, ron, rof, w_gate, w_up, w_down)

        quarter = sds((NB * S, L), F32)
        ynear, yfar, dnear, dfar, dg, gt = pl.pallas_call(
            pair_kernel,
            out_shape=[quarter] * Q + [sds((S, S, HALF), F32), sds((S, 32, NB), F32)],
            in_specs=[aspec(), aspec(), vspec(), vspec()],
            out_specs=[vspec()] * 6,
            scratch_shapes=[pltpu.VMEM((Q, NB * S, L), F32), pltpu.VMEM((Q, NB * S, L), F32), pltpu.VMEM((S, S, HALF), F32), pltpu.VMEM((S, 32, NB), F32),
                            dma((Q,)), dma((Q,)), dma((Q,)), dma((2, 7)), dma((2, 7))],
            compiler_params=pltpu.CompilerParams(collective_id=1, has_side_effects=True),
            name='k2_pair',
        )(yp, dxp, dgt, gto)

        yrec = lax.ppermute(yfar, 'ep', xswap)
        drec = lax.ppermute(dfar, 'ep', xswap)

        gspec = [pl.BlockSpec((1, D, FF), lambda e: (e, 0, 0)), pl.BlockSpec((1, D, FF), lambda e: (e, 0, 0)), pl.BlockSpec((1, FF, D), lambda e: (e, 0, 0))]
        grad_gate, grad_up, grad_down = pl.pallas_call(
            grad_kernel,
            grid=(NE,),
            out_shape=[sds((NE, D, FF), F32), sds((NE, D, FF), F32), sds((NE, FF, D), F32)],
            in_specs=[sspec()] * 3 + [aspec()] * S + wspec,
            out_specs=gspec,
            scratch_shapes=[pltpu.VMEM((X2, L), F32)] * 2 + [pltpu.VMEM((XT, L), F32)] * 2 + [pltpu.VMEM((T, D), BF16)] * 2
            + [pltpu.VMEM((SLOTS, NB, D), BF16), dma((SLOTS,))],
            compiler_params=pltpu.CompilerParams(vmem_limit_bytes=VMEM_MAX, dimension_semantics=('arbitrary',)),
            cost_estimate=pl.CostEstimate(flops=30 * 10 ** 9, bytes_accessed=90 * 10 ** 6, transcendentals=0),
            name='k3_grad',
        )(cnt, idx1, gat1, xon, xof, xqn, xqf, ron, rof, rqn, rqf, w_gate, w_up, w_down)

        y, dx, dwt = pl.pallas_call(
            final_kernel,
            out_shape=[sds((NB, D), F32), sds((NB, D), F32), sds((32, D), F32)],
            in_specs=[sspec()] + [vspec()] * 13,
            out_specs=[vspec()] * 3,
            scratch_shapes=[pltpu.VMEM((S, 32, NB), BF16)],
            compiler_params=pltpu.CompilerParams(vmem_limit_bytes=VMEM_MAX),
            name='k4_final',
        )(pid, tokens, r_proj, ynear, dnear, yrec, drec, dg.reshape(64, HALF), gt, w_router.T, xon, xof, xqn, xqf)
        return y, dx, grad_gate, grad_up, grad_down, dwt.T

    tok_spec = P(axes, None)
    exp_spec = P('ep', None, None)
    return jax.shard_map(local_step, mesh=mesh, in_specs=(tok_spec, P(), exp_spec, exp_spec, exp_spec, tok_spec, tok_spec), out_specs=(tok_spec, tok_spec, exp_spec, exp_spec, exp_spec, P()), check_vma=False)
```

```python
import functools

import jax
import jax.numpy as jnp
from jax import lax
from jax.experimental import pallas as pl
from jax.experimental.pallas import tpu as pltpu
from jax.sharding import PartitionSpec as P

F32 = jnp.float32
BF16 = jnp.bfloat16
MESH = pl.DeviceIdType.MESH
VMEM_MAX = 63 * 1024 * 1024
T = 256
NB = 256
HALF = 1024
D = 1024
FF = 512
NE = 8
NL = 17
SLOTS = 4
PT = 9
S = 8
L = 128
Q = 4
RB = 1032
R1 = 8256
R2 = 16448
X1 = 9288
X2 = 18504
XT = 2304


def dot(a, b, ca=1, cb=0):
    return lax.dot_general(a, b, (((ca,), (cb,)), ((), ())), preferred_element_type=F32)


def vspec():
    return pl.BlockSpec(memory_space=pltpu.VMEM)


def aspec():
    return pl.BlockSpec(memory_space=pl.ANY)


def sspec():
    return pl.BlockSpec(memory_space=pltpu.SMEM)


def barrier_all(dp, ep):
    bar = pltpu.get_barrier_semaphore()
    for k in range(1, S):
        pl.semaphore_signal(bar, inc=1, device_id=((dp + k // Q) % 2, (ep + k % Q) % Q), device_id_type=MESH)
    pl.semaphore_wait(bar, 7)


def gather_kernel(x_ref, r_ref, ids_ref, wr_ref, w1, w3, w2,
                  xon, xof, ron, rof, xqn, rqn, w1t, w3t, w2t, gt_out, idx_out, gat_out, cnt_out,
                  gt_s, pos_s, v_s, wide, tall, wide_t, tall_t, ssem, rsem, lsem, gsend, grecv, wsem, osem):
    dp = lax.axis_index('dp')
    ep = lax.axis_index('ep')
    c = ep % 2
    xc = ep // 2
    me = dp * Q + ep
    mate = (dp, xc * 2 + 1 - c)
    xnb = (dp, (1 - xc) * 2 + c)
    ynb = (1 - dp, ep)

    def wload(e):
        b = e % 2
        return [pltpu.make_async_copy(src.at[e], dst, wsem.at[b, i]) for i, (src, dst) in enumerate(((w1, tall.at[b, 0]), (w3, tall.at[b, 1]), (w2, wide.at[b])))]

    def wstore(e):
        b = e % 2
        return [pltpu.make_async_copy(src, dst.at[e], osem.at[b, i]) for i, (dst, src) in enumerate(((w1t, wide_t.at[b, 0]), (w3t, wide_t.at[b, 1]), (w2t, tall_t.at[b])))]

    for cp in wload(0):
        cp.start()
    barrier_all(dp, ep)

    def rcopy(src, dst, k, dev):
        return pltpu.make_async_remote_copy(src_ref=src, dst_ref=dst, send_sem=ssem.at[k], recv_sem=rsem.at[k], device_id=dev, device_id_type=MESH)

    zt = dot(wr_ref[...], x_ref[...], 1, 1)
    eio = lax.broadcasted_iota(jnp.int32, (32, NB), 0)
    sel = eio == ids_ref[0:1, :]
    for j in range(1, S):
        sel = sel | (eio == ids_ref[j:j + 1, :])
    zm = jnp.max(jnp.where(sel, zt, -jnp.inf), axis=0, keepdims=True)
    pe = jnp.where(sel, jnp.exp(zt - zm), 0.0)
    gt_out[...] = jnp.where(sel, pe / jnp.sum(pe, axis=0, keepdims=True), -1.0)
    gt_s[me] = gt_out[pl.ds(pl.multiple_of(ep * S, S), S), :]
    gcopies = []
    for k in range(1, S):
        dev = ((dp + k // Q) % 2, (ep + k % Q) % Q)
        cp = pltpu.make_async_remote_copy(src_ref=gt_out.at[pl.ds(pl.multiple_of(dev[1] * S, S), S)], dst_ref=gt_s.at[me], send_sem=gsend.at[k - 1], recv_sem=grecv.at[k - 1], device_id=dev, device_id_type=MESH)
        cp.start()
        gcopies.append(cp)
    direct = [
        rcopy(x_ref, xof.at[c], 0, xnb), rcopy(x_ref, xqn.at[c], 1, ynb),
        rcopy(r_ref, rof.at[c], 2, xnb), rcopy(r_ref, rqn.at[c], 3, ynb),
        rcopy(x_ref, xon.at[c], Q, mate), rcopy(r_ref, ron.at[c], 5, mate)]
    for cp in direct:
        cp.start()
    local = [pltpu.make_async_copy(x_ref, xon.at[c], lsem.at[0]), pltpu.make_async_copy(r_ref, ron.at[c], lsem.at[1])]
    for cp in local:
        cp.start()
    for cp in gcopies:
        cp.wait()

    tri = (lax.broadcasted_iota(jnp.int32, (NB, NB), 0) < lax.broadcasted_iota(jnp.int32, (NB, NB), 1)).astype(BF16)
    srow = lax.broadcasted_iota(jnp.int32, (S, NB), 0)
    tlan = lax.broadcasted_iota(jnp.int32, (S, NB), 1).astype(F32)
    for half in range(2):
        base = jnp.zeros((S, 1), F32)
        for k in range(Q):
            hd = dp if half == 0 else 1 - dp
            xx = xc if k < 2 else 1 - xc
            g = gt_s[hd * Q + xx * 2 + k % 2]
            m = g >= 0.0
            mf = m.astype(F32)
            pos = dot(mf.astype(BF16), tri) + base
            pos_s[half * Q + k] = jnp.where(m, pos, -1.0)
            base = base + jnp.sum(mf, axis=1, keepdims=True)
            g = jnp.where(m, g, 0.0)
            g1 = g.astype(BF16)
            e1 = g - g1.astype(F32)
            g2 = e1.astype(BF16)
            g3 = (e1 - g2.astype(F32)).astype(BF16)
            head = jnp.where(srow == 0, tlan, jnp.where(srow == 1, float(k), 0.0))
            v_s[half * Q + k] = jnp.concatenate([head, g1.astype(F32), g2.astype(F32), g3.astype(F32)], axis=0).astype(BF16)
        cnt_out[half] = jnp.broadcast_to(base, (S, L)).astype(jnp.int32)

    pio = lax.broadcasted_iota(jnp.int32, (NB, NB), 0).astype(F32)
    rio = lax.broadcasted_iota(jnp.int32, (32, NB), 0)
    lio = lax.broadcasted_iota(jnp.int32, (1, NB), 1)

    def list_body(he, carry):
        half = he // S
        e = he % S
        cnt_e = cnt_out[half, pl.ds(e, 1), 0:1]
        for pt in range(Q):
            acc = jnp.zeros((32, NB), F32)
            for k in range(pt, Q):
                prow = pos_s[half * Q + k, pl.ds(e, 1), :] - float(256 * pt)
                oh = (pio == prow).astype(F32).astype(BF16)
                acc = acc + dot(v_s[half * Q + k], oh, 1, 1)
            ids = (acc[0:1, :] + 256.0 * acc[1:2, :]).astype(jnp.int32)
            ids = jnp.where(lio + NB * pt < cnt_e, ids, HALF) + half * HALF
            gv = jnp.sum(jnp.where((rio >= S) & (rio % S == e), acc, 0.0), axis=0, keepdims=True)
            for q in range(2):
                idx_out[he, 2 * pt + q:2 * pt + q + 1, :] = ids[:, L * q:L * (q + 1)]
                gat_out[he, 2 * pt + q:2 * pt + q + 1, :] = gv[:, L * q:L * (q + 1)]
        return carry

    lax.fori_loop(0, 2 * S, list_body, 0)
    idx_out[2 * S] = jnp.zeros((S, L), jnp.int32)
    gat_out[2 * S] = jnp.zeros((S, L), F32)

    def wbody(e, carry):
        b = e % 2

        @pl.when(e + 1 < NE)
        def _():
            for cp in wload(e + 1):
                cp.start()

        for cp in wload(e):
            cp.wait()

        @pl.when(e >= 2)
        def _():
            for cp in wstore(e - 2):
                cp.wait()

        for i in range(2):
            for q in range(Q):
                wide_t[b, i, :, NB * q:NB * (q + 1)] = jnp.transpose(tall[b, i, NB * q:NB * (q + 1), :])
        for q in range(Q):
            tall_t[b, NB * q:NB * (q + 1), :] = jnp.transpose(wide[b, :, NB * q:NB * (q + 1)])
        for cp in wstore(e):
            cp.start()
        return carry

    lax.fori_loop(0, NE, wbody, 0)
    fwd = [
        rcopy(xof.at[c], xof.at[c], 6, mate), rcopy(xqn.at[c], xqn.at[c], 7, mate),
        rcopy(rof.at[c], rof.at[c], S, mate), rcopy(rqn.at[c], rqn.at[c], 9, mate)]
    for k in range(Q):
        direct[k].wait_recv()
        fwd[k].start()
    for e in (NE - 2, NE - 1):
        for cp in wstore(e):
            cp.wait()
    for cp in local:
        cp.wait()
    direct[Q].wait_recv()
    direct[5].wait_recv()
    for cp in direct:
        cp.wait_send()
    for cp in fwd:
        cp.wait()


def load_rows(srcs, tmp, sem):
    copies = [pltpu.make_async_copy(src, tmp.at[i % SLOTS], sem.at[i % SLOTS]) for i, (src, _, _) in enumerate(srcs)]
    for i in range(SLOTS):
        copies[i].start()
    for i, (_, dst2, row) in enumerate(srcs):
        copies[i].wait()

        def body(b, carry, i=i, dst2=dst2, row=row):
            r0 = pl.multiple_of(b * 64, 64)
            for s in range(S):
                dst2[pl.ds((row + r0) * PT + s, 64, stride=PT), :] = tmp[i % SLOTS, pl.ds(r0, 64), L * s:L * (s + 1)].astype(F32)
            return carry

        lax.fori_loop(0, NB // 64, body, 0)
        if i + SLOTS < len(srcs):
            copies[i + SLOTS].start()


def load_tokens(pairs, x2, r2, tmp, sem):
    srcs = []
    for i, (xa, ra) in enumerate(pairs):
        for c in range(2):
            srcs.append((xa.at[c], x2, (2 * i + c) * NB))
            srcs.append((ra.at[c], r2, (2 * i + c) * NB))
    load_rows(srcs, tmp, sem)
    for ref in (x2, r2):
        ref[row9(2 * len(pairs) * NB), :] = jnp.zeros((S, L), F32)


def strided(ref2, s):
    return ref2[pl.ds(s, T, stride=PT), :]


def zero_rows(ref2, n):
    def body(i, carry):
        ref2[pl.ds(pl.multiple_of(i * 64, 64), 64), :] = jnp.zeros((64, L), F32)
        return carry
    lax.fori_loop(0, n // 64, body, 0)


def row9(t):
    return pl.ds(t * PT, S)


def row8(t):
    return pl.ds(pl.multiple_of(t * S, S), S)


def own_kernel(cnt, idx, pid, gatv, xn, xf, rn, rf, w1, w3, w2, w1t, w3t, w2t,
               y_out, dx_out, dgt_out,
               x2, r2, ust, rst, us, rs, ds, o2, d2, dgs, dgd, gcs, tmp, prev, sem):
    e = pl.program_id(0)

    def gate_column(base):
        for q in range(2):
            gcs[L * q:L * (q + 1), :] = jnp.transpose(jnp.broadcast_to(gatv[pl.ds(base // L + q, 1), :], (L, L)))

    def gather(base, r0, n):
        for r in range(n):
            t = row9(idx[base + r])
            ust[row9(r0 + r), :] = x2[t, :]
            rst[row9(r0 + r), :] = r2[t, :]

    def scatter(base, r0, n):
        for c in range(0, n, S):
            ts = [idx[base + c + j] for j in range(S)]
            ys = [y_out[row8(ts[j]), :] + o2[row9(r0 + c + j), :] for j in range(S)]
            dl = [dx_out[row8(ts[j]), :] + d2[row9(r0 + c + j), :] for j in range(S)]
            gd = [dgd[pl.ds(ts[j], 1), :] + dgs[pl.ds(r0 + c + j, 1), :] for j in range(S)]
            for j in range(S):
                y_out[row8(ts[j]), :] = ys[j]
                dx_out[row8(ts[j]), :] = dl[j]
                dgd[pl.ds(ts[j], 1), :] = gd[j]

    @pl.when(e == 0)
    def _():
        load_tokens([(xn, rn), (xf, rf)], x2, r2, tmp, sem)
        zero_rows(y_out, R1)
        zero_rows(dx_out, R1)
        zero_rows(o2, XT)
        zero_rows(d2, XT)
        dgd[...] = jnp.zeros_like(dgd)
        dgs[...] = jnp.zeros_like(dgs)
        prev[0] = 0
        gate_column(0)

        def first(c, carry):
            gather(c * S, c * S, S)
            return carry
        lax.fori_loop(0, T // S, first, 0)

    n = cnt[0, e, 0]
    lane = lax.broadcasted_iota(jnp.int32, (T, L), 1)

    def tile_body(k, carry):
        base = k * T
        gcol = gcs[...]
        for s in range(S):
            cs = slice(L * s, L * (s + 1))
            us[:, cs] = strided(ust, s).astype(BF16)
            rv = strided(rst, s)
            rs[:, cs] = rv.astype(BF16)
            ds[:, cs] = (rv * gcol).astype(BF16)
        more = base + T < n
        nxt = jnp.where(more, e * HALF + base + T, jnp.minimum(e + 1, NE - 1) * HALF)
        gather(nxt, 0, T)
        scatter(prev[0], 0, T)
        u = us[...]
        h1 = dot(u, w1[0])
        h3 = dot(u, w3[0])
        sg = jax.nn.sigmoid(h1)
        sl = h1 * sg
        a = (sl * h3).astype(BF16)
        da = dot(ds[...], w2t[0])
        o = dot(a, w2[0]).astype(BF16).astype(F32)
        dh1 = (da * h3 * sg * (1.0 + h1 * (1.0 - sg))).astype(BF16)
        dh3 = (da * sl).astype(BF16)
        dr = (dot(dh1, w1t[0]) + dot(dh3, w3t[0])).astype(BF16).astype(F32)
        acc = jnp.zeros((T, L), F32)
        for s in range(S):
            cs = slice(L * s, L * (s + 1))
            o2[pl.ds(s, T, stride=PT), :] = o[:, cs] * gcol
            d2[pl.ds(s, T, stride=PT), :] = dr[:, cs]
            acc = acc + o[:, cs] * rs[:, cs].astype(F32)
        dgc = jnp.sum(acc, axis=1, keepdims=True)
        dgs[...] = jnp.where(lane == e, dgc, 0.0)
        prev[0] = e * HALF + base
        gate_column(nxt)
        return carry

    lax.fori_loop(0, jnp.maximum((n + T - 1) // T, 1), tile_body, 0)

    @pl.when(e == NE - 1)
    def _():
        def last(c, carry):
            scatter(prev[0] + c * S, c * S, S)
            return carry
        lax.fori_loop(0, T // S, last, 0)
        xc = pid[1] // 2
        tr = jnp.transpose(dgd[0:HALF, :])
        dgt_out[:, pl.ds(pl.multiple_of(xc * FF, FF), FF)] = tr[0:S, 0:FF]
        dgt_out[:, pl.ds(pl.multiple_of(FF - xc * FF, FF), FF)] = tr[0:S, FF:HALF]


def pair_kernel(yp, dxp, dgt, gt, ynear, yfar, dnear, dfar, dg_out, gt_out, rbuf, obuf, dgb, gtb, ssem, rsem, lsem, gsend, grecv):
    dp = lax.axis_index('dp')
    ep = lax.axis_index('ep')
    c = ep % 2
    me = dp * Q + ep
    mate = (dp, (ep // 2) * 2 + 1 - c)
    barrier_all(dp, ep)
    parts = [(yp, 4096), (dxp, 4096), (yp, 0), (dxp, 0)]
    outs = [yfar, dfar, ynear, dnear]
    sends, loads = [], []
    for i, (src, base) in enumerate(parts):
        cp = pltpu.make_async_remote_copy(
            src_ref=src.at[pl.ds(pl.multiple_of(base + (1 - c) * 2048, 2048), 2048)], dst_ref=rbuf.at[i],
            send_sem=ssem.at[i], recv_sem=rsem.at[i], device_id=mate, device_id_type=MESH)
        cp.start()
        sends.append(cp)
        ld = pltpu.make_async_copy(src.at[pl.ds(pl.multiple_of(base + c * 2048, 2048), 2048)], obuf.at[i], lsem.at[i])
        ld.start()
        loads.append(ld)
    gcopies = []
    for k in range(1, S):
        dev = ((dp + k // Q) % 2, (ep + k % Q) % Q)
        for q, (src, dst) in enumerate(((dgt, dgb), (gt, gtb))):
            cp = pltpu.make_async_remote_copy(src_ref=src, dst_ref=dst.at[me], send_sem=gsend.at[q, k - 1], recv_sem=grecv.at[q, k - 1], device_id=dev, device_id_type=MESH)
            cp.start()
            gcopies.append(cp)
    for i in range(Q):
        loads[i].wait()
        sends[i].wait_recv()

        def body(b, carry, i=i):
            s = pl.ds(pl.multiple_of(b * L, L), L)
            outs[i][s, :] = obuf[i, s, :] + rbuf[i, s, :]
            return carry

        lax.fori_loop(0, 16, body, 0)
    for cp in gcopies:
        cp.wait()
    for cp in sends:
        cp.wait_send()
    dgb[me] = dgt[...]
    dg_out[...] = dgb[...]
    gtb[me] = gt[...]
    gt_out[...] = gtb[...]


def grad_kernel(cnt, idx, gat, xon, xof, xqn, xqf, ron, rof, rqn, rqf, w1, w3, w2t,
                g1, g3, g2, x2, r2, ust, dst, us, ds, tmp, sem):
    e = pl.program_id(0)

    def gather(ne, nb, r0, n):
        n0 = cnt[0, ne, 0]
        a0 = ne * HALF
        a1 = NE * HALF + a0 - n0
        for r in range(n):
            q = nb + r
            q = q + jnp.where(q < n0, a0, a1)
            t = row9(idx[q])
            ust[row9(r0 + r), :] = x2[t, :]
            dst[row9(r0 + r), :] = r2[t, :] * gat[q]

    @pl.when(e == 0)
    def _():
        load_tokens([(xon, ron), (xof, rof), (xqn, rqn), (xqf, rqf)], x2, r2, tmp, sem)

        def first(c, carry):
            gather(0, c * S, c * S, S)
            return carry
        lax.fori_loop(0, T // S, first, 0)

    n = cnt[0, e, 0] + cnt[1, e, 0]
    rown = lax.broadcasted_iota(jnp.int32, (T, L), 0)

    def tile(k, first):
        base = k * T
        live = rown + base < n
        for s in range(S):
            cs = slice(L * s, L * (s + 1))
            us[:, cs] = strided(ust, s).astype(BF16)
            ds[:, cs] = jnp.where(live, strided(dst, s), 0.0).astype(BF16)
        more = base + T < n
        gather(jnp.where(more, e, jnp.minimum(e + 1, NE - 1)), jnp.where(more, base + T, 0), 0, T)
        u = us[...]
        do = ds[...]
        h1 = dot(u, w1[0])
        h3 = dot(u, w3[0])
        sg = jax.nn.sigmoid(h1)
        sl = h1 * sg
        a = (sl * h3).astype(BF16)
        da = dot(do, w2t[0])
        dh1 = (da * h3 * sg * (1.0 + h1 * (1.0 - sg))).astype(BF16)
        dh3 = (da * sl).astype(BF16)
        if first:
            g2[0] = dot(a, do, 0, 0)
            g1[0] = dot(u, dh1, 0, 0)
            g3[0] = dot(u, dh3, 0, 0)
        else:
            g2[0] += dot(a, do, 0, 0)
            g1[0] += dot(u, dh1, 0, 0)
            g3[0] += dot(u, dh3, 0, 0)

    tile(0, True)

    def tile_body(k, carry):
        tile(k, False)
        return carry

    lax.fori_loop(1, (n + T - 1) // T, tile_body, 0)


def final_kernel(pid, x, r, ynear, dnear, yrec, drec, dg, gt, wr, xon, xof, xqn, xqf,
                 y_out, dx_out, dw_out, dz_s):
    dp = pid[0]
    ep = pid[1]
    xc = ep // 2
    for b in range(S):
        gm = jnp.maximum(gt[b], 0.0)
        dgv = dg[32 * (b // Q):32 * (b // Q + 1), NB * (b % Q):NB * (b % Q + 1)]
        s = jnp.sum(gm * dgv, axis=0, keepdims=True)
        dz_s[b] = (gm * (dgv - s)).astype(BF16)
    acc = jnp.zeros((32, D), F32)
    for h, arrs in enumerate(((xon, xof), (xqn, xqf))):
        hd = dp if h == 0 else 1 - dp
        for f, arr in enumerate(arrs):
            xx = xc if f == 0 else 1 - xc
            for c in range(2):
                acc = acc + dot(dz_s[hd * Q + xx * 2 + c], arr[c])
    dw_out[...] = acc
    dxr = dot(dz_s[dp * Q + ep], wr[...], 0, 0)
    for s in range(S):
        cs = slice(L * s, L * (s + 1))
        rows = pl.ds(s, NB, stride=S)
        y_out[:, cs] = x[:, cs].astype(F32) + (ynear[rows, :] + yrec[rows, :])
        dx_out[:, cs] = r[:, cs].astype(F32) + dxr[:, cs] + (dnear[rows, :] + drec[rows, :])


def solution(mesh):
    axes = ('dp', 'ep')
    sds = jax.ShapeDtypeStruct

    def local_step(tokens, w_router, w_gate, w_up, w_down, top_ids, r_proj):
        pid = jnp.stack([lax.axis_index('dp'), lax.axis_index('ep')]).astype(jnp.int32)
        near = sds((2, NB, D), BF16)
        dma = pltpu.SemaphoreType.DMA
        xon, xof, ron, rof, xqn, rqn, w1t, w3t, w2t, gto, idx, gat, cnt = pl.pallas_call(
            gather_kernel,
            out_shape=[near] * 6 + [sds((NE, FF, D), BF16), sds((NE, FF, D), BF16), sds((NE, D, FF), BF16), sds((32, NB), F32), sds((NL, S, L), jnp.int32), sds((NL, S, L), F32), sds((2, S, L), jnp.int32)],
            in_specs=[vspec()] * Q + [aspec()] * 3,
            out_specs=[aspec()] * 9 + [vspec()] * Q,
            scratch_shapes=[pltpu.VMEM((S, S, NB), F32), pltpu.VMEM((S, S, NB), F32), pltpu.VMEM((S, 32, NB), BF16),
                            pltpu.VMEM((2, FF, D), BF16), pltpu.VMEM((2, 2, D, FF), BF16), pltpu.VMEM((2, 2, FF, D), BF16), pltpu.VMEM((2, D, FF), BF16),
                            dma((10,)), dma((10,)), dma((2,)), dma((7,)), dma((7,)), dma((2, 3)), dma((2, 3))],
            compiler_params=pltpu.CompilerParams(collective_id=0, has_side_effects=True, vmem_limit_bytes=VMEM_MAX),
            name='k0_gather',
        )(tokens, r_proj, top_ids.T, w_router.T, w_gate, w_up, w_down)

        idx1 = idx.reshape(-1)
        gat1 = gat.reshape(-1)
        xswap = [(0, 2), (2, 0), (1, 3), (3, 1)]
        xqf = lax.ppermute(xqn, 'ep', xswap)
        rqf = lax.ppermute(rof, 'dp', [(0, 1), (1, 0)])

        wspec = [pl.BlockSpec((1, D, FF), lambda e: (e, 0, 0)), pl.BlockSpec((1, D, FF), lambda e: (e, 0, 0)), pl.BlockSpec((1, FF, D), lambda e: (e, 0, 0))]
        tall_spec, wide_spec = wspec[0], wspec[2]
        tspec = [wide_spec, wide_spec, tall_spec]
        part = sds((R1, L), F32)
        pspec = pl.BlockSpec((R1, L), lambda e: (0, 0))
        yp, dxp, dgt = pl.pallas_call(
            own_kernel,
            grid=(NE,),
            out_shape=[part, part, sds((S, HALF), F32)],
            in_specs=[sspec()] * 3 + [vspec()] + [aspec()] * Q + wspec + tspec,
            out_specs=[pspec, pspec, pl.BlockSpec((S, HALF), lambda e: (0, 0))],
            scratch_shapes=[pltpu.VMEM((X1, L), F32)] * 2 + [pltpu.VMEM((XT, L), F32)] * 2 + [pltpu.VMEM((T, D), BF16)] * 3
            + [pltpu.VMEM((XT, L), F32)] * 2 + [pltpu.VMEM((T, L), F32), pltpu.VMEM((RB, L), F32), pltpu.VMEM((T, L), F32),
               pltpu.VMEM((SLOTS, NB, D), BF16), pltpu.SMEM((1,), jnp.int32), dma((SLOTS,))],
            compiler_params=pltpu.CompilerParams(vmem_limit_bytes=VMEM_MAX, dimension_semantics=('arbitrary',)),
            cost_estimate=pl.CostEstimate(flops=20 * 10 ** 9, bytes_accessed=40 * 10 ** 6, transcendentals=0),
            name='k1_own',
        )(cnt, idx1, pid, gat.reshape(NL * S, L), xon, xof, ron, rof, w_gate, w_up, w_down, w1t, w3t, w2t)

        quarter = sds((NB * S, L), F32)
        ynear, yfar, dnear, dfar, dg, gt = pl.pallas_call(
            pair_kernel,
            out_shape=[quarter] * Q + [sds((S, S, HALF), F32), sds((S, 32, NB), F32)],
            in_specs=[aspec(), aspec(), vspec(), vspec()],
            out_specs=[vspec()] * 6,
            scratch_shapes=[pltpu.VMEM((Q, NB * S, L), F32), pltpu.VMEM((Q, NB * S, L), F32), pltpu.VMEM((S, S, HALF), F32), pltpu.VMEM((S, 32, NB), F32),
                            dma((Q,)), dma((Q,)), dma((Q,)), dma((2, 7)), dma((2, 7))],
            compiler_params=pltpu.CompilerParams(collective_id=1, has_side_effects=True),
            name='k2_pair',
        )(yp, dxp, dgt, gto)

        yrec = lax.ppermute(yfar, 'ep', xswap)
        drec = lax.ppermute(dfar, 'ep', xswap)

        gspec = [pl.BlockSpec((1, D, FF), lambda e: (e, 0, 0)), pl.BlockSpec((1, D, FF), lambda e: (e, 0, 0)), pl.BlockSpec((1, FF, D), lambda e: (e, 0, 0))]
        grad_gate, grad_up, grad_down = pl.pallas_call(
            grad_kernel,
            grid=(NE,),
            out_shape=[sds((NE, D, FF), F32), sds((NE, D, FF), F32), sds((NE, FF, D), F32)],
            in_specs=[sspec()] * 3 + [aspec()] * S + wspec[:2] + [tall_spec],
            out_specs=gspec,
            scratch_shapes=[pltpu.VMEM((X2, L), F32)] * 2 + [pltpu.VMEM((XT, L), F32)] * 2 + [pltpu.VMEM((T, D), BF16)] * 2
            + [pltpu.VMEM((SLOTS, NB, D), BF16), dma((SLOTS,))],
            compiler_params=pltpu.CompilerParams(vmem_limit_bytes=VMEM_MAX, dimension_semantics=('arbitrary',)),
            cost_estimate=pl.CostEstimate(flops=30 * 10 ** 9, bytes_accessed=90 * 10 ** 6, transcendentals=0),
            name='k3_grad',
        )(cnt, idx1, gat1, xon, xof, xqn, xqf, ron, rof, rqn, rqf, w_gate, w_up, w2t)

        y, dx, dwt = pl.pallas_call(
            final_kernel,
            out_shape=[sds((NB, D), F32), sds((NB, D), F32), sds((32, D), F32)],
            in_specs=[sspec()] + [vspec()] * 13,
            out_specs=[vspec()] * 3,
            scratch_shapes=[pltpu.VMEM((S, 32, NB), BF16)],
            compiler_params=pltpu.CompilerParams(vmem_limit_bytes=VMEM_MAX),
            name='k4_final',
        )(pid, tokens, r_proj, ynear, dnear, yrec, drec, dg.reshape(64, HALF), gt, w_router.T, xon, xof, xqn, xqf)
        return y, dx, grad_gate, grad_up, grad_down, dwt.T

    tok_spec = P(axes, None)
    exp_spec = P('ep', None, None)
    return jax.shard_map(local_step, mesh=mesh, in_specs=(tok_spec, P(), exp_spec, exp_spec, exp_spec, tok_spec, tok_spec), out_specs=(tok_spec, tok_spec, exp_spec, exp_spec, exp_spec, P()), check_vma=False)
```

```python
import functools

import jax
import jax.numpy as jnp
from jax import lax
from jax.experimental import pallas as pl
from jax.experimental.pallas import tpu as pltpu
from jax.sharding import PartitionSpec as P

F32 = jnp.float32
BF16 = jnp.bfloat16
MESH = pl.DeviceIdType.MESH
VMEM_MAX = 63 * 1024 * 1024
T = 256
NB = 256
HALF = 1024
D = 1024
FF = 512
NE = 8
NL = 17
SLOTS = 8
PT = 9
S = 8
L = 128
Q = 4
RB = 1032
R1 = 8256
R2 = 16448
X1 = 9288
X2 = 18504
XT = 2304


def dot(a, b, ca=1, cb=0):
    return lax.dot_general(a, b, (((ca,), (cb,)), ((), ())), preferred_element_type=F32)


def vspec():
    return pl.BlockSpec(memory_space=pltpu.VMEM)


def aspec():
    return pl.BlockSpec(memory_space=pl.ANY)


def sspec():
    return pl.BlockSpec(memory_space=pltpu.SMEM)


def barrier_all(dp, ep):
    bar = pltpu.get_barrier_semaphore()
    for k in range(1, S):
        pl.semaphore_signal(bar, inc=1, device_id=((dp + k // Q) % 2, (ep + k % Q) % Q), device_id_type=MESH)
    pl.semaphore_wait(bar, 7)


def gather_kernel(x_ref, r_ref, ids_ref, wr_ref,
                  xon, xof, ron, rof, xqn, rqn, gt_out, idx_out, gat_out, cnt_out,
                  gt_s, pos_s, v_s, ssem, rsem, lsem, gsend, grecv):
    dp = lax.axis_index('dp')
    ep = lax.axis_index('ep')
    c = ep % 2
    xc = ep // 2
    me = dp * Q + ep
    mate = (dp, xc * 2 + 1 - c)
    xnb = (dp, (1 - xc) * 2 + c)
    ynb = (1 - dp, ep)
    barrier_all(dp, ep)

    def rcopy(src, dst, k, dev):
        return pltpu.make_async_remote_copy(src_ref=src, dst_ref=dst, send_sem=ssem.at[k], recv_sem=rsem.at[k], device_id=dev, device_id_type=MESH)

    direct = [
        rcopy(x_ref, xof.at[c], 0, xnb), rcopy(x_ref, xqn.at[c], 1, ynb),
        rcopy(r_ref, rof.at[c], 2, xnb), rcopy(r_ref, rqn.at[c], 3, ynb),
        rcopy(x_ref, xon.at[c], Q, mate), rcopy(r_ref, ron.at[c], 5, mate)]
    for cp in direct[:2] + direct[Q:5]:
        cp.start()
    local = [pltpu.make_async_copy(x_ref, xon.at[c], lsem.at[0]), pltpu.make_async_copy(r_ref, ron.at[c], lsem.at[1])]
    for cp in local:
        cp.start()

    zt = dot(wr_ref[...], x_ref[...], 1, 1)
    eio = lax.broadcasted_iota(jnp.int32, (32, NB), 0)
    sel = eio == ids_ref[0:1, :]
    for j in range(1, S):
        sel = sel | (eio == ids_ref[j:j + 1, :])
    zm = jnp.max(jnp.where(sel, zt, -jnp.inf), axis=0, keepdims=True)
    pe = jnp.where(sel, jnp.exp(zt - zm), 0.0)
    gt_out[...] = jnp.where(sel, pe / jnp.sum(pe, axis=0, keepdims=True), -1.0)
    gt_s[me] = gt_out[pl.ds(pl.multiple_of(ep * S, S), S), :]
    gcopies = []
    for k in range(1, S):
        dev = ((dp + k // Q) % 2, (ep + k % Q) % Q)
        cp = pltpu.make_async_remote_copy(src_ref=gt_out.at[pl.ds(pl.multiple_of(dev[1] * S, S), S)], dst_ref=gt_s.at[me], send_sem=gsend.at[k - 1], recv_sem=grecv.at[k - 1], device_id=dev, device_id_type=MESH)
        cp.start()
        gcopies.append(cp)
    for cp in direct[2:4] + direct[5:]:
        cp.start()
    fwd = [
        rcopy(xof.at[c], xof.at[c], 6, mate), rcopy(xqn.at[c], xqn.at[c], 7, mate),
        rcopy(rof.at[c], rof.at[c], S, mate), rcopy(rqn.at[c], rqn.at[c], 9, mate)]
    for k in range(2):
        direct[k].wait_recv()
        fwd[k].start()
    for cp in gcopies:
        cp.wait()

    tri = (lax.broadcasted_iota(jnp.int32, (NB, NB), 0) < lax.broadcasted_iota(jnp.int32, (NB, NB), 1)).astype(BF16)
    srow = lax.broadcasted_iota(jnp.int32, (S, NB), 0)
    tlan = lax.broadcasted_iota(jnp.int32, (S, NB), 1).astype(F32)
    for half in range(2):
        base = jnp.zeros((S, 1), F32)
        for k in range(Q):
            hd = dp if half == 0 else 1 - dp
            xx = xc if k < 2 else 1 - xc
            g = gt_s[hd * Q + xx * 2 + k % 2]
            m = g >= 0.0
            mf = m.astype(F32)
            pos = dot(mf.astype(BF16), tri) + base
            pos_s[half * Q + k] = jnp.where(m, pos, -1.0)
            base = base + jnp.sum(mf, axis=1, keepdims=True)
            g = jnp.where(m, g, 0.0)
            g1 = g.astype(BF16)
            e1 = g - g1.astype(F32)
            g2 = e1.astype(BF16)
            g3 = (e1 - g2.astype(F32)).astype(BF16)
            head = jnp.where(srow == 0, tlan, jnp.where(srow == 1, float(k), 0.0))
            v_s[half * Q + k] = jnp.concatenate([head, g1.astype(F32), g2.astype(F32), g3.astype(F32)], axis=0).astype(BF16)
        cnt_out[half] = jnp.broadcast_to(base, (S, L)).astype(jnp.int32)

    pio = lax.broadcasted_iota(jnp.int32, (NB, NB), 0).astype(F32)
    rio = lax.broadcasted_iota(jnp.int32, (32, NB), 0)
    lio = lax.broadcasted_iota(jnp.int32, (1, NB), 1)

    def list_body(he, carry):
        half = he // S
        e = he % S
        cnt_e = cnt_out[half, pl.ds(e, 1), 0:1]
        for pt in range(Q):
            acc = jnp.zeros((32, NB), F32)
            for k in range(pt, Q):
                prow = pos_s[half * Q + k, pl.ds(e, 1), :] - float(256 * pt)
                oh = (pio == prow).astype(F32).astype(BF16)
                acc = acc + dot(v_s[half * Q + k], oh, 1, 1)
            ids = (acc[0:1, :] + 256.0 * acc[1:2, :]).astype(jnp.int32)
            ids = jnp.where(lio + NB * pt < cnt_e, ids, HALF) + half * HALF
            gv = jnp.sum(jnp.where((rio >= S) & (rio % S == e), acc, 0.0), axis=0, keepdims=True)
            for q in range(2):
                idx_out[he, 2 * pt + q:2 * pt + q + 1, :] = ids[:, L * q:L * (q + 1)]
                gat_out[he, 2 * pt + q:2 * pt + q + 1, :] = gv[:, L * q:L * (q + 1)]
        return carry

    lax.fori_loop(0, 2 * S, list_body, 0)
    cnt_out[2] = jnp.full((S, L), dp, jnp.int32)
    cnt_out[3] = jnp.full((S, L), ep, jnp.int32)
    idx_out[2 * S] = jnp.zeros((S, L), jnp.int32)
    gat_out[2 * S] = jnp.zeros((S, L), F32)

    for k in range(2, Q):
        direct[k].wait_recv()
        fwd[k].start()
    for cp in local:
        cp.wait()
    direct[Q].wait_recv()
    direct[5].wait_recv()
    for cp in direct:
        cp.wait_send()
    for cp in fwd:
        cp.wait()


def load_tokens(pairs, x2, r2, tmp, sem, before, hook):
    srcs = []
    for i, (xa, ra) in enumerate(pairs):
        for c in range(2):
            srcs.append((xa.at[c], x2, (2 * i + c) * NB))
            srcs.append((ra.at[c], r2, (2 * i + c) * NB))
    copies = [pltpu.make_async_copy(src, tmp.at[i % SLOTS], sem.at[i % SLOTS]) for i, (src, _, _) in enumerate(srcs)]
    for i in range(SLOTS):
        copies[i].start()
    before()
    for i, (_, dst2, row) in enumerate(srcs):
        copies[i].wait()

        def body(b, carry, i=i, dst2=dst2, row=row):
            r0 = pl.multiple_of(b * 64, 64)
            for s in range(S):
                dst2[pl.ds((row + r0) * PT + s, 64, stride=PT), :] = tmp[i % SLOTS, pl.ds(r0, 64), L * s:L * (s + 1)].astype(F32)
            return carry

        lax.fori_loop(0, NB // 64, body, 0)
        if hook is not None and i % 2 == 0:
            hook(i // 2, tmp.at[i % SLOTS])
        if i + SLOTS < len(srcs):
            copies[i + SLOTS].start()
    for ref in (x2, r2):
        ref[row9(2 * len(pairs) * NB), :] = jnp.zeros((S, L), F32)


def strided(ref2, s):
    return ref2[pl.ds(s, T, stride=PT), :]


def zero_rows(ref2, n):
    step = n // 12

    def body(i, carry):
        ref2[pl.ds(pl.multiple_of(i * step, S), step), :] = jnp.zeros((step, L), F32)
        return carry
    lax.fori_loop(0, 12, body, 0)


def row9(t):
    return pl.ds(t * PT, S)


def row8(t):
    return pl.ds(pl.multiple_of(t * S, S), S)


def own_kernel(cnt, idx, gatv, xn, xf, rn, rf, w1, w3, w2,
               y_out, dx_out, dgt_out,
               x2, r2, ust, rst, us, ds, o2, d2, dgs, dgd, gcs, tmp, prev, sem):
    e = pl.program_id(0)
    lane1 = lax.broadcasted_iota(jnp.int32, (1, L), 1)

    def gate_column(base):
        for q in range(2):
            gcs[L * q:L * (q + 1), :] = jnp.transpose(jnp.broadcast_to(gatv[pl.ds(base // L + q, 1), :], (L, L)))

    def gather(base, r0, n, slot):
        for r in range(n):
            t = row9(idx[base + r])
            ust[row9(r0 + r), :] = x2[t, :]
            rst[slot, row9(r0 + r), :] = r2[t, :]

    def scatter(base, r0, n):
        mine = lane1 == base // HALF
        for c in range(0, n, S):
            ts = [idx[base + c + j] for j in range(S)]
            ys = [y_out[row8(ts[j]), :] + o2[row9(r0 + c + j), :] for j in range(S)]
            dl = [dx_out[row8(ts[j]), :] + d2[row9(r0 + c + j), :] for j in range(S)]
            gd = [dgs[pl.ds(r0 + c + j, 1), :] for j in range(S)]
            for j in range(S):
                y_out[row8(ts[j]), :] = ys[j]
                dx_out[row8(ts[j]), :] = dl[j]
                pltpu.store(dgd.at[pl.ds(ts[j], 1), :], gd[j], mask=mine)

    @pl.when(e == 0)
    def _():
        def clear():
            zero_rows(y_out, R1)
            zero_rows(dx_out, R1)
            zero_rows(o2, XT)
            zero_rows(d2, XT)
            dgd[...] = jnp.zeros_like(dgd)
            dgs[...] = jnp.zeros_like(dgs)
            prev[0] = 0
            prev[1] = 0
            gate_column(0)

        load_tokens([(xn, rn), (xf, rf)], x2, r2, tmp, sem, clear, None)

        def first(c, carry):
            gather(c * S, c * S, S, 0)
            return carry
        lax.fori_loop(0, T // S, first, 0)

    n = cnt[0, e, 0]

    def tile_body(k, carry):
        base = k * T
        slot = prev[1]
        gcol = gcs[...]
        for s in range(S):
            cs = slice(L * s, L * (s + 1))
            us[:, cs] = strided(ust, s).astype(BF16)
            ds[:, cs] = (rst[slot, pl.ds(s, T, stride=PT), :] * gcol).astype(BF16)
        more = base + T < n
        nxt = jnp.where(more, e * HALF + base + T, jnp.minimum(e + 1, NE - 1) * HALF)
        gather(nxt, 0, T, 1 - slot)
        scatter(prev[0], 0, T)
        u = us[...]
        h1 = dot(u, w1[0])
        h3 = dot(u, w3[0])
        sg = jax.nn.sigmoid(h1)
        sl = h1 * sg
        a = (sl * h3).astype(BF16)
        da = dot(ds[...], w2[0], 1, 1)
        o = dot(a, w2[0]).astype(BF16).astype(F32)
        dh1 = (da * h3 * sg * (1.0 + h1 * (1.0 - sg))).astype(BF16)
        dh3 = (da * sl).astype(BF16)
        dr = (dot(dh1, w1[0], 1, 1) + dot(dh3, w3[0], 1, 1)).astype(BF16).astype(F32)
        acc = jnp.zeros((T, L), F32)
        for s in range(S):
            cs = slice(L * s, L * (s + 1))
            o2[pl.ds(s, T, stride=PT), :] = o[:, cs] * gcol
            d2[pl.ds(s, T, stride=PT), :] = dr[:, cs]
            acc = acc + o[:, cs] * rst[slot, pl.ds(s, T, stride=PT), :]
        dgs[...] = jnp.broadcast_to(jnp.sum(acc, axis=1, keepdims=True), (T, L))
        prev[0] = e * HALF + base
        prev[1] = 1 - slot
        gate_column(nxt)
        return carry

    lax.fori_loop(0, jnp.maximum((n + T - 1) // T, 1), tile_body, 0)

    @pl.when(e == NE - 1)
    def _():
        def last(c, carry):
            scatter(prev[0] + c * S, c * S, S)
            return carry
        lax.fori_loop(0, T // S, last, 0)
        xc = cnt[3, 0, 0] // 2
        tr = jnp.transpose(dgd[0:HALF, :])
        dgt_out[:, pl.ds(pl.multiple_of(xc * FF, FF), FF)] = tr[0:S, 0:FF]
        dgt_out[:, pl.ds(pl.multiple_of(FF - xc * FF, FF), FF)] = tr[0:S, FF:HALF]


def pair_kernel(yp, dxp, dgt, gt, far, near, dg_out, gt_out, rbuf, obuf, dgb, gtb, ssem, rsem, lsem, wsem, gsend, grecv):
    dp = lax.axis_index('dp')
    ep = lax.axis_index('ep')
    c = ep % 2
    me = dp * Q + ep
    mate = (dp, (ep // 2) * 2 + 1 - c)
    barrier_all(dp, ep)
    parts = [(yp, 4096), (dxp, 4096), (yp, 0), (dxp, 0)]
    outs = [far.at[0], far.at[1], near.at[0], near.at[1]]
    stores = [pltpu.make_async_copy(obuf.at[i], outs[i], wsem.at[i]) for i in range(Q)]
    sends, loads = [], []
    for i, (src, base) in enumerate(parts):
        cp = pltpu.make_async_remote_copy(
            src_ref=src.at[pl.ds(pl.multiple_of(base + (1 - c) * 2048, 2048), 2048)], dst_ref=rbuf.at[i],
            send_sem=ssem.at[i], recv_sem=rsem.at[i], device_id=mate, device_id_type=MESH)
        cp.start()
        sends.append(cp)
        ld = pltpu.make_async_copy(src.at[pl.ds(pl.multiple_of(base + c * 2048, 2048), 2048)], obuf.at[i], lsem.at[i])
        ld.start()
        loads.append(ld)
    gcopies = []
    for k in range(1, S):
        dev = ((dp + k // Q) % 2, (ep + k % Q) % Q)
        for q, (src, dst) in enumerate(((dgt, dgb), (gt, gtb))):
            cp = pltpu.make_async_remote_copy(src_ref=src, dst_ref=dst.at[me], send_sem=gsend.at[q, k - 1], recv_sem=grecv.at[q, k - 1], device_id=dev, device_id_type=MESH)
            cp.start()
            gcopies.append(cp)
    for i in range(Q):
        loads[i].wait()
        sends[i].wait_recv()

        def body(b, carry, i=i):
            s = pl.ds(pl.multiple_of(b * L, L), L)
            obuf[i, s, :] = obuf[i, s, :] + rbuf[i, s, :]
            return carry

        lax.fori_loop(0, NB // 16, body, 0)
        stores[i].start()
    for cp in gcopies:
        cp.wait()
    for cp in sends:
        cp.wait_send()
    dgb[me] = dgt[...]
    dg_out[...] = dgb[...]
    gtb[me] = gt[...]
    gt_out[...] = gtb[...]
    for cp in stores:
        cp.wait()


def grad_kernel(cnt, idx, gat, dg, gt, xon, xof, xqn, xqf, ron, rof, rqn, rqf, w1, w3, w2,
                g1, g3, g2, dw_out, dz_out, x2, r2, ust, dst, us, ds, tmp, dz_s, sem):
    e = pl.program_id(0)

    def gather(ne, nb, r0, n):
        n0 = cnt[0, ne, 0]
        a0 = ne * HALF
        a1 = NE * HALF + a0 - n0
        for r in range(n):
            q = nb + r
            q = q + jnp.where(q < n0, a0, a1)
            t = row9(idx[q])
            ust[row9(r0 + r), :] = x2[t, :]
            dst[row9(r0 + r), :] = r2[t, :] * gat[q]

    @pl.when(e == 0)
    def _():
        dp = cnt[2, 0, 0]
        ep = cnt[3, 0, 0]

        def router_grads():
            for b in range(S):
                gm = jnp.maximum(gt[b], 0.0)
                dgv = dg[32 * (b // Q):32 * (b // Q + 1), NB * (b % Q):NB * (b % Q + 1)]
                tot = jnp.sum(gm * dgv, axis=0, keepdims=True)
                dz_s[b] = (gm * (dgv - tot)).astype(BF16)
            dz_out[...] = dz_s[dp * Q + ep]
            dw_out[...] = jnp.zeros_like(dw_out)

        def add_chunk(i, xc_ref):
            hd = dp if i < Q else 1 - dp
            xx = ep // 2 if i % Q < 2 else 1 - ep // 2
            dw_out[...] += dot(dz_s[hd * Q + xx * 2 + i % 2], xc_ref[...])

        load_tokens([(xon, ron), (xof, rof), (xqn, rqn), (xqf, rqf)], x2, r2, tmp, sem, router_grads, add_chunk)

        def first(c, carry):
            gather(0, c * S, c * S, S)
            return carry
        lax.fori_loop(0, T // S, first, 0)

    n = cnt[0, e, 0] + cnt[1, e, 0]
    rown = lax.broadcasted_iota(jnp.int32, (T, L), 0)

    def tile(k, first):
        base = k * T
        live = rown + base < n
        for s in range(S):
            cs = slice(L * s, L * (s + 1))
            us[:, cs] = strided(ust, s).astype(BF16)
            ds[:, cs] = jnp.where(live, strided(dst, s), 0.0).astype(BF16)
        more = base + T < n
        gather(jnp.where(more, e, jnp.minimum(e + 1, NE - 1)), jnp.where(more, base + T, 0), 0, T)
        u = us[...]
        do = ds[...]
        h1 = dot(u, w1[0])
        h3 = dot(u, w3[0])
        sg = jax.nn.sigmoid(h1)
        sl = h1 * sg
        a = (sl * h3).astype(BF16)
        da = dot(do, w2[0], 1, 1)
        dh1 = (da * h3 * sg * (1.0 + h1 * (1.0 - sg))).astype(BF16)
        dh3 = (da * sl).astype(BF16)
        if first:
            g2[0] = dot(a, do, 0, 0)
            g1[0] = dot(u, dh1, 0, 0)
            g3[0] = dot(u, dh3, 0, 0)
        else:
            g2[0] += dot(a, do, 0, 0)
            g1[0] += dot(u, dh1, 0, 0)
            g3[0] += dot(u, dh3, 0, 0)

    tile(0, True)

    def tile_body(k, carry):
        tile(k, False)
        return carry

    lax.fori_loop(1, (n + T - 1) // T, tile_body, 0)


def final_kernel(x, r, near, rec, dz, wr, y_out, dx_out):
    dxr = dot(dz[...], wr[...], 0, 0)
    for s in range(S):
        cs = slice(L * s, L * (s + 1))
        rows = pl.ds(s, L, stride=S)
        y_out[:, cs] = x[:, cs].astype(F32) + (near[0, rows, :] + rec[0, rows, :])
        dx_out[:, cs] = r[:, cs].astype(F32) + dxr[:, cs] + (near[1, rows, :] + rec[1, rows, :])


def solution(mesh):
    axes = ('dp', 'ep')
    sds = jax.ShapeDtypeStruct

    def local_step(tokens, w_router, w_gate, w_up, w_down, top_ids, r_proj):
        near = sds((2, NB, D), BF16)
        dma = pltpu.SemaphoreType.DMA
        xon, xof, ron, rof, xqn, rqn, gto, idx, gat, cnt = pl.pallas_call(
            gather_kernel,
            out_shape=[near] * 6 + [sds((32, NB), F32), sds((NL, S, L), jnp.int32), sds((NL, S, L), F32), sds((Q, S, L), jnp.int32)],
            in_specs=[vspec()] * Q,
            out_specs=[aspec()] * 6 + [vspec()] * Q,
            scratch_shapes=[pltpu.VMEM((S, S, NB), F32), pltpu.VMEM((S, S, NB), F32), pltpu.VMEM((S, 32, NB), BF16),
                            dma((10,)), dma((10,)), dma((2,)), dma((7,)), dma((7,))],
            compiler_params=pltpu.CompilerParams(collective_id=0, has_side_effects=True),
            name='k0_gather',
        )(tokens, r_proj, top_ids.T, w_router.T)

        idx1 = idx.reshape(-1)
        gat1 = gat.reshape(-1)
        xswap = [(0, 2), (2, 0), (1, 3), (3, 1)]
        xqf = lax.ppermute(xqn, 'ep', xswap)
        rqf = lax.ppermute(rof, 'dp', [(0, 1), (1, 0)])

        wspec = [pl.BlockSpec((1, D, FF), lambda e: (e, 0, 0)), pl.BlockSpec((1, D, FF), lambda e: (e, 0, 0)), pl.BlockSpec((1, FF, D), lambda e: (e, 0, 0))]
        part = sds((R1, L), F32)
        pspec = pl.BlockSpec((R1, L), lambda e: (0, 0))
        yp, dxp, dgt = pl.pallas_call(
            own_kernel,
            grid=(NE,),
            out_shape=[part, part, sds((S, HALF), F32)],
            in_specs=[sspec()] * 2 + [vspec()] + [aspec()] * Q + wspec,
            out_specs=[pspec, pspec, pl.BlockSpec((S, HALF), lambda e: (0, 0))],
            scratch_shapes=[pltpu.VMEM((X1, L), F32)] * 2 + [pltpu.VMEM((XT, L), F32), pltpu.VMEM((2, XT, L), F32)] + [pltpu.VMEM((T, D), BF16)] * 2
            + [pltpu.VMEM((XT, L), F32)] * 2 + [pltpu.VMEM((T, L), F32), pltpu.VMEM((RB, L), F32), pltpu.VMEM((T, L), F32),
               pltpu.VMEM((SLOTS, NB, D), BF16), pltpu.SMEM((2,), jnp.int32), dma((SLOTS,))],
            compiler_params=pltpu.CompilerParams(vmem_limit_bytes=VMEM_MAX, dimension_semantics=('arbitrary',)),
            cost_estimate=pl.CostEstimate(flops=20 * 10 ** 9, bytes_accessed=40 * 10 ** 6, transcendentals=0),
            name='k1_own',
        )(cnt, idx1, gat.reshape(NL * S, L), xon, xof, ron, rof, w_gate, w_up, w_down)

        quarter = sds((2, NB * S, L), F32)
        far, near2, dg, gt = pl.pallas_call(
            pair_kernel,
            out_shape=[quarter] * 2 + [sds((S, S, HALF), F32), sds((S, 32, NB), F32)],
            in_specs=[aspec(), aspec(), vspec(), vspec()],
            out_specs=[aspec()] * 2 + [vspec()] * 2,
            scratch_shapes=[pltpu.VMEM((Q, NB * S, L), F32), pltpu.VMEM((Q, NB * S, L), F32), pltpu.VMEM((S, S, HALF), F32), pltpu.VMEM((S, 32, NB), F32),
                            dma((Q,)), dma((Q,)), dma((Q,)), dma((Q,)), dma((2, 7)), dma((2, 7))],
            compiler_params=pltpu.CompilerParams(collective_id=1, has_side_effects=True),
            name='k2_pair',
        )(yp, dxp, dgt, gto)

        rec = lax.ppermute(far, 'ep', xswap)

        gspec = [pl.BlockSpec((1, D, FF), lambda e: (e, 0, 0)), pl.BlockSpec((1, D, FF), lambda e: (e, 0, 0)), pl.BlockSpec((1, FF, D), lambda e: (e, 0, 0))]
        grad_gate, grad_up, grad_down, dwt, dz = pl.pallas_call(
            grad_kernel,
            grid=(NE,),
            out_shape=[sds((NE, D, FF), F32), sds((NE, D, FF), F32), sds((NE, FF, D), F32), sds((32, D), F32), sds((32, NB), BF16)],
            in_specs=[sspec()] * 3 + [vspec()] * 2 + [aspec()] * S + wspec,
            out_specs=gspec + [pl.BlockSpec((32, D), lambda e: (0, 0)), pl.BlockSpec((32, NB), lambda e: (0, 0))],
            scratch_shapes=[pltpu.VMEM((X2, L), F32)] * 2 + [pltpu.VMEM((XT, L), F32)] * 2 + [pltpu.VMEM((T, D), BF16)] * 2
            + [pltpu.VMEM((SLOTS, NB, D), BF16), pltpu.VMEM((S, 32, NB), BF16), dma((SLOTS,))],
            compiler_params=pltpu.CompilerParams(vmem_limit_bytes=VMEM_MAX, dimension_semantics=('arbitrary',)),
            cost_estimate=pl.CostEstimate(flops=30 * 10 ** 9, bytes_accessed=90 * 10 ** 6, transcendentals=0),
            name='k3_grad',
        )(cnt, idx1, gat1, dg.reshape(64, HALF), gt, xon, xof, xqn, xqf, ron, rof, rqn, rqf, w_gate, w_up, w_down)

        rspec = pl.BlockSpec((L, D), lambda i: (i, 0))
        qspec = pl.BlockSpec((2, L * S, L), lambda i: (0, i, 0))
        y, dx = pl.pallas_call(
            final_kernel,
            grid=(2,),
            out_shape=[sds((NB, D), F32), sds((NB, D), F32)],
            in_specs=[rspec, rspec, qspec, qspec, pl.BlockSpec((32, L), lambda i: (0, i)), pl.BlockSpec((32, D), lambda i: (0, 0))],
            out_specs=[rspec, rspec],
            compiler_params=pltpu.CompilerParams(vmem_limit_bytes=VMEM_MAX),
            name='k4_final',
        )(tokens, r_proj, near2, rec, dz, w_router.T)
        return y, dx, grad_gate, grad_up, grad_down, dwt.T

    tok_spec = P(axes, None)
    exp_spec = P('ep', None, None)
    return jax.shard_map(local_step, mesh=mesh, in_specs=(tok_spec, P(), exp_spec, exp_spec, exp_spec, tok_spec, tok_spec), out_specs=(tok_spec, tok_spec, exp_spec, exp_spec, exp_spec, P()), check_vma=False)
```

```python
import functools

import jax
import jax.numpy as jnp
from jax import lax
from jax.experimental import pallas as pl
from jax.experimental.pallas import tpu as pltpu
from jax.sharding import PartitionSpec as P

F32 = jnp.float32
BF16 = jnp.bfloat16
MESH = pl.DeviceIdType.MESH
VMEM_MAX = 63 * 1024 * 1024
T = 256
NB = 256
HALF = 1024
D = 1024
FF = 512
NE = 8
NL = 17
SLOTS = 8
PT = 9
S = 8
L = 128
Q = 4
RB = 1032
R1 = 8256
R2 = 16448
X1 = 9288
X2 = 18504
XT = 2304


def dot(a, b, ca=1, cb=0):
    return lax.dot_general(a, b, (((ca,), (cb,)), ((), ())), preferred_element_type=F32)


def vspec():
    return pl.BlockSpec(memory_space=pltpu.VMEM)


def aspec():
    return pl.BlockSpec(memory_space=pl.ANY)


def sspec():
    return pl.BlockSpec(memory_space=pltpu.SMEM)


def barrier_all(dp, ep):
    bar = pltpu.get_barrier_semaphore()
    for k in range(1, S):
        pl.semaphore_signal(bar, inc=1, device_id=((dp + k // Q) % 2, (ep + k % Q) % Q), device_id_type=MESH)
    pl.semaphore_wait(bar, 7)


def gather_kernel(x_ref, r_ref, ids_ref, wr_ref,
                  xon, xof, ron, rof, xqn, rqn, gt_out, idx_out, gat_out, cnt_out,
                  gt_s, pos_s, v_s, ssem, rsem, lsem, gsend, grecv):
    dp = lax.axis_index('dp')
    ep = lax.axis_index('ep')
    c = ep % 2
    xc = ep // 2
    me = dp * Q + ep
    mate = (dp, xc * 2 + 1 - c)
    xnb = (dp, (1 - xc) * 2 + c)
    ynb = (1 - dp, ep)
    barrier_all(dp, ep)

    def rcopy(src, dst, k, dev):
        return pltpu.make_async_remote_copy(src_ref=src, dst_ref=dst, send_sem=ssem.at[k], recv_sem=rsem.at[k], device_id=dev, device_id_type=MESH)

    direct = [
        rcopy(x_ref, xof.at[c], 0, xnb), rcopy(x_ref, xqn.at[c], 1, ynb),
        rcopy(r_ref, rof.at[c], 2, xnb), rcopy(r_ref, rqn.at[c], 3, ynb),
        rcopy(x_ref, xon.at[c], Q, mate), rcopy(r_ref, ron.at[c], 5, mate)]
    for cp in direct[:2] + direct[Q:5]:
        cp.start()
    local = [pltpu.make_async_copy(x_ref, xon.at[c], lsem.at[0]), pltpu.make_async_copy(r_ref, ron.at[c], lsem.at[1])]
    for cp in local:
        cp.start()

    zt = dot(wr_ref[...], x_ref[...], 1, 1)
    eio = lax.broadcasted_iota(jnp.int32, (32, NB), 0)
    sel = eio == ids_ref[0:1, :]
    for j in range(1, S):
        sel = sel | (eio == ids_ref[j:j + 1, :])
    zm = jnp.max(jnp.where(sel, zt, -jnp.inf), axis=0, keepdims=True)
    pe = jnp.where(sel, jnp.exp(zt - zm), 0.0)
    gt_out[...] = jnp.where(sel, pe / jnp.sum(pe, axis=0, keepdims=True), -1.0)
    gt_s[me] = gt_out[pl.ds(pl.multiple_of(ep * S, S), S), :]
    gcopies = []
    for k in range(1, S):
        dev = ((dp + k // Q) % 2, (ep + k % Q) % Q)
        cp = pltpu.make_async_remote_copy(src_ref=gt_out.at[pl.ds(pl.multiple_of(dev[1] * S, S), S)], dst_ref=gt_s.at[me], send_sem=gsend.at[k - 1], recv_sem=grecv.at[k - 1], device_id=dev, device_id_type=MESH)
        cp.start()
        gcopies.append(cp)
    for cp in direct[2:4] + direct[5:]:
        cp.start()
    fwd = [
        rcopy(xof.at[c], xof.at[c], 6, mate), rcopy(xqn.at[c], xqn.at[c], 7, mate),
        rcopy(rof.at[c], rof.at[c], S, mate), rcopy(rqn.at[c], rqn.at[c], 9, mate)]
    for k in range(2):
        direct[k].wait_recv()
        fwd[k].start()
    for cp in gcopies:
        cp.wait()

    tri = (lax.broadcasted_iota(jnp.int32, (NB, NB), 0) < lax.broadcasted_iota(jnp.int32, (NB, NB), 1)).astype(BF16)
    srow = lax.broadcasted_iota(jnp.int32, (S, NB), 0)
    tlan = lax.broadcasted_iota(jnp.int32, (S, NB), 1).astype(F32)
    for half in range(2):
        base = jnp.zeros((S, 1), F32)
        for k in range(Q):
            hd = dp if half == 0 else 1 - dp
            xx = xc if k < 2 else 1 - xc
            g = gt_s[hd * Q + xx * 2 + k % 2]
            m = g >= 0.0
            mf = m.astype(F32)
            pos = dot(mf.astype(BF16), tri) + base
            pos_s[half * Q + k] = jnp.where(m, pos, -1.0)
            base = base + jnp.sum(mf, axis=1, keepdims=True)
            g = jnp.where(m, g, 0.0)
            g1 = g.astype(BF16)
            e1 = g - g1.astype(F32)
            g2 = e1.astype(BF16)
            g3 = (e1 - g2.astype(F32)).astype(BF16)
            head = jnp.where(srow == 0, tlan, jnp.where(srow == 1, float(k), 0.0))
            v_s[half * Q + k] = jnp.concatenate([head, g1.astype(F32), g2.astype(F32), g3.astype(F32)], axis=0).astype(BF16)
        cnt_out[half] = jnp.broadcast_to(base, (S, L)).astype(jnp.int32)

    pio = lax.broadcasted_iota(jnp.int32, (NB, NB), 0).astype(F32)
    rio = lax.broadcasted_iota(jnp.int32, (32, NB), 0)
    lio = lax.broadcasted_iota(jnp.int32, (1, NB), 1)

    def list_body(he, carry):
        half = he // S
        e = he % S
        cnt_e = cnt_out[half, pl.ds(e, 1), 0:1]
        for pt in range(Q):
            acc = jnp.zeros((32, NB), F32)
            for k in range(pt, Q):
                prow = pos_s[half * Q + k, pl.ds(e, 1), :] - float(256 * pt)
                oh = (pio == prow).astype(F32).astype(BF16)
                acc = acc + dot(v_s[half * Q + k], oh, 1, 1)
            ids = (acc[0:1, :] + 256.0 * acc[1:2, :]).astype(jnp.int32)
            ids = jnp.where(lio + NB * pt < cnt_e, ids, HALF) + half * HALF
            gv = jnp.sum(jnp.where((rio >= S) & (rio % S == e), acc, 0.0), axis=0, keepdims=True)
            for q in range(2):
                idx_out[he, 2 * pt + q:2 * pt + q + 1, :] = ids[:, L * q:L * (q + 1)]
                gat_out[he, 2 * pt + q:2 * pt + q + 1, :] = gv[:, L * q:L * (q + 1)]
        return carry

    lax.fori_loop(0, 2 * S, list_body, 0)
    cnt_out[2] = jnp.full((S, L), dp, jnp.int32)
    cnt_out[3] = jnp.full((S, L), ep, jnp.int32)
    idx_out[2 * S] = jnp.zeros((S, L), jnp.int32)
    gat_out[2 * S] = jnp.zeros((S, L), F32)

    for k in range(2, Q):
        direct[k].wait_recv()
        fwd[k].start()
    for cp in local:
        cp.wait()
    direct[Q].wait_recv()
    direct[5].wait_recv()
    for cp in direct:
        cp.wait_send()
    for cp in fwd:
        cp.wait()


def load_tokens(pairs, x2, r2, tmp, sem, before, hook):
    srcs = []
    for i, (xa, ra) in enumerate(pairs):
        for c in range(2):
            srcs.append((xa.at[c], x2, (2 * i + c) * NB))
            srcs.append((ra.at[c], r2, (2 * i + c) * NB))
    copies = [pltpu.make_async_copy(src, tmp.at[i % SLOTS], sem.at[i % SLOTS]) for i, (src, _, _) in enumerate(srcs)]
    for i in range(SLOTS):
        copies[i].start()
    before()
    for i, (_, dst2, row) in enumerate(srcs):
        copies[i].wait()

        def body(b, carry, i=i, dst2=dst2, row=row):
            r0 = pl.multiple_of(b * 64, 64)
            for s in range(S):
                dst2[pl.ds((row + r0) * PT + s, 64, stride=PT), :] = tmp[i % SLOTS, pl.ds(r0, 64), L * s:L * (s + 1)].astype(F32)
            return carry

        lax.fori_loop(0, NB // 64, body, 0)
        if hook is not None and i % 2 == 0:
            hook(i // 2, tmp.at[i % SLOTS])
        if i + SLOTS < len(srcs):
            copies[i + SLOTS].start()
    for ref in (x2, r2):
        ref[row9(2 * len(pairs) * NB), :] = jnp.zeros((S, L), F32)


def strided(ref2, s):
    return ref2[pl.ds(s, T, stride=PT), :]


def zero_rows(ref2, n):
    step = n // 12

    def body(i, carry):
        ref2[pl.ds(pl.multiple_of(i * step, S), step), :] = jnp.zeros((step, L), F32)
        return carry
    lax.fori_loop(0, 12, body, 0)


def row9(t):
    return pl.ds(t * PT, S)


def row8(t):
    return pl.ds(pl.multiple_of(t * S, S), S)


def own_kernel(cnt, idx, gatv, xn, xf, rn, rf, w1, w3, w2,
               y_out, dx_out, dgt_out,
               x2, r2, ust, rsta, rstb, us, ds, o2a, o2b, d2a, d2b, dgsa, dgsb, dgd, gcs, tmp, prev, sem):
    e = pl.program_id(0)
    lane1 = lax.broadcasted_iota(jnp.int32, (1, L), 1)

    def gate_column(base):
        for q in range(2):
            gcs[L * q:L * (q + 1), :] = jnp.transpose(jnp.broadcast_to(gatv[pl.ds(base // L + q, 1), :], (L, L)))

    rsts, o2s, d2s, dgss = (rsta, rstb), (o2a, o2b), (d2a, d2b), (dgsa, dgsb)

    def gather(base, r0, n, slot):
        for r in range(n):
            t = row9(idx[base + r])
            ust[row9(r0 + r), :] = x2[t, :]
            rsts[slot][row9(r0 + r), :] = r2[t, :]

    def scatter(base, r0, n, slot):
        o2, d2, dgs = o2s[slot], d2s[slot], dgss[slot]
        mine = lane1 == base // HALF
        for c in range(0, n, S):
            ts = [idx[base + c + j] for j in range(S)]
            ys = [y_out[row8(ts[j]), :] + o2[row9(r0 + c + j), :] for j in range(S)]
            dl = [dx_out[row8(ts[j]), :] + d2[row9(r0 + c + j), :] for j in range(S)]
            gd = [dgs[pl.ds(r0 + c + j, 1), :] for j in range(S)]
            for j in range(S):
                y_out[row8(ts[j]), :] = ys[j]
                dx_out[row8(ts[j]), :] = dl[j]
                pltpu.store(dgd.at[pl.ds(ts[j], 1), :], gd[j], mask=mine)

    @pl.when(e == 0)
    def _():
        def clear():
            zero_rows(y_out, R1)
            zero_rows(dx_out, R1)
            zero_rows(o2b, XT)
            zero_rows(d2b, XT)
            dgd[...] = jnp.zeros_like(dgd)
            dgsb[...] = jnp.zeros_like(dgsb)
            prev[0] = 0
            prev[1] = 0
            gate_column(0)

        load_tokens([(xn, rn), (xf, rf)], x2, r2, tmp, sem, clear, None)

        def first(c, carry):
            gather(c * S, c * S, S, 0)
            return carry
        lax.fori_loop(0, T // S, first, 0)

    n = cnt[0, e, 0]

    def tile(k, slot):
        base = k * T
        o2, d2, rst = o2s[slot], d2s[slot], rsts[slot]
        gcol = gcs[...]
        for s in range(S):
            cs = slice(L * s, L * (s + 1))
            us[:, cs] = strided(ust, s).astype(BF16)
            ds[:, cs] = (strided(rst, s) * gcol).astype(BF16)
        more = base + T < n
        nxt = jnp.where(more, e * HALF + base + T, jnp.minimum(e + 1, NE - 1) * HALF)
        gather(nxt, 0, T, 1 - slot)
        scatter(prev[0], 0, T, 1 - slot)
        u = us[...]
        h1 = dot(u, w1[0])
        h3 = dot(u, w3[0])
        sg = jax.nn.sigmoid(h1)
        sl = h1 * sg
        a = (sl * h3).astype(BF16)
        da = dot(ds[...], w2[0], 1, 1)
        o = dot(a, w2[0]).astype(BF16).astype(F32)
        dh1 = (da * h3 * sg * (1.0 + h1 * (1.0 - sg))).astype(BF16)
        dh3 = (da * sl).astype(BF16)
        dr = (dot(dh1, w1[0], 1, 1) + dot(dh3, w3[0], 1, 1)).astype(BF16).astype(F32)
        acc = jnp.zeros((T, L), F32)
        for s in range(S):
            cs = slice(L * s, L * (s + 1))
            o2[pl.ds(s, T, stride=PT), :] = o[:, cs] * gcol
            d2[pl.ds(s, T, stride=PT), :] = dr[:, cs]
            acc = acc + o[:, cs] * strided(rst, s)
        dgss[slot][...] = jnp.broadcast_to(jnp.sum(acc, axis=1, keepdims=True), (T, L))
        prev[0] = e * HALF + base
        prev[1] = 1 - slot
        gate_column(nxt)

    def tile_body(k, carry):
        par = prev[1]
        for slot in range(2):
            pl.when(par == slot)(functools.partial(tile, k, slot))
        return carry

    lax.fori_loop(0, jnp.maximum((n + T - 1) // T, 1), tile_body, 0)

    @pl.when(e == NE - 1)
    def _():
        def last(c, carry):
            for slot in range(2):
                pl.when(prev[1] != slot)(functools.partial(scatter, prev[0] + c * S, c * S, S, slot))
            return carry
        lax.fori_loop(0, T // S, last, 0)
        xc = cnt[3, 0, 0] // 2
        tr = jnp.transpose(dgd[0:HALF, :])
        dgt_out[:, pl.ds(pl.multiple_of(xc * FF, FF), FF)] = tr[0:S, 0:FF]
        dgt_out[:, pl.ds(pl.multiple_of(FF - xc * FF, FF), FF)] = tr[0:S, FF:HALF]


def pair_kernel(yp, dxp, dgt, gt, far, near, dg_out, gt_out, rbuf, obuf, dgb, gtb, ssem, rsem, lsem, wsem, gsend, grecv):
    dp = lax.axis_index('dp')
    ep = lax.axis_index('ep')
    c = ep % 2
    me = dp * Q + ep
    mate = (dp, (ep // 2) * 2 + 1 - c)
    barrier_all(dp, ep)
    parts = [(yp, 4096), (dxp, 4096), (yp, 0), (dxp, 0)]
    outs = [far.at[0], far.at[1], near.at[0], near.at[1]]
    stores = [pltpu.make_async_copy(obuf.at[i], outs[i], wsem.at[i]) for i in range(Q)]
    sends, loads = [], []
    for i, (src, base) in enumerate(parts):
        cp = pltpu.make_async_remote_copy(
            src_ref=src.at[pl.ds(pl.multiple_of(base + (1 - c) * 2048, 2048), 2048)], dst_ref=rbuf.at[i],
            send_sem=ssem.at[i], recv_sem=rsem.at[i], device_id=mate, device_id_type=MESH)
        cp.start()
        sends.append(cp)
        ld = pltpu.make_async_copy(src.at[pl.ds(pl.multiple_of(base + c * 2048, 2048), 2048)], obuf.at[i], lsem.at[i])
        ld.start()
        loads.append(ld)
    gcopies = []
    for k in range(1, S):
        dev = ((dp + k // Q) % 2, (ep + k % Q) % Q)
        for q, (src, dst) in enumerate(((dgt, dgb), (gt, gtb))):
            cp = pltpu.make_async_remote_copy(src_ref=src, dst_ref=dst.at[me], send_sem=gsend.at[q, k - 1], recv_sem=grecv.at[q, k - 1], device_id=dev, device_id_type=MESH)
            cp.start()
            gcopies.append(cp)
    for i in range(Q):
        loads[i].wait()
        sends[i].wait_recv()

        def body(b, carry, i=i):
            s = pl.ds(pl.multiple_of(b * L, L), L)
            obuf[i, s, :] = obuf[i, s, :] + rbuf[i, s, :]
            return carry

        lax.fori_loop(0, NB // 16, body, 0)
        stores[i].start()
    for cp in gcopies:
        cp.wait()
    for cp in sends:
        cp.wait_send()
    dgb[me] = dgt[...]
    dg_out[...] = dgb[...]
    gtb[me] = gt[...]
    gt_out[...] = gtb[...]
    for cp in stores:
        cp.wait()


def grad_kernel(cnt, idx, gat, dg, gt, xon, xof, xqn, xqf, ron, rof, rqn, rqf, w1, w3, w2,
                g1, g3, g2, dw_out, dz_out, x2, r2, ust, dst, us, ds, tmp, dz_s, sem):
    e = pl.program_id(0)

    def gather(ne, nb, r0, n):
        n0 = cnt[0, ne, 0]
        a0 = ne * HALF
        a1 = NE * HALF + a0 - n0
        for r in range(n):
            q = nb + r
            q = q + jnp.where(q < n0, a0, a1)
            t = row9(idx[q])
            ust[row9(r0 + r), :] = x2[t, :]
            dst[row9(r0 + r), :] = r2[t, :] * gat[q]

    @pl.when(e == 0)
    def _():
        dp = cnt[2, 0, 0]
        ep = cnt[3, 0, 0]

        def router_grads():
            for b in range(S):
                gm = jnp.maximum(gt[b], 0.0)
                dgv = dg[32 * (b // Q):32 * (b // Q + 1), NB * (b % Q):NB * (b % Q + 1)]
                tot = jnp.sum(gm * dgv, axis=0, keepdims=True)
                dz_s[b] = (gm * (dgv - tot)).astype(BF16)
            dz_out[...] = dz_s[dp * Q + ep]
            dw_out[...] = jnp.zeros_like(dw_out)

        def add_chunk(i, xc_ref):
            hd = dp if i < Q else 1 - dp
            xx = ep // 2 if i % Q < 2 else 1 - ep // 2
            dw_out[...] += dot(dz_s[hd * Q + xx * 2 + i % 2], xc_ref[...])

        load_tokens([(xon, ron), (xof, rof), (xqn, rqn), (xqf, rqf)], x2, r2, tmp, sem, router_grads, add_chunk)

        def first(c, carry):
            gather(0, c * S, c * S, S)
            return carry
        lax.fori_loop(0, T // S, first, 0)

    n = cnt[0, e, 0] + cnt[1, e, 0]
    rown = lax.broadcasted_iota(jnp.int32, (T, L), 0)

    def tile(k, first):
        base = k * T
        live = rown + base < n
        for s in range(S):
            cs = slice(L * s, L * (s + 1))
            us[:, cs] = strided(ust, s).astype(BF16)
            ds[:, cs] = jnp.where(live, strided(dst, s), 0.0).astype(BF16)
        more = base + T < n
        gather(jnp.where(more, e, jnp.minimum(e + 1, NE - 1)), jnp.where(more, base + T, 0), 0, T)
        u = us[...]
        do = ds[...]
        h1 = dot(u, w1[0])
        h3 = dot(u, w3[0])
        sg = jax.nn.sigmoid(h1)
        sl = h1 * sg
        a = (sl * h3).astype(BF16)
        da = dot(do, w2[0], 1, 1)
        dh1 = (da * h3 * sg * (1.0 + h1 * (1.0 - sg))).astype(BF16)
        dh3 = (da * sl).astype(BF16)
        if first:
            g2[0] = dot(a, do, 0, 0)
            g1[0] = dot(u, dh1, 0, 0)
            g3[0] = dot(u, dh3, 0, 0)
        else:
            g2[0] += dot(a, do, 0, 0)
            g1[0] += dot(u, dh1, 0, 0)
            g3[0] += dot(u, dh3, 0, 0)

    tile(0, True)

    def tile_body(k, carry):
        tile(k, False)
        return carry

    lax.fori_loop(1, (n + T - 1) // T, tile_body, 0)


def final_kernel(x, r, near, rec, dz, wr, y_out, dx_out):
    dxr = dot(dz[...], wr[...], 0, 0)
    for s in range(S):
        cs = slice(L * s, L * (s + 1))
        rows = pl.ds(s, L, stride=S)
        y_out[:, cs] = x[:, cs].astype(F32) + (near[0, rows, :] + rec[0, rows, :])
        dx_out[:, cs] = r[:, cs].astype(F32) + dxr[:, cs] + (near[1, rows, :] + rec[1, rows, :])


def solution(mesh):
    axes = ('dp', 'ep')
    sds = jax.ShapeDtypeStruct

    def local_step(tokens, w_router, w_gate, w_up, w_down, top_ids, r_proj):
        near = sds((2, NB, D), BF16)
        dma = pltpu.SemaphoreType.DMA
        xon, xof, ron, rof, xqn, rqn, gto, idx, gat, cnt = pl.pallas_call(
            gather_kernel,
            out_shape=[near] * 6 + [sds((32, NB), F32), sds((NL, S, L), jnp.int32), sds((NL, S, L), F32), sds((Q, S, L), jnp.int32)],
            in_specs=[vspec()] * Q,
            out_specs=[aspec()] * 6 + [vspec()] * Q,
            scratch_shapes=[pltpu.VMEM((S, S, NB), F32), pltpu.VMEM((S, S, NB), F32), pltpu.VMEM((S, 32, NB), BF16),
                            dma((10,)), dma((10,)), dma((2,)), dma((7,)), dma((7,))],
            compiler_params=pltpu.CompilerParams(collective_id=0, has_side_effects=True),
            name='k0_gather',
        )(tokens, r_proj, top_ids.T, w_router.T)

        idx1 = idx.reshape(-1)
        gat1 = gat.reshape(-1)
        xswap = [(0, 2), (2, 0), (1, 3), (3, 1)]
        xqf = lax.ppermute(xqn, 'ep', xswap)
        rqf = lax.ppermute(rof, 'dp', [(0, 1), (1, 0)])

        wspec = [pl.BlockSpec((1, D, FF), lambda e: (e, 0, 0)), pl.BlockSpec((1, D, FF), lambda e: (e, 0, 0)), pl.BlockSpec((1, FF, D), lambda e: (e, 0, 0))]
        part = sds((R1, L), F32)
        pspec = pl.BlockSpec((R1, L), lambda e: (0, 0))
        yp, dxp, dgt = pl.pallas_call(
            own_kernel,
            grid=(NE,),
            out_shape=[part, part, sds((S, HALF), F32)],
            in_specs=[sspec()] * 2 + [vspec()] + [aspec()] * Q + wspec,
            out_specs=[pspec, pspec, pl.BlockSpec((S, HALF), lambda e: (0, 0))],
            scratch_shapes=[pltpu.VMEM((X1, L), F32)] * 2 + [pltpu.VMEM((XT, L), F32)] * 3 + [pltpu.VMEM((T, D), BF16)] * 2
            + [pltpu.VMEM((XT, L), F32)] * Q + [pltpu.VMEM((T, L), F32)] * 2 + [pltpu.VMEM((RB, L), F32), pltpu.VMEM((T, L), F32),
               pltpu.VMEM((SLOTS, NB, D), BF16), pltpu.SMEM((2,), jnp.int32), dma((SLOTS,))],
            compiler_params=pltpu.CompilerParams(vmem_limit_bytes=VMEM_MAX, dimension_semantics=('arbitrary',)),
            cost_estimate=pl.CostEstimate(flops=20 * 10 ** 9, bytes_accessed=40 * 10 ** 6, transcendentals=0),
            name='k1_own',
        )(cnt, idx1, gat.reshape(NL * S, L), xon, xof, ron, rof, w_gate, w_up, w_down)

        quarter = sds((2, NB * S, L), F32)
        far, near2, dg, gt = pl.pallas_call(
            pair_kernel,
            out_shape=[quarter] * 2 + [sds((S, S, HALF), F32), sds((S, 32, NB), F32)],
            in_specs=[aspec(), aspec(), vspec(), vspec()],
            out_specs=[aspec()] * 2 + [vspec()] * 2,
            scratch_shapes=[pltpu.VMEM((Q, NB * S, L), F32), pltpu.VMEM((Q, NB * S, L), F32), pltpu.VMEM((S, S, HALF), F32), pltpu.VMEM((S, 32, NB), F32),
                            dma((Q,)), dma((Q,)), dma((Q,)), dma((Q,)), dma((2, 7)), dma((2, 7))],
            compiler_params=pltpu.CompilerParams(collective_id=1, has_side_effects=True),
            name='k2_pair',
        )(yp, dxp, dgt, gto)

        rec = lax.ppermute(far, 'ep', xswap)

        gspec = [pl.BlockSpec((1, D, FF), lambda e: (e, 0, 0)), pl.BlockSpec((1, D, FF), lambda e: (e, 0, 0)), pl.BlockSpec((1, FF, D), lambda e: (e, 0, 0))]
        grad_gate, grad_up, grad_down, dwt, dz = pl.pallas_call(
            grad_kernel,
            grid=(NE,),
            out_shape=[sds((NE, D, FF), F32), sds((NE, D, FF), F32), sds((NE, FF, D), F32), sds((32, D), F32), sds((32, NB), BF16)],
            in_specs=[sspec()] * 3 + [vspec()] * 2 + [aspec()] * S + wspec,
            out_specs=gspec + [pl.BlockSpec((32, D), lambda e: (0, 0)), pl.BlockSpec((32, NB), lambda e: (0, 0))],
            scratch_shapes=[pltpu.VMEM((X2, L), F32)] * 2 + [pltpu.VMEM((XT, L), F32)] * 2 + [pltpu.VMEM((T, D), BF16)] * 2
            + [pltpu.VMEM((SLOTS, NB, D), BF16), pltpu.VMEM((S, 32, NB), BF16), dma((SLOTS,))],
            compiler_params=pltpu.CompilerParams(vmem_limit_bytes=VMEM_MAX, dimension_semantics=('arbitrary',)),
            cost_estimate=pl.CostEstimate(flops=30 * 10 ** 9, bytes_accessed=90 * 10 ** 6, transcendentals=0),
            name='k3_grad',
        )(cnt, idx1, gat1, dg.reshape(64, HALF), gt, xon, xof, xqn, xqf, ron, rof, rqn, rqf, w_gate, w_up, w_down)

        rspec = pl.BlockSpec((L, D), lambda i: (i, 0))
        qspec = pl.BlockSpec((2, L * S, L), lambda i: (0, i, 0))
        y, dx = pl.pallas_call(
            final_kernel,
            grid=(2,),
            out_shape=[sds((NB, D), F32), sds((NB, D), F32)],
            in_specs=[rspec, rspec, qspec, qspec, pl.BlockSpec((32, L), lambda i: (0, i)), pl.BlockSpec((32, D), lambda i: (0, 0))],
            out_specs=[rspec, rspec],
            compiler_params=pltpu.CompilerParams(vmem_limit_bytes=VMEM_MAX),
            name='k4_final',
        )(tokens, r_proj, near2, rec, dz, w_router.T)
        return y, dx, grad_gate, grad_up, grad_down, dwt.T

    tok_spec = P(axes, None)
    exp_spec = P('ep', None, None)
    return jax.shard_map(local_step, mesh=mesh, in_specs=(tok_spec, P(), exp_spec, exp_spec, exp_spec, tok_spec, tok_spec), out_specs=(tok_spec, tok_spec, exp_spec, exp_spec, exp_spec, P()), check_vma=False)
```

```python
import functools

import jax
import jax.numpy as jnp
from jax import lax
from jax.experimental import pallas as pl
from jax.experimental.pallas import tpu as pltpu
from jax.sharding import PartitionSpec as P

F32 = jnp.float32
BF16 = jnp.bfloat16
MESH = pl.DeviceIdType.MESH
VMEM_MAX = 63 * 1024 * 1024
T = 256
NB = 256
HALF = 1024
D = 1024
FF = 512
NE = 8
NL = 17
SLOTS = 8
PT = 9
S = 8
L = 128
Q = 4
RB = 1032
R1 = 8256
R2 = 16448
X1 = 9288
X2 = 18504
XT = 2304


def dot(a, b, ca=1, cb=0):
    return lax.dot_general(a, b, (((ca,), (cb,)), ((), ())), preferred_element_type=F32)


def vspec():
    return pl.BlockSpec(memory_space=pltpu.VMEM)


def aspec():
    return pl.BlockSpec(memory_space=pl.ANY)


def sspec():
    return pl.BlockSpec(memory_space=pltpu.SMEM)


def barrier_all(dp, ep):
    bar = pltpu.get_barrier_semaphore()
    for k in range(1, S):
        pl.semaphore_signal(bar, inc=1, device_id=((dp + k // Q) % 2, (ep + k % Q) % Q), device_id_type=MESH)
    pl.semaphore_wait(bar, 7)


def gather_kernel(x_ref, r_ref, ids_ref, wr_ref,
                  xon, ron, far, xqn, rqn, gt_out, idx_out, gat_out, cnt_out,
                  gt_s, pos_s, v_s, ssem, rsem, lsem, gsend, grecv):
    dp = lax.axis_index('dp')
    ep = lax.axis_index('ep')
    c = ep % 2
    xc = ep // 2
    me = dp * Q + ep
    mate = (dp, xc * 2 + 1 - c)
    xnb = (dp, (1 - xc) * 2 + c)
    ynb = (1 - dp, ep)
    barrier_all(dp, ep)

    def rcopy(src, dst, k, dev):
        return pltpu.make_async_remote_copy(src_ref=src, dst_ref=dst, send_sem=ssem.at[k], recv_sem=rsem.at[k], device_id=dev, device_id_type=MESH)

    direct = [
        rcopy(x_ref, far.at[c], 0, xnb), rcopy(x_ref, xqn.at[c], 1, ynb),
        rcopy(r_ref, far.at[2 + c], 2, xnb), rcopy(r_ref, rqn.at[c], 3, ynb),
        rcopy(x_ref, xon.at[c], Q, mate), rcopy(r_ref, ron.at[c], 5, mate)]
    for cp in direct[:2] + direct[Q:5]:
        cp.start()
    local = [pltpu.make_async_copy(x_ref, xon.at[c], lsem.at[0]), pltpu.make_async_copy(r_ref, ron.at[c], lsem.at[1])]
    for cp in local:
        cp.start()

    zt = dot(wr_ref[...], x_ref[...], 1, 1)
    eio = lax.broadcasted_iota(jnp.int32, (32, NB), 0)
    sel = eio == ids_ref[0:1, :]
    for j in range(1, S):
        sel = sel | (eio == ids_ref[j:j + 1, :])
    zm = jnp.max(jnp.where(sel, zt, -jnp.inf), axis=0, keepdims=True)
    pe = jnp.where(sel, jnp.exp(zt - zm), 0.0)
    gt_out[...] = jnp.where(sel, pe / jnp.sum(pe, axis=0, keepdims=True), -1.0)
    gt_s[me] = gt_out[pl.ds(pl.multiple_of(ep * S, S), S), :]
    gcopies = []
    for k in range(1, S):
        dev = ((dp + k // Q) % 2, (ep + k % Q) % Q)
        cp = pltpu.make_async_remote_copy(src_ref=gt_out.at[pl.ds(pl.multiple_of(dev[1] * S, S), S)], dst_ref=gt_s.at[me], send_sem=gsend.at[k - 1], recv_sem=grecv.at[k - 1], device_id=dev, device_id_type=MESH)
        cp.start()
        gcopies.append(cp)
    for cp in direct[2:4] + direct[5:]:
        cp.start()
    fwd = [
        rcopy(far.at[c], far.at[c], 6, mate), rcopy(xqn.at[c], xqn.at[c], 7, mate),
        rcopy(far.at[2 + c], far.at[2 + c], S, mate), rcopy(rqn.at[c], rqn.at[c], 9, mate)]
    for k in range(2):
        direct[k].wait_recv()
        fwd[k].start()
    for cp in gcopies:
        cp.wait()

    tri = (lax.broadcasted_iota(jnp.int32, (NB, NB), 0) < lax.broadcasted_iota(jnp.int32, (NB, NB), 1)).astype(BF16)
    srow = lax.broadcasted_iota(jnp.int32, (S, NB), 0)
    tlan = lax.broadcasted_iota(jnp.int32, (S, NB), 1).astype(F32)
    for half in range(2):
        base = jnp.zeros((S, 1), F32)
        for k in range(Q):
            hd = dp if half == 0 else 1 - dp
            xx = xc if k < 2 else 1 - xc
            g = gt_s[hd * Q + xx * 2 + k % 2]
            m = g >= 0.0
            mf = m.astype(F32)
            pos = dot(mf.astype(BF16), tri) + base
            pos_s[half * Q + k] = jnp.where(m, pos, -1.0)
            base = base + jnp.sum(mf, axis=1, keepdims=True)
            g = jnp.where(m, g, 0.0)
            g1 = g.astype(BF16)
            e1 = g - g1.astype(F32)
            g2 = e1.astype(BF16)
            g3 = (e1 - g2.astype(F32)).astype(BF16)
            head = jnp.where(srow == 0, tlan, jnp.where(srow == 1, float(k), 0.0))
            v_s[half * Q + k] = jnp.concatenate([head, g1.astype(F32), g2.astype(F32), g3.astype(F32)], axis=0).astype(BF16)
        cnt_out[half] = jnp.broadcast_to(base, (S, L)).astype(jnp.int32)

    pio = lax.broadcasted_iota(jnp.int32, (NB, NB), 0).astype(F32)
    rio = lax.broadcasted_iota(jnp.int32, (32, NB), 0)
    lio = lax.broadcasted_iota(jnp.int32, (1, NB), 1)

    def list_body(he, carry):
        half = he // S
        e = he % S
        cnt_e = cnt_out[half, pl.ds(e, 1), 0:1]
        for pt in range(Q):
            acc = jnp.zeros((32, NB), F32)
            for k in range(pt, Q):
                prow = pos_s[half * Q + k, pl.ds(e, 1), :] - float(256 * pt)
                oh = (pio == prow).astype(F32).astype(BF16)
                acc = acc + dot(v_s[half * Q + k], oh, 1, 1)
            ids = (acc[0:1, :] + 256.0 * acc[1:2, :]).astype(jnp.int32)
            ids = jnp.where(lio + NB * pt < cnt_e, ids, HALF) + half * HALF
            gv = jnp.sum(jnp.where((rio >= S) & (rio % S == e), acc, 0.0), axis=0, keepdims=True)
            for q in range(2):
                idx_out[he, 2 * pt + q:2 * pt + q + 1, :] = ids[:, L * q:L * (q + 1)]
                gat_out[he, 2 * pt + q:2 * pt + q + 1, :] = gv[:, L * q:L * (q + 1)]
        return carry

    lax.fori_loop(0, 2 * S, list_body, 0)
    cnt_out[2] = jnp.full((S, L), dp, jnp.int32)
    cnt_out[3] = jnp.full((S, L), ep, jnp.int32)
    idx_out[2 * S] = jnp.zeros((S, L), jnp.int32)
    gat_out[2 * S] = jnp.zeros((S, L), F32)

    for k in range(2, Q):
        direct[k].wait_recv()
        fwd[k].start()
    for cp in local:
        cp.wait()
    direct[Q].wait_recv()
    direct[5].wait_recv()
    for cp in direct:
        cp.wait_send()
    for cp in fwd:
        cp.wait()


def load_tokens(pairs, x2, r2, tmp, sem, before, hook):
    srcs = []
    for i, (xa, ra, off) in enumerate(pairs):
        for c in range(2):
            srcs.append((xa.at[c], x2, (2 * i + c) * NB))
            srcs.append((ra.at[off + c], r2, (2 * i + c) * NB))
    copies = [pltpu.make_async_copy(src, tmp.at[i % SLOTS], sem.at[i % SLOTS]) for i, (src, _, _) in enumerate(srcs)]
    for i in range(SLOTS):
        copies[i].start()
    before()
    for i, (_, dst2, row) in enumerate(srcs):
        copies[i].wait()

        def body(b, carry, i=i, dst2=dst2, row=row):
            r0 = pl.multiple_of(b * 64, 64)
            for s in range(S):
                dst2[pl.ds((row + r0) * PT + s, 64, stride=PT), :] = tmp[i % SLOTS, pl.ds(r0, 64), L * s:L * (s + 1)].astype(F32)
            return carry

        lax.fori_loop(0, NB // 64, body, 0)
        if hook is not None and i % 2 == 0:
            hook(i // 2, tmp.at[i % SLOTS])
        if i + SLOTS < len(srcs):
            copies[i + SLOTS].start()
    for ref in (x2, r2):
        ref[row9(2 * len(pairs) * NB), :] = jnp.zeros((S, L), F32)


def strided(ref2, s):
    return ref2[pl.ds(s, T, stride=PT), :]


def zero_rows(ref2, n):
    step = n // 12

    def body(i, carry):
        ref2[pl.ds(pl.multiple_of(i * step, S), step), :] = jnp.zeros((step, L), F32)
        return carry
    lax.fori_loop(0, 12, body, 0)


def row9(t):
    return pl.ds(t * PT, S)


def row8(t):
    return pl.ds(pl.multiple_of(t * S, S), S)


def own_kernel(cnt, idx, gatv, xn, rn, far, w1, w3, w2,
               y_out, dx_out, dgt_out,
               x2, r2, ust, rsta, rstb, us, ds, o2a, o2b, d2a, d2b, dgsa, dgsb, dgd, gcs, tmp, prev, sem):
    e = pl.program_id(0)
    lane1 = lax.broadcasted_iota(jnp.int32, (1, L), 1)

    def gate_column(base):
        for q in range(2):
            gcs[L * q:L * (q + 1), :] = jnp.transpose(jnp.broadcast_to(gatv[pl.ds(base // L + q, 1), :], (L, L)))

    rsts, o2s, d2s, dgss = (rsta, rstb), (o2a, o2b), (d2a, d2b), (dgsa, dgsb)

    def gather(base, r0, n, slot):
        for r in range(n):
            t = row9(idx[base + r])
            ust[row9(r0 + r), :] = x2[t, :]
            rsts[slot][row9(r0 + r), :] = r2[t, :]

    def scatter(base, r0, n, slot):
        o2, d2, dgs = o2s[slot], d2s[slot], dgss[slot]
        mine = lane1 == base // HALF
        for c in range(0, n, S):
            ts = [idx[base + c + j] for j in range(S)]
            ys = [y_out[row8(ts[j]), :] + o2[row9(r0 + c + j), :] for j in range(S)]
            dl = [dx_out[row8(ts[j]), :] + d2[row9(r0 + c + j), :] for j in range(S)]
            gd = [dgs[pl.ds(r0 + c + j, 1), :] for j in range(S)]
            for j in range(S):
                y_out[row8(ts[j]), :] = ys[j]
                dx_out[row8(ts[j]), :] = dl[j]
                pltpu.store(dgd.at[pl.ds(ts[j], 1), :], gd[j], mask=mine)

    @pl.when(e == 0)
    def _():
        def clear():
            zero_rows(y_out, R1)
            zero_rows(dx_out, R1)
            zero_rows(o2b, XT)
            zero_rows(d2b, XT)
            dgd[...] = jnp.zeros_like(dgd)
            dgsb[...] = jnp.zeros_like(dgsb)
            prev[0] = 0
            prev[1] = 0
            gate_column(0)

        load_tokens([(xn, rn, 0), (far, far, 2)], x2, r2, tmp, sem, clear, None)

        def first(c, carry):
            gather(c * 32, c * 32, 32, 0)
            return carry
        lax.fori_loop(0, T // 32, first, 0)

    n = cnt[0, e, 0]

    def tile(k, slot):
        base = k * T
        o2, d2, rst = o2s[slot], d2s[slot], rsts[slot]
        gcol = gcs[...]
        for s in range(S):
            cs = slice(L * s, L * (s + 1))
            us[:, cs] = strided(ust, s).astype(BF16)
            ds[:, cs] = (strided(rst, s) * gcol).astype(BF16)
        more = base + T < n
        nxt = jnp.where(more, e * HALF + base + T, jnp.minimum(e + 1, NE - 1) * HALF)
        gather(nxt, 0, T, 1 - slot)
        scatter(prev[0], 0, T, 1 - slot)
        u = us[...]
        h1 = dot(u, w1[0])
        h3 = dot(u, w3[0])
        sg = jax.nn.sigmoid(h1)
        sl = h1 * sg
        a = (sl * h3).astype(BF16)
        da = dot(ds[...], w2[0], 1, 1)
        o = dot(a, w2[0]).astype(BF16).astype(F32)
        dh1 = (da * h3 * sg * (1.0 + h1 * (1.0 - sg))).astype(BF16)
        dh3 = (da * sl).astype(BF16)
        dr = (dot(dh1, w1[0], 1, 1) + dot(dh3, w3[0], 1, 1)).astype(BF16).astype(F32)
        acc = jnp.zeros((T, L), F32)
        for s in range(S):
            cs = slice(L * s, L * (s + 1))
            o2[pl.ds(s, T, stride=PT), :] = o[:, cs] * gcol
            d2[pl.ds(s, T, stride=PT), :] = dr[:, cs]
            acc = acc + o[:, cs] * strided(rst, s)
        dgss[slot][...] = jnp.broadcast_to(jnp.sum(acc, axis=1, keepdims=True), (T, L))
        prev[0] = e * HALF + base
        prev[1] = 1 - slot
        gate_column(nxt)

    def tile_body(k, carry):
        par = prev[1]
        for slot in range(2):
            pl.when(par == slot)(functools.partial(tile, k, slot))
        return carry

    lax.fori_loop(0, jnp.maximum((n + T - 1) // T, 1), tile_body, 0)

    @pl.when(e == NE - 1)
    def _():
        def last(c, carry):
            for slot in range(2):
                pl.when(prev[1] != slot)(functools.partial(scatter, prev[0] + c * 32, c * 32, 32, slot))
            return carry
        lax.fori_loop(0, T // 32, last, 0)
        xc = cnt[3, 0, 0] // 2
        tr = jnp.transpose(dgd[0:HALF, :])
        dgt_out[:, pl.ds(pl.multiple_of(xc * FF, FF), FF)] = tr[0:S, 0:FF]
        dgt_out[:, pl.ds(pl.multiple_of(FF - xc * FF, FF), FF)] = tr[0:S, FF:HALF]


def pair_kernel(yp, dxp, dgt, gt, far, near, dg_out, gt_out, rbuf, obuf, dgb, gtb, ssem, rsem, lsem, wsem, gsend, grecv):
    dp = lax.axis_index('dp')
    ep = lax.axis_index('ep')
    c = ep % 2
    me = dp * Q + ep
    mate = (dp, (ep // 2) * 2 + 1 - c)
    barrier_all(dp, ep)
    parts = [(yp, 4096), (dxp, 4096), (yp, 0), (dxp, 0)]
    outs = [far.at[0], far.at[1], near.at[0], near.at[1]]
    stores = [pltpu.make_async_copy(obuf.at[i], outs[i], wsem.at[i]) for i in range(Q)]
    sends, loads = [], []
    for i, (src, base) in enumerate(parts):
        cp = pltpu.make_async_remote_copy(
            src_ref=src.at[pl.ds(pl.multiple_of(base + (1 - c) * 2048, 2048), 2048)], dst_ref=rbuf.at[i],
            send_sem=ssem.at[i], recv_sem=rsem.at[i], device_id=mate, device_id_type=MESH)
        cp.start()
        sends.append(cp)
        ld = pltpu.make_async_copy(src.at[pl.ds(pl.multiple_of(base + c * 2048, 2048), 2048)], obuf.at[i], lsem.at[i])
        ld.start()
        loads.append(ld)
    gcopies = []
    for k in range(1, S):
        dev = ((dp + k // Q) % 2, (ep + k % Q) % Q)
        for q, (src, dst) in enumerate(((dgt, dgb), (gt, gtb))):
            cp = pltpu.make_async_remote_copy(src_ref=src, dst_ref=dst.at[me], send_sem=gsend.at[q, k - 1], recv_sem=grecv.at[q, k - 1], device_id=dev, device_id_type=MESH)
            cp.start()
            gcopies.append(cp)
    for i in range(Q):
        loads[i].wait()
        sends[i].wait_recv()

        def body(b, carry, i=i):
            s = pl.ds(pl.multiple_of(b * L, L), L)
            obuf[i, s, :] = obuf[i, s, :] + rbuf[i, s, :]
            return carry

        lax.fori_loop(0, NB // 16, body, 0)
        stores[i].start()
    for cp in gcopies:
        cp.wait()
    for cp in sends:
        cp.wait_send()
    dgb[me] = dgt[...]
    dg_out[...] = dgb[...]
    gtb[me] = gt[...]
    gt_out[...] = gtb[...]
    for cp in stores:
        cp.wait()


def grad_kernel(cnt, idx, gat, dg, gt, xon, ron, far, xqn, rqn, qfar, w1, w3, w2,
                g1, g3, g2, dw_out, dz_out, x2, r2, ust, dst, us, ds, tmp, dz_s, sem):
    e = pl.program_id(0)

    def gather(ne, nb, r0, n):
        n0 = cnt[0, ne, 0]
        a0 = ne * HALF
        a1 = NE * HALF + a0 - n0
        for r in range(n):
            q = nb + r
            q = q + jnp.where(q < n0, a0, a1)
            t = row9(idx[q])
            ust[row9(r0 + r), :] = x2[t, :]
            dst[row9(r0 + r), :] = r2[t, :] * gat[q]

    @pl.when(e == 0)
    def _():
        dp = cnt[2, 0, 0]
        ep = cnt[3, 0, 0]

        def router_grads():
            for b in range(S):
                gm = jnp.maximum(gt[b], 0.0)
                dgv = dg[32 * (b // Q):32 * (b // Q + 1), NB * (b % Q):NB * (b % Q + 1)]
                tot = jnp.sum(gm * dgv, axis=0, keepdims=True)
                dz_s[b] = (gm * (dgv - tot)).astype(BF16)
            dz_out[...] = dz_s[dp * Q + ep]
            dw_out[...] = jnp.zeros_like(dw_out)

        def add_chunk(i, xc_ref):
            hd = dp if i < Q else 1 - dp
            xx = ep // 2 if i % Q < 2 else 1 - ep // 2
            dw_out[...] += dot(dz_s[hd * Q + xx * 2 + i % 2], xc_ref[...])

        load_tokens([(xon, ron, 0), (far, far, 2), (xqn, rqn, 0), (qfar, qfar, 2)], x2, r2, tmp, sem, router_grads, add_chunk)

        def first(c, carry):
            gather(0, c * 32, c * 32, 32)
            return carry
        lax.fori_loop(0, T // 32, first, 0)

    n = cnt[0, e, 0] + cnt[1, e, 0]
    rown = lax.broadcasted_iota(jnp.int32, (T, L), 0)

    def tile(k, first):
        base = k * T
        live = rown + base < n
        for s in range(S):
            cs = slice(L * s, L * (s + 1))
            us[:, cs] = strided(ust, s).astype(BF16)
            ds[:, cs] = jnp.where(live, strided(dst, s), 0.0).astype(BF16)
        more = base + T < n
        gather(jnp.where(more, e, jnp.minimum(e + 1, NE - 1)), jnp.where(more, base + T, 0), 0, T)
        u = us[...]
        do = ds[...]
        h1 = dot(u, w1[0])
        h3 = dot(u, w3[0])
        sg = jax.nn.sigmoid(h1)
        sl = h1 * sg
        a = (sl * h3).astype(BF16)
        da = dot(do, w2[0], 1, 1)
        dh1 = (da * h3 * sg * (1.0 + h1 * (1.0 - sg))).astype(BF16)
        dh3 = (da * sl).astype(BF16)
        if first:
            g2[0] = dot(a, do, 0, 0)
            g1[0] = dot(u, dh1, 0, 0)
            g3[0] = dot(u, dh3, 0, 0)
        else:
            g2[0] += dot(a, do, 0, 0)
            g1[0] += dot(u, dh1, 0, 0)
            g3[0] += dot(u, dh3, 0, 0)

    tile(0, True)

    def tile_body(k, carry):
        tile(k, False)
        return carry

    lax.fori_loop(1, (n + T - 1) // T, tile_body, 0)


def final_kernel(x, r, near, rec, dz, wr, y_out, dx_out):
    dxr = dot(dz[...], wr[...], 0, 0)
    for s in range(S):
        cs = slice(L * s, L * (s + 1))
        rows = pl.ds(s, L, stride=S)
        y_out[:, cs] = x[:, cs].astype(F32) + (near[0, rows, :] + rec[0, rows, :])
        dx_out[:, cs] = r[:, cs].astype(F32) + dxr[:, cs] + (near[1, rows, :] + rec[1, rows, :])


def solution(mesh):
    axes = ('dp', 'ep')
    sds = jax.ShapeDtypeStruct

    def local_step(tokens, w_router, w_gate, w_up, w_down, top_ids, r_proj):
        near = sds((2, NB, D), BF16)
        dma = pltpu.SemaphoreType.DMA
        xon, ron, far, xqn, rqn, gto, idx, gat, cnt = pl.pallas_call(
            gather_kernel,
            out_shape=[near] * 2 + [sds((Q, NB, D), BF16)] + [near] * 2 + [sds((32, NB), F32), sds((NL, S, L), jnp.int32), sds((NL, S, L), F32), sds((Q, S, L), jnp.int32)],
            in_specs=[vspec()] * Q,
            out_specs=[aspec()] * 5 + [vspec()] * Q,
            scratch_shapes=[pltpu.VMEM((S, S, NB), F32), pltpu.VMEM((S, S, NB), F32), pltpu.VMEM((S, 32, NB), BF16),
                            dma((10,)), dma((10,)), dma((2,)), dma((7,)), dma((7,))],
            compiler_params=pltpu.CompilerParams(collective_id=0, has_side_effects=True),
            name='k0_gather',
        )(tokens, r_proj, top_ids.T, w_router.T)

        idx1 = idx.reshape(-1)
        gat1 = gat.reshape(-1)
        xswap = [(0, 2), (2, 0), (1, 3), (3, 1)]
        qfar = lax.ppermute(far, 'dp', [(0, 1), (1, 0)])

        wspec = [pl.BlockSpec((1, D, FF), lambda e: (e, 0, 0)), pl.BlockSpec((1, D, FF), lambda e: (e, 0, 0)), pl.BlockSpec((1, FF, D), lambda e: (e, 0, 0))]
        part = sds((R1, L), F32)
        pspec = pl.BlockSpec((R1, L), lambda e: (0, 0))
        yp, dxp, dgt = pl.pallas_call(
            own_kernel,
            grid=(NE,),
            out_shape=[part, part, sds((S, HALF), F32)],
            in_specs=[sspec()] * 2 + [vspec()] + [aspec()] * 3 + wspec,
            out_specs=[pspec, pspec, pl.BlockSpec((S, HALF), lambda e: (0, 0))],
            scratch_shapes=[pltpu.VMEM((X1, L), F32)] * 2 + [pltpu.VMEM((XT, L), F32)] * 3 + [pltpu.VMEM((T, D), BF16)] * 2
            + [pltpu.VMEM((XT, L), F32)] * Q + [pltpu.VMEM((T, L), F32)] * 2 + [pltpu.VMEM((RB, L), F32), pltpu.VMEM((T, L), F32),
               pltpu.VMEM((SLOTS, NB, D), BF16), pltpu.SMEM((2,), jnp.int32), dma((SLOTS,))],
            compiler_params=pltpu.CompilerParams(vmem_limit_bytes=VMEM_MAX, dimension_semantics=('arbitrary',)),
            cost_estimate=pl.CostEstimate(flops=20 * 10 ** 9, bytes_accessed=40 * 10 ** 6, transcendentals=0),
            name='k1_own',
        )(cnt, idx1, gat.reshape(NL * S, L), xon, ron, far, w_gate, w_up, w_down)

        quarter = sds((2, NB * S, L), F32)
        farsum, near2, dg, gt = pl.pallas_call(
            pair_kernel,
            out_shape=[quarter] * 2 + [sds((S, S, HALF), F32), sds((S, 32, NB), F32)],
            in_specs=[aspec(), aspec(), vspec(), vspec()],
            out_specs=[aspec()] * 2 + [vspec()] * 2,
            scratch_shapes=[pltpu.VMEM((Q, NB * S, L), F32), pltpu.VMEM((Q, NB * S, L), F32), pltpu.VMEM((S, S, HALF), F32), pltpu.VMEM((S, 32, NB), F32),
                            dma((Q,)), dma((Q,)), dma((Q,)), dma((Q,)), dma((2, 7)), dma((2, 7))],
            compiler_params=pltpu.CompilerParams(collective_id=1, has_side_effects=True),
            name='k2_pair',
        )(yp, dxp, dgt, gto)

        rec = lax.ppermute(farsum, 'ep', xswap)

        gspec = [pl.BlockSpec((1, D, FF), lambda e: (e, 0, 0)), pl.BlockSpec((1, D, FF), lambda e: (e, 0, 0)), pl.BlockSpec((1, FF, D), lambda e: (e, 0, 0))]
        grad_gate, grad_up, grad_down, dwt, dz = pl.pallas_call(
            grad_kernel,
            grid=(NE,),
            out_shape=[sds((NE, D, FF), F32), sds((NE, D, FF), F32), sds((NE, FF, D), F32), sds((32, D), F32), sds((32, NB), BF16)],
            in_specs=[sspec()] * 3 + [vspec()] * 2 + [aspec()] * 6 + wspec,
            out_specs=gspec + [pl.BlockSpec((32, D), lambda e: (0, 0)), pl.BlockSpec((32, NB), lambda e: (0, 0))],
            scratch_shapes=[pltpu.VMEM((X2, L), F32)] * 2 + [pltpu.VMEM((XT, L), F32)] * 2 + [pltpu.VMEM((T, D), BF16)] * 2
            + [pltpu.VMEM((SLOTS, NB, D), BF16), pltpu.VMEM((S, 32, NB), BF16), dma((SLOTS,))],
            compiler_params=pltpu.CompilerParams(vmem_limit_bytes=VMEM_MAX, dimension_semantics=('arbitrary',)),
            cost_estimate=pl.CostEstimate(flops=30 * 10 ** 9, bytes_accessed=90 * 10 ** 6, transcendentals=0),
            name='k3_grad',
        )(cnt, idx1, gat1, dg.reshape(64, HALF), gt, xon, ron, far, xqn, rqn, qfar, w_gate, w_up, w_down)

        rspec = pl.BlockSpec((L, D), lambda i: (i, 0))
        qspec = pl.BlockSpec((2, L * S, L), lambda i: (0, i, 0))
        y, dx = pl.pallas_call(
            final_kernel,
            grid=(2,),
            out_shape=[sds((NB, D), F32), sds((NB, D), F32)],
            in_specs=[rspec, rspec, qspec, qspec, pl.BlockSpec((32, L), lambda i: (0, i)), pl.BlockSpec((32, D), lambda i: (0, 0))],
            out_specs=[rspec, rspec],
            compiler_params=pltpu.CompilerParams(vmem_limit_bytes=VMEM_MAX),
            name='k4_final',
        )(tokens, r_proj, near2, rec, dz, w_router.T)
        return y, dx, grad_gate, grad_up, grad_down, dwt.T

    tok_spec = P(axes, None)
    exp_spec = P('ep', None, None)
    return jax.shard_map(local_step, mesh=mesh, in_specs=(tok_spec, P(), exp_spec, exp_spec, exp_spec, tok_spec, tok_spec), out_specs=(tok_spec, tok_spec, exp_spec, exp_spec, exp_spec, P()), check_vma=False)
```

```python
import functools

import jax
import jax.numpy as jnp
from jax import lax
from jax.experimental import pallas as pl
from jax.experimental.pallas import tpu as pltpu
from jax.sharding import PartitionSpec as P

F32 = jnp.float32
BF16 = jnp.bfloat16
MESH = pl.DeviceIdType.MESH
VMEM_MAX = 63 * 1024 * 1024
T = 256
NB = 256
HALF = 1024
D = 1024
FF = 512
NE = 8
NL = 17
SLOTS = 8
PT = 9
S = 8
L = 128
Q = 4
RB = 1032
R1 = 8256
R2 = 16448
X1 = 9288
X2 = 18504
XT = 2304


def dot(a, b, ca=1, cb=0):
    return lax.dot_general(a, b, (((ca,), (cb,)), ((), ())), preferred_element_type=F32)


def vspec():
    return pl.BlockSpec(memory_space=pltpu.VMEM)


def aspec():
    return pl.BlockSpec(memory_space=pl.ANY)


def sspec():
    return pl.BlockSpec(memory_space=pltpu.SMEM)


def barrier_all(dp, ep):
    bar = pltpu.get_barrier_semaphore()
    for k in range(1, S):
        pl.semaphore_signal(bar, inc=1, device_id=((dp + k // Q) % 2, (ep + k % Q) % Q), device_id_type=MESH)
    pl.semaphore_wait(bar, 7)


def gather_kernel(x_ref, r_ref, ids_ref, wr_ref,
                  xon, ron, far, xqn, rqn, gt_out, idx_out, gat_out, cnt_out,
                  gt_s, pos_s, v_s, ssem, rsem, lsem, gsend, grecv):
    dp = lax.axis_index('dp')
    ep = lax.axis_index('ep')
    c = ep % 2
    xc = ep // 2
    me = dp * Q + ep
    mate = (dp, xc * 2 + 1 - c)
    xnb = (dp, (1 - xc) * 2 + c)
    ynb = (1 - dp, ep)
    barrier_all(dp, ep)

    def rcopy(src, dst, k, dev):
        return pltpu.make_async_remote_copy(src_ref=src, dst_ref=dst, send_sem=ssem.at[k], recv_sem=rsem.at[k], device_id=dev, device_id_type=MESH)

    direct = [
        rcopy(x_ref, far.at[c], 0, xnb), rcopy(x_ref, xqn.at[c], 1, ynb),
        rcopy(r_ref, far.at[2 + c], 2, xnb), rcopy(r_ref, rqn.at[c], 3, ynb),
        rcopy(x_ref, xon.at[c], Q, mate), rcopy(r_ref, ron.at[c], 5, mate)]
    for cp in direct[:2] + direct[Q:5]:
        cp.start()
    local = [pltpu.make_async_copy(x_ref, xon.at[c], lsem.at[0]), pltpu.make_async_copy(r_ref, ron.at[c], lsem.at[1])]
    for cp in local:
        cp.start()

    zt = dot(wr_ref[...], x_ref[...], 1, 1)
    eio = lax.broadcasted_iota(jnp.int32, (32, NB), 0)
    sel = eio == ids_ref[0:1, :]
    for j in range(1, S):
        sel = sel | (eio == ids_ref[j:j + 1, :])
    zm = jnp.max(jnp.where(sel, zt, -jnp.inf), axis=0, keepdims=True)
    pe = jnp.where(sel, jnp.exp(zt - zm), 0.0)
    gt_out[...] = jnp.where(sel, pe / jnp.sum(pe, axis=0, keepdims=True), -1.0)
    gt_s[me] = gt_out[pl.ds(pl.multiple_of(ep * S, S), S), :]
    gcopies = []
    for k in range(1, S):
        dev = ((dp + k // Q) % 2, (ep + k % Q) % Q)
        cp = pltpu.make_async_remote_copy(src_ref=gt_out.at[pl.ds(pl.multiple_of(dev[1] * S, S), S)], dst_ref=gt_s.at[me], send_sem=gsend.at[k - 1], recv_sem=grecv.at[k - 1], device_id=dev, device_id_type=MESH)
        cp.start()
        gcopies.append(cp)
    for cp in direct[2:4] + direct[5:]:
        cp.start()
    fwd = [
        rcopy(far.at[c], far.at[c], 6, mate), rcopy(xqn.at[c], xqn.at[c], 7, mate),
        rcopy(far.at[2 + c], far.at[2 + c], S, mate), rcopy(rqn.at[c], rqn.at[c], 9, mate)]
    for k in range(2):
        direct[k].wait_recv()
        fwd[k].start()
    for cp in gcopies:
        cp.wait()

    tri = (lax.broadcasted_iota(jnp.int32, (NB, NB), 0) < lax.broadcasted_iota(jnp.int32, (NB, NB), 1)).astype(BF16)
    srow = lax.broadcasted_iota(jnp.int32, (S, NB), 0)
    tlan = lax.broadcasted_iota(jnp.int32, (S, NB), 1).astype(F32)
    for half in range(2):
        base = jnp.zeros((S, 1), F32)
        for k in range(Q):
            hd = dp if half == 0 else 1 - dp
            xx = xc if k < 2 else 1 - xc
            g = gt_s[hd * Q + xx * 2 + k % 2]
            m = g >= 0.0
            mf = m.astype(F32)
            pos = dot(mf.astype(BF16), tri) + base
            pos_s[half * Q + k] = jnp.where(m, pos, -1.0)
            base = base + jnp.sum(mf, axis=1, keepdims=True)
            g = jnp.where(m, g, 0.0)
            g1 = g.astype(BF16)
            e1 = g - g1.astype(F32)
            g2 = e1.astype(BF16)
            g3 = (e1 - g2.astype(F32)).astype(BF16)
            head = jnp.where(srow == 0, tlan, jnp.where(srow == 1, float(k), 0.0))
            v_s[half * Q + k] = jnp.concatenate([head, g1.astype(F32), g2.astype(F32), g3.astype(F32)], axis=0).astype(BF16)
        cnt_out[half] = jnp.broadcast_to(base, (S, L)).astype(jnp.int32)

    pio = lax.broadcasted_iota(jnp.int32, (NB, NB), 0).astype(F32)
    rio = lax.broadcasted_iota(jnp.int32, (32, NB), 0)
    lio = lax.broadcasted_iota(jnp.int32, (1, NB), 1)

    def list_body(he, carry):
        half = he // S
        e = he % S
        cnt_e = cnt_out[half, pl.ds(e, 1), 0:1]
        for pt in range(Q):
            acc = jnp.zeros((32, NB), F32)
            for k in range(pt, Q):
                prow = pos_s[half * Q + k, pl.ds(e, 1), :] - float(256 * pt)
                oh = (pio == prow).astype(F32).astype(BF16)
                acc = acc + dot(v_s[half * Q + k], oh, 1, 1)
            ids = (acc[0:1, :] + 256.0 * acc[1:2, :]).astype(jnp.int32)
            ids = jnp.where(lio + NB * pt < cnt_e, ids, HALF) + half * HALF
            gv = jnp.sum(jnp.where((rio >= S) & (rio % S == e), acc, 0.0), axis=0, keepdims=True)
            for q in range(2):
                idx_out[he, 2 * pt + q:2 * pt + q + 1, :] = ids[:, L * q:L * (q + 1)]
                gat_out[he, 2 * pt + q:2 * pt + q + 1, :] = gv[:, L * q:L * (q + 1)]
        return carry

    lax.fori_loop(0, 2 * S, list_body, 0)
    cnt_out[2] = jnp.full((S, L), dp, jnp.int32)
    cnt_out[3] = jnp.full((S, L), ep, jnp.int32)
    idx_out[2 * S] = jnp.zeros((S, L), jnp.int32)
    gat_out[2 * S] = jnp.zeros((S, L), F32)

    for k in range(2, Q):
        direct[k].wait_recv()
        fwd[k].start()
    for cp in local:
        cp.wait()
    direct[Q].wait_recv()
    direct[5].wait_recv()
    for cp in direct:
        cp.wait_send()
    for cp in fwd:
        cp.wait()


def load_tokens(pairs, x2, r2, tmp, sem, before, hook):
    srcs = []
    for i, (xa, ra, off) in enumerate(pairs):
        for c in range(2):
            srcs.append((xa.at[c], x2, (2 * i + c) * NB))
            srcs.append((ra.at[off + c], r2, (2 * i + c) * NB))
    copies = [pltpu.make_async_copy(src, tmp.at[i % SLOTS], sem.at[i % SLOTS]) for i, (src, _, _) in enumerate(srcs)]
    for i in range(SLOTS):
        copies[i].start()
    before()
    for i, (_, dst2, row) in enumerate(srcs):
        copies[i].wait()

        def body(b, carry, i=i, dst2=dst2, row=row):
            r0 = pl.multiple_of(b * 64, 64)
            for s in range(S):
                dst2[pl.ds((row + r0) * PT + s, 64, stride=PT), :] = tmp[i % SLOTS, pl.ds(r0, 64), L * s:L * (s + 1)].astype(F32)
            return carry

        lax.fori_loop(0, NB // 64, body, 0)
        if hook is not None and i % 2 == 0:
            hook(i // 2, tmp.at[i % SLOTS])
        if i + SLOTS < len(srcs):
            copies[i + SLOTS].start()
    for ref in (x2, r2):
        ref[row9(2 * len(pairs) * NB), :] = jnp.zeros((S, L), F32)


def strided(ref2, s):
    return ref2[pl.ds(s, T, stride=PT), :]


def zero_rows(ref2, n):
    step = n // 12

    def body(i, carry):
        ref2[pl.ds(pl.multiple_of(i * step, S), step), :] = jnp.zeros((step, L), F32)
        return carry
    lax.fori_loop(0, 12, body, 0)


def row9(t):
    return pl.ds(t * PT, S)


def row8(t):
    return pl.ds(pl.multiple_of(t * S, S), S)


def own_kernel(cnt, idx, gatv, xn, rn, far, w1, w3, w2,
               mine, mate, far_out, dgt_out,
               y_out, dx_out, x2, r2, ust, rsta, rstb, us, ds, o2a, o2b, d2a, d2b, dgsa, dgsb, dgd, gcs, tmp, prev, sem, osem):
    e = pl.program_id(0)
    lane1 = lax.broadcasted_iota(jnp.int32, (1, L), 1)

    def gate_column(base):
        for q in range(2):
            gcs[L * q:L * (q + 1), :] = jnp.transpose(jnp.broadcast_to(gatv[pl.ds(base // L + q, 1), :], (L, L)))

    rsts, o2s, d2s, dgss = (rsta, rstb), (o2a, o2b), (d2a, d2b), (dgsa, dgsb)

    def gather(base, r0, n, slot):
        for r in range(n):
            t = row9(idx[base + r])
            ust[row9(r0 + r), :] = x2[t, :]
            rsts[slot][row9(r0 + r), :] = r2[t, :]

    def scatter(base, r0, n, slot):
        o2, d2, dgs = o2s[slot], d2s[slot], dgss[slot]
        mine = lane1 == base // HALF
        for c in range(0, n, S):
            ts = [idx[base + c + j] for j in range(S)]
            ys = [y_out[row8(ts[j]), :] + o2[row9(r0 + c + j), :] for j in range(S)]
            dl = [dx_out[row8(ts[j]), :] + d2[row9(r0 + c + j), :] for j in range(S)]
            gd = [dgs[pl.ds(r0 + c + j, 1), :] for j in range(S)]
            for j in range(S):
                y_out[row8(ts[j]), :] = ys[j]
                dx_out[row8(ts[j]), :] = dl[j]
                pltpu.store(dgd.at[pl.ds(ts[j], 1), :], gd[j], mask=mine)

    @pl.when(e == 0)
    def _():
        def clear():
            zero_rows(y_out, R1)
            zero_rows(dx_out, R1)
            zero_rows(o2b, XT)
            zero_rows(d2b, XT)
            dgd[...] = jnp.zeros_like(dgd)
            dgsb[...] = jnp.zeros_like(dgsb)
            prev[0] = 0
            prev[1] = 0
            gate_column(0)

        load_tokens([(xn, rn, 0), (far, far, 2)], x2, r2, tmp, sem, clear, None)

        def first(c, carry):
            gather(c * 32, c * 32, 32, 0)
            return carry
        lax.fori_loop(0, T // 32, first, 0)

    n = cnt[0, e, 0]

    def tile(k, slot):
        base = k * T
        o2, d2, rst = o2s[slot], d2s[slot], rsts[slot]
        gcol = gcs[...]
        for s in range(S):
            cs = slice(L * s, L * (s + 1))
            us[:, cs] = strided(ust, s).astype(BF16)
            ds[:, cs] = (strided(rst, s) * gcol).astype(BF16)
        more = base + T < n
        nxt = jnp.where(more, e * HALF + base + T, jnp.minimum(e + 1, NE - 1) * HALF)
        gather(nxt, 0, T, 1 - slot)
        scatter(prev[0], 0, T, 1 - slot)
        u = us[...]
        h1 = dot(u, w1[0])
        h3 = dot(u, w3[0])
        sg = jax.nn.sigmoid(h1)
        sl = h1 * sg
        a = (sl * h3).astype(BF16)
        da = dot(ds[...], w2[0], 1, 1)
        o = dot(a, w2[0]).astype(BF16).astype(F32)
        dh1 = (da * h3 * sg * (1.0 + h1 * (1.0 - sg))).astype(BF16)
        dh3 = (da * sl).astype(BF16)
        dr = (dot(dh1, w1[0], 1, 1) + dot(dh3, w3[0], 1, 1)).astype(BF16).astype(F32)
        acc = jnp.zeros((T, L), F32)
        for s in range(S):
            cs = slice(L * s, L * (s + 1))
            o2[pl.ds(s, T, stride=PT), :] = o[:, cs] * gcol
            d2[pl.ds(s, T, stride=PT), :] = dr[:, cs]
            acc = acc + o[:, cs] * strided(rst, s)
        dgss[slot][...] = jnp.broadcast_to(jnp.sum(acc, axis=1, keepdims=True), (T, L))
        prev[0] = e * HALF + base
        prev[1] = 1 - slot
        gate_column(nxt)

    def tile_body(k, carry):
        par = prev[1]
        for slot in range(2):
            pl.when(par == slot)(functools.partial(tile, k, slot))
        return carry

    lax.fori_loop(0, jnp.maximum((n + T - 1) // T, 1), tile_body, 0)

    @pl.when(e == NE - 1)
    def _():
        def last(c, carry):
            for slot in range(2):
                pl.when(prev[1] != slot)(functools.partial(scatter, prev[0] + c * 32, c * 32, 32, slot))
            return carry
        lax.fori_loop(0, T // 32, last, 0)
        c = cnt[3, 0, 0] % 2
        outs = []
        for i, src in enumerate((y_out, dx_out)):
            for q, dst in enumerate((mine, mate)):
                row = pl.multiple_of((c if q == 0 else 1 - c) * NB * S, NB * S)
                outs.append(pltpu.make_async_copy(src.at[pl.ds(row, NB * S)], dst.at[i], osem.at[i, q]))
            outs.append(pltpu.make_async_copy(src.at[pl.ds(FF * S, FF * S)], far_out.at[i], osem.at[i, 2]))
        for cp in outs:
            cp.start()
        xc = cnt[3, 0, 0] // 2
        tr = jnp.transpose(dgd[0:HALF, :])
        dgt_out[:, pl.ds(pl.multiple_of(xc * FF, FF), FF)] = tr[0:S, 0:FF]
        dgt_out[:, pl.ds(pl.multiple_of(FF - xc * FF, FF), FF)] = tr[0:S, FF:HALF]
        for cp in outs:
            cp.wait()


def pair_kernel(fpart, dgt, gt, far, dg_out, gt_out, rbuf, obuf, dgb, gtb, ssem, rsem, lsem, wsem, gsend, grecv):
    dp = lax.axis_index('dp')
    ep = lax.axis_index('ep')
    c = ep % 2
    me = dp * Q + ep
    mate = (dp, (ep // 2) * 2 + 1 - c)
    barrier_all(dp, ep)
    parts = [fpart.at[0], fpart.at[1]]
    stores = [pltpu.make_async_copy(obuf.at[i], far.at[i], wsem.at[i]) for i in range(2)]
    sends, loads = [], []
    for i, src in enumerate(parts):
        cp = pltpu.make_async_remote_copy(
            src_ref=src.at[pl.ds(pl.multiple_of((1 - c) * NB * S, NB * S), NB * S)], dst_ref=rbuf.at[i],
            send_sem=ssem.at[i], recv_sem=rsem.at[i], device_id=mate, device_id_type=MESH)
        cp.start()
        sends.append(cp)
        ld = pltpu.make_async_copy(src.at[pl.ds(pl.multiple_of(c * NB * S, NB * S), NB * S)], obuf.at[i], lsem.at[i])
        ld.start()
        loads.append(ld)
    gcopies = []
    for k in range(1, S):
        dev = ((dp + k // Q) % 2, (ep + k % Q) % Q)
        for q, (src, dst) in enumerate(((dgt, dgb), (gt, gtb))):
            cp = pltpu.make_async_remote_copy(src_ref=src, dst_ref=dst.at[me], send_sem=gsend.at[q, k - 1], recv_sem=grecv.at[q, k - 1], device_id=dev, device_id_type=MESH)
            cp.start()
            gcopies.append(cp)
    for i in range(2):
        loads[i].wait()
        sends[i].wait_recv()

        def body(b, carry, i=i):
            s = pl.ds(pl.multiple_of(b * L, L), L)
            obuf[i, s, :] = obuf[i, s, :] + rbuf[i, s, :]
            return carry

        lax.fori_loop(0, NB // 16, body, 0)
        stores[i].start()
    for cp in gcopies:
        cp.wait()
    for cp in sends:
        cp.wait_send()
    dgb[me] = dgt[...]
    dg_out[...] = dgb[...]
    gtb[me] = gt[...]
    gt_out[...] = gtb[...]
    for cp in stores:
        cp.wait()


def grad_kernel(cnt, idx, gat, dg, gt, xon, ron, far, xqn, rqn, qfar, w1, w3, w2,
                g1, g3, g2, dw_out, dz_out, x2, r2, ust, dst, us, ds, tmp, dz_s, sem):
    e = pl.program_id(0)

    def gather(ne, nb, r0, n):
        n0 = cnt[0, ne, 0]
        a0 = ne * HALF
        a1 = NE * HALF + a0 - n0
        for r in range(n):
            q = nb + r
            q = q + jnp.where(q < n0, a0, a1)
            t = row9(idx[q])
            ust[row9(r0 + r), :] = x2[t, :]
            dst[row9(r0 + r), :] = r2[t, :] * gat[q]

    @pl.when(e == 0)
    def _():
        dp = cnt[2, 0, 0]
        ep = cnt[3, 0, 0]

        def router_grads():
            for b in range(S):
                gm = jnp.maximum(gt[b], 0.0)
                dgv = dg[32 * (b // Q):32 * (b // Q + 1), NB * (b % Q):NB * (b % Q + 1)]
                tot = jnp.sum(gm * dgv, axis=0, keepdims=True)
                dz_s[b] = (gm * (dgv - tot)).astype(BF16)
            dz_out[...] = dz_s[dp * Q + ep]
            dw_out[...] = jnp.zeros_like(dw_out)

        def add_chunk(i, xc_ref):
            hd = dp if i < Q else 1 - dp
            xx = ep // 2 if i % Q < 2 else 1 - ep // 2
            dw_out[...] += dot(dz_s[hd * Q + xx * 2 + i % 2], xc_ref[...])

        load_tokens([(xon, ron, 0), (far, far, 2), (xqn, rqn, 0), (qfar, qfar, 2)], x2, r2, tmp, sem, router_grads, add_chunk)

        def first(c, carry):
            gather(0, c * 32, c * 32, 32)
            return carry
        lax.fori_loop(0, T // 32, first, 0)

    n = cnt[0, e, 0] + cnt[1, e, 0]
    rown = lax.broadcasted_iota(jnp.int32, (T, L), 0)

    def tile(k, first):
        base = k * T
        live = rown + base < n
        for s in range(S):
            cs = slice(L * s, L * (s + 1))
            us[:, cs] = strided(ust, s).astype(BF16)
            ds[:, cs] = jnp.where(live, strided(dst, s), 0.0).astype(BF16)
        more = base + T < n
        gather(jnp.where(more, e, jnp.minimum(e + 1, NE - 1)), jnp.where(more, base + T, 0), 0, T)
        u = us[...]
        do = ds[...]
        h1 = dot(u, w1[0])
        h3 = dot(u, w3[0])
        sg = jax.nn.sigmoid(h1)
        sl = h1 * sg
        a = (sl * h3).astype(BF16)
        da = dot(do, w2[0], 1, 1)
        dh1 = (da * h3 * sg * (1.0 + h1 * (1.0 - sg))).astype(BF16)
        dh3 = (da * sl).astype(BF16)
        if first:
            g2[0] = dot(a, do, 0, 0)
            g1[0] = dot(u, dh1, 0, 0)
            g3[0] = dot(u, dh3, 0, 0)
        else:
            g2[0] += dot(a, do, 0, 0)
            g1[0] += dot(u, dh1, 0, 0)
            g3[0] += dot(u, dh3, 0, 0)

    tile(0, True)

    def tile_body(k, carry):
        tile(k, False)
        return carry

    lax.fori_loop(1, (n + T - 1) // T, tile_body, 0)


def final_kernel(x, r, mine, mate, rec, dz, wr, y_out, dx_out):
    dxr = dot(dz[...], wr[...], 0, 0)
    for s in range(S):
        cs = slice(L * s, L * (s + 1))
        rows = pl.ds(s, L, stride=S)
        y_out[:, cs] = x[:, cs].astype(F32) + ((mine[0, rows, :] + mate[0, rows, :]) + rec[0, rows, :])
        dx_out[:, cs] = r[:, cs].astype(F32) + dxr[:, cs] + ((mine[1, rows, :] + mate[1, rows, :]) + rec[1, rows, :])


def solution(mesh):
    axes = ('dp', 'ep')
    sds = jax.ShapeDtypeStruct

    def local_step(tokens, w_router, w_gate, w_up, w_down, top_ids, r_proj):
        near = sds((2, NB, D), BF16)
        dma = pltpu.SemaphoreType.DMA
        xon, ron, far, xqn, rqn, gto, idx, gat, cnt = pl.pallas_call(
            gather_kernel,
            out_shape=[near] * 2 + [sds((Q, NB, D), BF16)] + [near] * 2 + [sds((32, NB), F32), sds((NL, S, L), jnp.int32), sds((NL, S, L), F32), sds((Q, S, L), jnp.int32)],
            in_specs=[vspec()] * Q,
            out_specs=[aspec()] * 5 + [vspec()] * Q,
            scratch_shapes=[pltpu.VMEM((S, S, NB), F32), pltpu.VMEM((S, S, NB), F32), pltpu.VMEM((S, 32, NB), BF16),
                            dma((10,)), dma((10,)), dma((2,)), dma((7,)), dma((7,))],
            compiler_params=pltpu.CompilerParams(collective_id=0, has_side_effects=True),
            name='k0_gather',
        )(tokens, r_proj, top_ids.T, w_router.T)

        idx1 = idx.reshape(-1)
        gat1 = gat.reshape(-1)
        xswap = [(0, 2), (2, 0), (1, 3), (3, 1)]
        qfar = lax.ppermute(far, 'dp', [(0, 1), (1, 0)])

        wspec = [pl.BlockSpec((1, D, FF), lambda e: (e, 0, 0)), pl.BlockSpec((1, D, FF), lambda e: (e, 0, 0)), pl.BlockSpec((1, FF, D), lambda e: (e, 0, 0))]
        quarter = sds((2, NB * S, L), F32)
        mine, mate, fpart, dgt = pl.pallas_call(
            own_kernel,
            grid=(NE,),
            out_shape=[quarter, quarter, sds((2, FF * S, L), F32), sds((S, HALF), F32)],
            in_specs=[sspec()] * 2 + [vspec()] + [aspec()] * 3 + wspec,
            out_specs=[aspec()] * 3 + [pl.BlockSpec((S, HALF), lambda e: (0, 0))],
            scratch_shapes=[pltpu.VMEM((R1, L), F32)] * 2 + [pltpu.VMEM((X1, L), F32)] * 2 + [pltpu.VMEM((XT, L), F32)] * 3 + [pltpu.VMEM((T, D), BF16)] * 2
            + [pltpu.VMEM((XT, L), F32)] * Q + [pltpu.VMEM((T, L), F32)] * 2 + [pltpu.VMEM((RB, L), F32), pltpu.VMEM((T, L), F32),
               pltpu.VMEM((SLOTS, NB, D), BF16), pltpu.SMEM((2,), jnp.int32), dma((SLOTS,)), dma((2, 3))],
            compiler_params=pltpu.CompilerParams(vmem_limit_bytes=VMEM_MAX, dimension_semantics=('arbitrary',)),
            cost_estimate=pl.CostEstimate(flops=20 * 10 ** 9, bytes_accessed=40 * 10 ** 6, transcendentals=0),
            name='k1_own',
        )(cnt, idx1, gat.reshape(NL * S, L), xon, ron, far, w_gate, w_up, w_down)

        matesum = lax.ppermute(mate, 'ep', [(0, 1), (1, 0), (2, 3), (3, 2)])
        farsum, dg, gt = pl.pallas_call(
            pair_kernel,
            out_shape=[quarter, sds((S, S, HALF), F32), sds((S, 32, NB), F32)],
            in_specs=[aspec(), vspec(), vspec()],
            out_specs=[aspec()] + [vspec()] * 2,
            scratch_shapes=[pltpu.VMEM((2, NB * S, L), F32), pltpu.VMEM((2, NB * S, L), F32), pltpu.VMEM((S, S, HALF), F32), pltpu.VMEM((S, 32, NB), F32),
                            dma((2,)), dma((2,)), dma((2,)), dma((2,)), dma((2, 7)), dma((2, 7))],
            compiler_params=pltpu.CompilerParams(collective_id=1, has_side_effects=True),
            name='k2_pair',
        )(fpart, dgt, gto)

        rec = lax.ppermute(farsum, 'ep', xswap)

        gspec = [pl.BlockSpec((1, D, FF), lambda e: (e, 0, 0)), pl.BlockSpec((1, D, FF), lambda e: (e, 0, 0)), pl.BlockSpec((1, FF, D), lambda e: (e, 0, 0))]
        grad_gate, grad_up, grad_down, dwt, dz = pl.pallas_call(
            grad_kernel,
            grid=(NE,),
            out_shape=[sds((NE, D, FF), F32), sds((NE, D, FF), F32), sds((NE, FF, D), F32), sds((32, D), F32), sds((32, NB), BF16)],
            in_specs=[sspec()] * 3 + [vspec()] * 2 + [aspec()] * 6 + wspec,
            out_specs=gspec + [pl.BlockSpec((32, D), lambda e: (0, 0)), pl.BlockSpec((32, NB), lambda e: (0, 0))],
            scratch_shapes=[pltpu.VMEM((X2, L), F32)] * 2 + [pltpu.VMEM((XT, L), F32)] * 2 + [pltpu.VMEM((T, D), BF16)] * 2
            + [pltpu.VMEM((SLOTS, NB, D), BF16), pltpu.VMEM((S, 32, NB), BF16), dma((SLOTS,))],
            compiler_params=pltpu.CompilerParams(vmem_limit_bytes=VMEM_MAX, dimension_semantics=('arbitrary',)),
            cost_estimate=pl.CostEstimate(flops=30 * 10 ** 9, bytes_accessed=90 * 10 ** 6, transcendentals=0),
            name='k3_grad',
        )(cnt, idx1, gat1, dg.reshape(64, HALF), gt, xon, ron, far, xqn, rqn, qfar, w_gate, w_up, w_down)

        rspec = pl.BlockSpec((L, D), lambda i: (i, 0))
        qspec = pl.BlockSpec((2, L * S, L), lambda i: (0, i, 0))
        y, dx = pl.pallas_call(
            final_kernel,
            grid=(2,),
            out_shape=[sds((NB, D), F32), sds((NB, D), F32)],
            in_specs=[rspec, rspec, qspec, qspec, qspec, pl.BlockSpec((32, L), lambda i: (0, i)), pl.BlockSpec((32, D), lambda i: (0, 0))],
            out_specs=[rspec, rspec],
            compiler_params=pltpu.CompilerParams(vmem_limit_bytes=VMEM_MAX),
            name='k4_final',
        )(tokens, r_proj, mine, matesum, rec, dz, w_router.T)
        return y, dx, grad_gate, grad_up, grad_down, dwt.T

    tok_spec = P(axes, None)
    exp_spec = P('ep', None, None)
    return jax.shard_map(local_step, mesh=mesh, in_specs=(tok_spec, P(), exp_spec, exp_spec, exp_spec, tok_spec, tok_spec), out_specs=(tok_spec, tok_spec, exp_spec, exp_spec, exp_spec, P()), check_vma=False)
```

```python
import functools

import jax
import jax.numpy as jnp
from jax import lax
from jax.experimental import pallas as pl
from jax.experimental.pallas import tpu as pltpu
from jax.sharding import PartitionSpec as P

F32 = jnp.float32
BF16 = jnp.bfloat16
MESH = pl.DeviceIdType.MESH
VMEM_MAX = 63 * 1024 * 1024
T = 256
NB = 256
HALF = 1024
D = 1024
FF = 512
NE = 8
NL = 17
SLOTS = 8
PT = 9
S = 8
L = 128
Q = 4
RB = 1032
R1 = 8256
R2 = 16448
X1 = 9288
X2 = 18504
XT = 2304


def dot(a, b, ca=1, cb=0):
    return lax.dot_general(a, b, (((ca,), (cb,)), ((), ())), preferred_element_type=F32)


def vspec():
    return pl.BlockSpec(memory_space=pltpu.VMEM)


def aspec():
    return pl.BlockSpec(memory_space=pl.ANY)


def sspec():
    return pl.BlockSpec(memory_space=pltpu.SMEM)


def barrier_all(dp, ep):
    bar = pltpu.get_barrier_semaphore()
    for k in range(1, S):
        pl.semaphore_signal(bar, inc=1, device_id=((dp + k // Q) % 2, (ep + k % Q) % Q), device_id_type=MESH)
    pl.semaphore_wait(bar, 7)


def gather_kernel(x_ref, r_ref, ids_ref, wr_ref,
                  xon, ron, far, xqn, rqn, gt_out, idx_out, gat_out, cnt_out,
                  gt_s, pos_s, v_s, ssem, rsem, lsem, gsend, grecv):
    dp = lax.axis_index('dp')
    ep = lax.axis_index('ep')
    c = ep % 2
    xc = ep // 2
    me = dp * Q + ep
    mate = (dp, xc * 2 + 1 - c)
    xnb = (dp, (1 - xc) * 2 + c)
    ynb = (1 - dp, ep)
    barrier_all(dp, ep)

    def rcopy(src, dst, k, dev):
        return pltpu.make_async_remote_copy(src_ref=src, dst_ref=dst, send_sem=ssem.at[k], recv_sem=rsem.at[k], device_id=dev, device_id_type=MESH)

    direct = [
        rcopy(x_ref, far.at[c], 0, xnb), rcopy(x_ref, xqn.at[c], 1, ynb),
        rcopy(r_ref, far.at[2 + c], 2, xnb), rcopy(r_ref, rqn.at[c], 3, ynb),
        rcopy(x_ref, xon.at[c], Q, mate), rcopy(r_ref, ron.at[c], 5, mate)]
    for cp in direct[:2] + direct[Q:5]:
        cp.start()
    local = [pltpu.make_async_copy(x_ref, xon.at[c], lsem.at[0]), pltpu.make_async_copy(r_ref, ron.at[c], lsem.at[1])]
    for cp in local:
        cp.start()

    zt = dot(wr_ref[...], x_ref[...], 1, 1)
    eio = lax.broadcasted_iota(jnp.int32, (32, NB), 0)
    sel = eio == ids_ref[0:1, :]
    for j in range(1, S):
        sel = sel | (eio == ids_ref[j:j + 1, :])
    zm = jnp.max(jnp.where(sel, zt, -jnp.inf), axis=0, keepdims=True)
    pe = jnp.where(sel, jnp.exp(zt - zm), 0.0)
    gt_out[...] = jnp.where(sel, pe / jnp.sum(pe, axis=0, keepdims=True), -1.0)
    gt_s[me] = gt_out[pl.ds(pl.multiple_of(ep * S, S), S), :]
    gcopies = []
    for k in range(1, S):
        dev = ((dp + k // Q) % 2, (ep + k % Q) % Q)
        cp = pltpu.make_async_remote_copy(src_ref=gt_out.at[pl.ds(pl.multiple_of(dev[1] * S, S), S)], dst_ref=gt_s.at[me], send_sem=gsend.at[k - 1], recv_sem=grecv.at[k - 1], device_id=dev, device_id_type=MESH)
        cp.start()
        gcopies.append(cp)
    for cp in direct[2:4] + direct[5:]:
        cp.start()
    fwd = [
        rcopy(far.at[c], far.at[c], 6, mate), rcopy(xqn.at[c], xqn.at[c], 7, mate),
        rcopy(far.at[2 + c], far.at[2 + c], S, mate), rcopy(rqn.at[c], rqn.at[c], 9, mate)]
    for k in range(2):
        direct[k].wait_recv()
        fwd[k].start()
    for cp in gcopies:
        cp.wait()

    tri = (lax.broadcasted_iota(jnp.int32, (NB, NB), 0) < lax.broadcasted_iota(jnp.int32, (NB, NB), 1)).astype(BF16)
    srow = lax.broadcasted_iota(jnp.int32, (S, NB), 0)
    tlan = lax.broadcasted_iota(jnp.int32, (S, NB), 1).astype(F32)
    for half in range(2):
        base = jnp.zeros((S, 1), F32)
        for k in range(Q):
            hd = dp if half == 0 else 1 - dp
            xx = xc if k < 2 else 1 - xc
            g = gt_s[hd * Q + xx * 2 + k % 2]
            m = g >= 0.0
            mf = m.astype(F32)
            pos = dot(mf.astype(BF16), tri) + base
            pos_s[half * Q + k] = jnp.where(m, pos, -1.0)
            base = base + jnp.sum(mf, axis=1, keepdims=True)
            g = jnp.where(m, g, 0.0)
            g1 = g.astype(BF16)
            e1 = g - g1.astype(F32)
            g2 = e1.astype(BF16)
            g3 = (e1 - g2.astype(F32)).astype(BF16)
            head = jnp.where(srow == 0, tlan, jnp.where(srow == 1, float(k), 0.0))
            v_s[half * Q + k] = jnp.concatenate([head, g1.astype(F32), g2.astype(F32), g3.astype(F32)], axis=0).astype(BF16)
        cnt_out[half] = jnp.broadcast_to(base, (S, L)).astype(jnp.int32)

    pio = lax.broadcasted_iota(jnp.int32, (NB, NB), 0).astype(F32)
    rio = lax.broadcasted_iota(jnp.int32, (32, NB), 0)
    lio = lax.broadcasted_iota(jnp.int32, (1, NB), 1)

    def list_body(he, carry):
        half = he // S
        e = he % S
        cnt_e = cnt_out[half, pl.ds(e, 1), 0:1]
        for pt in range(Q):
            acc = jnp.zeros((32, NB), F32)
            for k in range(pt, Q):
                prow = pos_s[half * Q + k, pl.ds(e, 1), :] - float(256 * pt)
                oh = (pio == prow).astype(F32).astype(BF16)
                acc = acc + dot(v_s[half * Q + k], oh, 1, 1)
            ids = (acc[0:1, :] + 256.0 * acc[1:2, :]).astype(jnp.int32)
            ids = jnp.where(lio + NB * pt < cnt_e, ids, HALF) + half * HALF
            gv = jnp.sum(jnp.where((rio >= S) & (rio % S == e), acc, 0.0), axis=0, keepdims=True)
            for q in range(2):
                idx_out[he, 2 * pt + q:2 * pt + q + 1, :] = ids[:, L * q:L * (q + 1)]
                gat_out[he, 2 * pt + q:2 * pt + q + 1, :] = gv[:, L * q:L * (q + 1)]
        return carry

    lax.fori_loop(0, 2 * S, list_body, 0)
    cnt_out[2] = jnp.full((S, L), dp, jnp.int32)
    cnt_out[3] = jnp.full((S, L), ep, jnp.int32)
    idx_out[2 * S] = jnp.zeros((S, L), jnp.int32)
    gat_out[2 * S] = jnp.zeros((S, L), F32)

    for k in range(2, Q):
        direct[k].wait_recv()
        fwd[k].start()
    for cp in local:
        cp.wait()
    direct[Q].wait_recv()
    direct[5].wait_recv()
    for cp in direct:
        cp.wait_send()
    for cp in fwd:
        cp.wait()


def load_tokens(pairs, x2, r2, tmp, sem, before, hook):
    srcs = []
    for i, (xa, ra, off) in enumerate(pairs):
        for c in range(2):
            srcs.append((xa.at[c], x2, (2 * i + c) * NB))
            srcs.append((ra.at[off + c], r2, (2 * i + c) * NB))
    copies = [pltpu.make_async_copy(src, tmp.at[i % SLOTS], sem.at[i % SLOTS]) for i, (src, _, _) in enumerate(srcs)]
    for i in range(SLOTS):
        copies[i].start()
    before()
    for i, (_, dst2, row) in enumerate(srcs):
        copies[i].wait()

        def body(b, carry, i=i, dst2=dst2, row=row):
            r0 = pl.multiple_of(b * 64, 64)
            for s in range(S):
                dst2[pl.ds((row + r0) * PT + s, 64, stride=PT), :] = tmp[i % SLOTS, pl.ds(r0, 64), L * s:L * (s + 1)].astype(F32)
            return carry

        lax.fori_loop(0, NB // 64, body, 0)
        if hook is not None and i % 2 == 0:
            hook(i // 2, tmp.at[i % SLOTS])
        if i + SLOTS < len(srcs):
            copies[i + SLOTS].start()
    for ref in (x2, r2):
        ref[row9(2 * len(pairs) * NB), :] = jnp.zeros((S, L), F32)


def strided(ref2, s):
    return ref2[pl.ds(s, T, stride=PT), :]


def zero_rows(ref2, n):
    step = n // 12

    def body(i, carry):
        ref2[pl.ds(pl.multiple_of(i * step, S), step), :] = jnp.zeros((step, L), F32)
        return carry
    lax.fori_loop(0, 12, body, 0)


def row9(t):
    return pl.ds(t * PT, S)


def row8(t):
    return pl.ds(pl.multiple_of(t * S, S), S)


def own_kernel(cnt, idx, gatv, xn, rn, far, w1, w3, w2,
               mine, mate, far_out, dgt_out,
               y_out, dx_out, x2, r2, ust, rsta, rstb, us, ds, o2a, o2b, d2a, d2b, dgsa, dgsb, dgd, gcs, tmp, prev, sem, osem):
    e = pl.program_id(0)
    lane1 = lax.broadcasted_iota(jnp.int32, (1, L), 1)

    def gate_column(base):
        for q in range(2):
            gcs[L * q:L * (q + 1), :] = jnp.transpose(jnp.broadcast_to(gatv[pl.ds(base // L + q, 1), :], (L, L)))

    rsts, o2s, d2s, dgss = (rsta, rstb), (o2a, o2b), (d2a, d2b), (dgsa, dgsb)

    def gather(base, r0, n, slot):
        for r in range(n):
            t = row9(idx[base + r])
            ust[row9(r0 + r), :] = x2[t, :]
            rsts[slot][row9(r0 + r), :] = r2[t, :]

    def scatter(base, r0, n, slot):
        o2, d2, dgs = o2s[slot], d2s[slot], dgss[slot]
        mine = lane1 == base // HALF
        for c in range(0, n, S):
            ts = [idx[base + c + j] for j in range(S)]
            ys = [y_out[row8(ts[j]), :] + o2[row9(r0 + c + j), :] for j in range(S)]
            dl = [dx_out[row8(ts[j]), :] + d2[row9(r0 + c + j), :] for j in range(S)]
            gd = [dgs[pl.ds(r0 + c + j, 1), :] for j in range(S)]
            for j in range(S):
                y_out[row8(ts[j]), :] = ys[j]
                dx_out[row8(ts[j]), :] = dl[j]
                pltpu.store(dgd.at[pl.ds(ts[j], 1), :], gd[j], mask=mine)

    @pl.when(e == 0)
    def _():
        def clear():
            zero_rows(y_out, R1)
            zero_rows(dx_out, R1)
            zero_rows(o2b, XT)
            zero_rows(d2b, XT)
            dgd[...] = jnp.zeros_like(dgd)
            dgsb[...] = jnp.zeros_like(dgsb)
            prev[0] = 0
            prev[1] = 0
            gate_column(0)

        load_tokens([(xn, rn, 0), (far, far, 2)], x2, r2, tmp, sem, clear, None)

        def first(c, carry):
            gather(c * 32, c * 32, 32, 0)
            return carry
        lax.fori_loop(0, T // 32, first, 0)

    n = cnt[0, e, 0]

    def tile(k, slot):
        base = k * T
        o2, d2, rst = o2s[slot], d2s[slot], rsts[slot]
        gcol = gcs[...]
        for s in range(S):
            cs = slice(L * s, L * (s + 1))
            us[:, cs] = strided(ust, s).astype(BF16)
            ds[:, cs] = (strided(rst, s) * gcol).astype(BF16)
        more = base + T < n
        nxt = jnp.where(more, e * HALF + base + T, jnp.minimum(e + 1, NE - 1) * HALF)
        gather(nxt, 0, T, 1 - slot)
        scatter(prev[0], 0, T, 1 - slot)
        u = us[...]
        h1 = dot(u, w1[0])
        h3 = dot(u, w3[0])
        sg = jax.nn.sigmoid(h1)
        sl = h1 * sg
        a = (sl * h3).astype(BF16)
        da = dot(ds[...], w2[0], 1, 1)
        o = dot(a, w2[0]).astype(BF16).astype(F32)
        dh1 = (da * h3 * sg * (1.0 + h1 * (1.0 - sg))).astype(BF16)
        dh3 = (da * sl).astype(BF16)
        dr = (dot(dh1, w1[0], 1, 1) + dot(dh3, w3[0], 1, 1)).astype(BF16).astype(F32)
        acc = jnp.zeros((T, L), F32)
        for s in range(S):
            cs = slice(L * s, L * (s + 1))
            o2[pl.ds(s, T, stride=PT), :] = o[:, cs] * gcol
            d2[pl.ds(s, T, stride=PT), :] = dr[:, cs]
            acc = acc + o[:, cs] * strided(rst, s)
        dgss[slot][...] = jnp.broadcast_to(jnp.sum(acc, axis=1, keepdims=True), (T, L))
        prev[0] = e * HALF + base
        prev[1] = 1 - slot
        gate_column(nxt)

    def tile_body(k, carry):
        par = prev[1]
        for slot in range(2):
            pl.when(par == slot)(functools.partial(tile, k, slot))
        return carry

    lax.fori_loop(0, jnp.maximum((n + T - 1) // T, 1), tile_body, 0)

    @pl.when(e == NE - 1)
    def _():
        def last(c, carry):
            for slot in range(2):
                pl.when(prev[1] != slot)(functools.partial(scatter, prev[0] + c * 32, c * 32, 32, slot))
            return carry
        lax.fori_loop(0, T // 32, last, 0)
        c = cnt[3, 0, 0] % 2
        outs = []
        for i, src in enumerate((y_out, dx_out)):
            for q, dst in enumerate((mine, mate)):
                row = pl.multiple_of((c if q == 0 else 1 - c) * NB * S, NB * S)
                outs.append(pltpu.make_async_copy(src.at[pl.ds(row, NB * S)], dst.at[i], osem.at[i, q]))
            outs.append(pltpu.make_async_copy(src.at[pl.ds(FF * S, FF * S)], far_out.at[i], osem.at[i, 2]))
        for cp in outs:
            cp.start()
        xc = cnt[3, 0, 0] // 2
        tr = jnp.transpose(dgd[0:HALF, :])
        dgt_out[:, pl.ds(pl.multiple_of(xc * FF, FF), FF)] = tr[0:S, 0:FF]
        dgt_out[:, pl.ds(pl.multiple_of(FF - xc * FF, FF), FF)] = tr[0:S, FF:HALF]
        for cp in outs:
            cp.wait()


def pair_kernel(fpart, dgt, gt, mate_in, far, dz_all, dz_own, mate_out, rbuf, obuf, dgb, dzb, ssem, rsem, lsem, wsem, gsend, grecv, zsend, zrecv):
    dp = lax.axis_index('dp')
    ep = lax.axis_index('ep')
    c = ep % 2
    me = dp * Q + ep
    mate = (dp, (ep // 2) * 2 + 1 - c)
    barrier_all(dp, ep)
    mine = pl.ds(pl.multiple_of(ep * S, S), S)
    gcopies = []
    for k in range(1, Q):
        other = (ep + k) % Q
        cp = pltpu.make_async_remote_copy(
            src_ref=dgt.at[:, pl.ds(pl.multiple_of(other * NB, NB), NB)], dst_ref=dgb.at[mine],
            send_sem=gsend.at[k - 1], recv_sem=grecv.at[k - 1], device_id=(dp, other), device_id_type=MESH)
        cp.start()
        gcopies.append(cp)
    sends, loads, stores = [], [], []
    for i in range(2):
        cp = pltpu.make_async_remote_copy(
            src_ref=fpart.at[i, pl.ds(pl.multiple_of((1 - c) * NB * S, NB * S), NB * S)], dst_ref=rbuf.at[i],
            send_sem=ssem.at[i], recv_sem=rsem.at[i], device_id=mate, device_id_type=MESH)
        cp.start()
        sends.append(cp)
        ld = pltpu.make_async_copy(fpart.at[i, pl.ds(pl.multiple_of(c * NB * S, NB * S), NB * S)], obuf.at[i], lsem.at[i])
        ld.start()
        loads.append(ld)
        stores.append(pltpu.make_async_copy(obuf.at[i], far.at[i], wsem.at[i]))
    dgb[mine, :] = dgt[:, pl.ds(pl.multiple_of(ep * NB, NB), NB)]
    for cp in gcopies:
        cp.wait()
    gm = jnp.maximum(gt[...], 0.0)
    dgv = dgb[...]
    dz = (gm * (dgv - jnp.sum(gm * dgv, axis=0, keepdims=True))).astype(BF16)
    dzb[me] = dz
    dz_own[...] = dz
    zcopies = []
    for k in range(1, S):
        dev = ((dp + k // Q) % 2, (ep + k % Q) % Q)
        cp = pltpu.make_async_remote_copy(src_ref=dzb.at[me], dst_ref=dzb.at[me], send_sem=zsend.at[k - 1], recv_sem=zrecv.at[k - 1], device_id=dev, device_id_type=MESH)
        cp.start()
        zcopies.append(cp)
    for i in range(2):
        loads[i].wait()
        sends[i].wait_recv()

        def body(b, carry, i=i):
            rows = pl.ds(pl.multiple_of(b * L, L), L)
            obuf[i, rows, :] = obuf[i, rows, :] + rbuf[i, rows, :]
            return carry

        lax.fori_loop(0, NB // 16, body, 0)
        stores[i].start()
    for cp in zcopies:
        cp.wait()
    dz_all[...] = dzb[...]
    for cp in sends:
        cp.wait_send()
    for cp in stores:
        cp.wait()


def grad_kernel(cnt, idx, gat, dz_all, xon, ron, far, xqn, rqn, qfar, w1, w3, w2,
                g1, g3, g2, dw_out, x2, r2, ust, dst, us, ds, tmp, sem):
    e = pl.program_id(0)

    def gather(ne, nb, r0, n):
        n0 = cnt[0, ne, 0]
        a0 = ne * HALF
        a1 = NE * HALF + a0 - n0
        for r in range(n):
            q = nb + r
            q = q + jnp.where(q < n0, a0, a1)
            t = row9(idx[q])
            ust[row9(r0 + r), :] = x2[t, :]
            dst[row9(r0 + r), :] = r2[t, :] * gat[q]

    @pl.when(e == 0)
    def _():
        dp = cnt[2, 0, 0]
        ep = cnt[3, 0, 0]

        def clear():
            dw_out[...] = jnp.zeros_like(dw_out)

        def add_chunk(i, xc_ref):
            hd = dp if i < Q else 1 - dp
            xx = ep // 2 if i % Q < 2 else 1 - ep // 2
            dw_out[...] += dot(dz_all[hd * Q + xx * 2 + i % 2], xc_ref[...])

        load_tokens([(xon, ron, 0), (far, far, 2), (xqn, rqn, 0), (qfar, qfar, 2)], x2, r2, tmp, sem, clear, add_chunk)

        def first(c, carry):
            gather(0, c * 32, c * 32, 32)
            return carry
        lax.fori_loop(0, T // 32, first, 0)

    n = cnt[0, e, 0] + cnt[1, e, 0]
    rown = lax.broadcasted_iota(jnp.int32, (T, L), 0)

    def tile(k, first):
        base = k * T
        live = rown + base < n
        for s in range(S):
            cs = slice(L * s, L * (s + 1))
            us[:, cs] = strided(ust, s).astype(BF16)
            ds[:, cs] = jnp.where(live, strided(dst, s), 0.0).astype(BF16)
        more = base + T < n
        gather(jnp.where(more, e, jnp.minimum(e + 1, NE - 1)), jnp.where(more, base + T, 0), 0, T)
        u = us[...]
        do = ds[...]
        h1 = dot(u, w1[0])
        h3 = dot(u, w3[0])
        sg = jax.nn.sigmoid(h1)
        sl = h1 * sg
        a = (sl * h3).astype(BF16)
        da = dot(do, w2[0], 1, 1)
        dh1 = (da * h3 * sg * (1.0 + h1 * (1.0 - sg))).astype(BF16)
        dh3 = (da * sl).astype(BF16)
        if first:
            g2[0] = dot(a, do, 0, 0)
            g1[0] = dot(u, dh1, 0, 0)
            g3[0] = dot(u, dh3, 0, 0)
        else:
            g2[0] += dot(a, do, 0, 0)
            g1[0] += dot(u, dh1, 0, 0)
            g3[0] += dot(u, dh3, 0, 0)

    tile(0, True)

    def tile_body(k, carry):
        tile(k, False)
        return carry

    lax.fori_loop(1, (n + T - 1) // T, tile_body, 0)


def final_kernel(x, r, mine, mate, rec, dz, wr, after, y_out, dx_out):
    dxr = dot(dz[...], wr[...], 0, 0)
    for s in range(S):
        cs = slice(L * s, L * (s + 1))
        rows = pl.ds(s, L, stride=S)
        y_out[:, cs] = x[:, cs].astype(F32) + ((mine[0, rows, :] + mate[0, rows, :]) + rec[0, rows, :])
        dx_out[:, cs] = r[:, cs].astype(F32) + dxr[:, cs] + ((mine[1, rows, :] + mate[1, rows, :]) + rec[1, rows, :])


def solution(mesh):
    axes = ('dp', 'ep')
    sds = jax.ShapeDtypeStruct

    def local_step(tokens, w_router, w_gate, w_up, w_down, top_ids, r_proj):
        near = sds((2, NB, D), BF16)
        dma = pltpu.SemaphoreType.DMA
        xon, ron, far, xqn, rqn, gto, idx, gat, cnt = pl.pallas_call(
            gather_kernel,
            out_shape=[near] * 2 + [sds((Q, NB, D), BF16)] + [near] * 2 + [sds((32, NB), F32), sds((NL, S, L), jnp.int32), sds((NL, S, L), F32), sds((Q, S, L), jnp.int32)],
            in_specs=[vspec()] * Q,
            out_specs=[aspec()] * 5 + [vspec()] * Q,
            scratch_shapes=[pltpu.VMEM((S, S, NB), F32), pltpu.VMEM((S, S, NB), F32), pltpu.VMEM((S, 32, NB), BF16),
                            dma((10,)), dma((10,)), dma((2,)), dma((7,)), dma((7,))],
            compiler_params=pltpu.CompilerParams(collective_id=0, has_side_effects=True),
            name='k0_gather',
        )(tokens, r_proj, top_ids.T, w_router.T)

        idx1 = idx.reshape(-1)
        gat1 = gat.reshape(-1)
        xswap = [(0, 2), (2, 0), (1, 3), (3, 1)]
        qfar = lax.ppermute(far, 'dp', [(0, 1), (1, 0)])

        wspec = [pl.BlockSpec((1, D, FF), lambda e: (e, 0, 0)), pl.BlockSpec((1, D, FF), lambda e: (e, 0, 0)), pl.BlockSpec((1, FF, D), lambda e: (e, 0, 0))]
        quarter = sds((2, NB * S, L), F32)
        mine, mate, fpart, dgt = pl.pallas_call(
            own_kernel,
            grid=(NE,),
            out_shape=[quarter, quarter, sds((2, FF * S, L), F32), sds((S, HALF), F32)],
            in_specs=[sspec()] * 2 + [vspec()] + [aspec()] * 3 + wspec,
            out_specs=[aspec()] * 3 + [pl.BlockSpec((S, HALF), lambda e: (0, 0))],
            scratch_shapes=[pltpu.VMEM((R1, L), F32)] * 2 + [pltpu.VMEM((X1, L), F32)] * 2 + [pltpu.VMEM((XT, L), F32)] * 3 + [pltpu.VMEM((T, D), BF16)] * 2
            + [pltpu.VMEM((XT, L), F32)] * Q + [pltpu.VMEM((T, L), F32)] * 2 + [pltpu.VMEM((RB, L), F32), pltpu.VMEM((T, L), F32),
               pltpu.VMEM((SLOTS, NB, D), BF16), pltpu.SMEM((2,), jnp.int32), dma((SLOTS,)), dma((2, 3))],
            compiler_params=pltpu.CompilerParams(vmem_limit_bytes=VMEM_MAX, dimension_semantics=('arbitrary',)),
            cost_estimate=pl.CostEstimate(flops=20 * 10 ** 9, bytes_accessed=40 * 10 ** 6, transcendentals=0),
            name='k1_own',
        )(cnt, idx1, gat.reshape(NL * S, L), xon, ron, far, w_gate, w_up, w_down)

        farsum, dz_all, dz, mate = pl.pallas_call(
            pair_kernel,
            out_shape=[quarter, sds((S, 32, NB), BF16), sds((32, NB), BF16), quarter],
            in_specs=[aspec(), vspec(), vspec(), aspec()],
            out_specs=[aspec()] + [vspec()] * 2 + [aspec()],
            input_output_aliases={3: 3},
            scratch_shapes=[pltpu.VMEM((2, NB * S, L), F32), pltpu.VMEM((2, NB * S, L), F32), pltpu.VMEM((32, NB), F32), pltpu.VMEM((S, 32, NB), BF16),
                            dma((2,)), dma((2,)), dma((2,)), dma((2,)), dma((3,)), dma((3,)), dma((7,)), dma((7,))],
            compiler_params=pltpu.CompilerParams(collective_id=1, has_side_effects=True),
            name='k2_pair',
        )(fpart, dgt, gto, mate)
        matesum = lax.ppermute(mate, 'ep', [(0, 1), (1, 0), (2, 3), (3, 2)])
        rec = lax.ppermute(farsum, 'ep', xswap)

        gspec = [pl.BlockSpec((1, D, FF), lambda e: (e, 0, 0)), pl.BlockSpec((1, D, FF), lambda e: (e, 0, 0)), pl.BlockSpec((1, FF, D), lambda e: (e, 0, 0))]
        grad_gate, grad_up, grad_down, dwt = pl.pallas_call(
            grad_kernel,
            grid=(NE,),
            out_shape=[sds((NE, D, FF), F32), sds((NE, D, FF), F32), sds((NE, FF, D), F32), sds((32, D), F32)],
            in_specs=[sspec()] * 3 + [vspec()] + [aspec()] * 6 + wspec,
            out_specs=gspec + [pl.BlockSpec((32, D), lambda e: (0, 0))],
            scratch_shapes=[pltpu.VMEM((X2, L), F32)] * 2 + [pltpu.VMEM((XT, L), F32)] * 2 + [pltpu.VMEM((T, D), BF16)] * 2
            + [pltpu.VMEM((SLOTS, NB, D), BF16), dma((SLOTS,))],
            compiler_params=pltpu.CompilerParams(vmem_limit_bytes=VMEM_MAX, dimension_semantics=('arbitrary',)),
            cost_estimate=pl.CostEstimate(flops=30 * 10 ** 9, bytes_accessed=90 * 10 ** 6, transcendentals=0),
            name='k3_grad',
        )(cnt, idx1, gat1, dz_all, xon, ron, far, xqn, rqn, qfar, w_gate, w_up, w_down)

        rspec = pl.BlockSpec((L, D), lambda i: (i, 0))
        qspec = pl.BlockSpec((2, L * S, L), lambda i: (0, i, 0))
        y, dx = pl.pallas_call(
            final_kernel,
            grid=(2,),
            out_shape=[sds((NB, D), F32), sds((NB, D), F32)],
            in_specs=[rspec, rspec, qspec, qspec, qspec, pl.BlockSpec((32, L), lambda i: (0, i)), pl.BlockSpec((32, D), lambda i: (0, 0)), aspec()],
            out_specs=[rspec, rspec],
            compiler_params=pltpu.CompilerParams(vmem_limit_bytes=VMEM_MAX),
            name='k4_final',
        )(tokens, r_proj, mine, matesum, rec, dz, w_router.T, dwt)
        return y, dx, grad_gate, grad_up, grad_down, dwt.T

    tok_spec = P(axes, None)
    exp_spec = P('ep', None, None)
    return jax.shard_map(local_step, mesh=mesh, in_specs=(tok_spec, P(), exp_spec, exp_spec, exp_spec, tok_spec, tok_spec), out_specs=(tok_spec, tok_spec, exp_spec, exp_spec, exp_spec, P()), check_vma=False)
```

```python
import functools

import jax
import jax.numpy as jnp
from jax import lax
from jax.experimental import pallas as pl
from jax.experimental.pallas import tpu as pltpu
from jax.sharding import PartitionSpec as P

F32 = jnp.float32
BF16 = jnp.bfloat16
MESH = pl.DeviceIdType.MESH
VMEM_MAX = 63 * 1024 * 1024
T = 256
NB = 256
HALF = 1024
D = 1024
FF = 512
NE = 8
NL = 17
SLOTS = 8
PT = 9
S = 8
L = 128
Q = 4
RB = 1032
R1 = 8256
R2 = 16448
X1 = 9288
X2 = 18504
XT = 2304


def dot(a, b, ca=1, cb=0):
    return lax.dot_general(a, b, (((ca,), (cb,)), ((), ())), preferred_element_type=F32)


def vspec():
    return pl.BlockSpec(memory_space=pltpu.VMEM)


def aspec():
    return pl.BlockSpec(memory_space=pl.ANY)


def sspec():
    return pl.BlockSpec(memory_space=pltpu.SMEM)


def barrier_all(dp, ep):
    bar = pltpu.get_barrier_semaphore()
    for k in range(1, S):
        pl.semaphore_signal(bar, inc=1, device_id=((dp + k // Q) % 2, (ep + k % Q) % Q), device_id_type=MESH)
    pl.semaphore_wait(bar, 7)


def gather_kernel(x_ref, r_ref, ids_ref, wr_ref,
                  xon, ron, far, xqn, rqn, gt_out, idx_out, gat_out, cnt_out,
                  gt_s, pos_s, v_s, ssem, rsem, lsem, gsend, grecv):
    dp = lax.axis_index('dp')
    ep = lax.axis_index('ep')
    c = ep % 2
    xc = ep // 2
    me = dp * Q + ep
    mate = (dp, xc * 2 + 1 - c)
    xnb = (dp, (1 - xc) * 2 + c)
    ynb = (1 - dp, ep)
    barrier_all(dp, ep)

    def rcopy(src, dst, k, dev):
        return pltpu.make_async_remote_copy(src_ref=src, dst_ref=dst, send_sem=ssem.at[k], recv_sem=rsem.at[k], device_id=dev, device_id_type=MESH)

    direct = [
        rcopy(x_ref, far.at[c], 0, xnb), rcopy(x_ref, xqn.at[c], 1, ynb),
        rcopy(r_ref, far.at[2 + c], 2, xnb), rcopy(r_ref, rqn.at[c], 3, ynb),
        rcopy(x_ref, xon.at[c], Q, mate), rcopy(r_ref, ron.at[c], 5, mate)]
    for cp in direct[:2] + direct[Q:5]:
        cp.start()
    local = [pltpu.make_async_copy(x_ref, xon.at[c], lsem.at[0]), pltpu.make_async_copy(r_ref, ron.at[c], lsem.at[1])]
    for cp in local:
        cp.start()

    zt = dot(wr_ref[...], x_ref[...], 1, 1)
    eio = lax.broadcasted_iota(jnp.int32, (32, NB), 0)
    sel = eio == ids_ref[0:1, :]
    for j in range(1, S):
        sel = sel | (eio == ids_ref[j:j + 1, :])
    zm = jnp.max(jnp.where(sel, zt, -jnp.inf), axis=0, keepdims=True)
    pe = jnp.where(sel, jnp.exp(zt - zm), 0.0)
    gt_out[...] = jnp.where(sel, pe / jnp.sum(pe, axis=0, keepdims=True), -1.0)
    gt_s[me] = gt_out[pl.ds(pl.multiple_of(ep * S, S), S), :]
    gcopies = []
    for k in range(1, S):
        dev = ((dp + k // Q) % 2, (ep + k % Q) % Q)
        cp = pltpu.make_async_remote_copy(src_ref=gt_out.at[pl.ds(pl.multiple_of(dev[1] * S, S), S)], dst_ref=gt_s.at[me], send_sem=gsend.at[k - 1], recv_sem=grecv.at[k - 1], device_id=dev, device_id_type=MESH)
        cp.start()
        gcopies.append(cp)
    for cp in direct[2:4] + direct[5:]:
        cp.start()
    fwd = [
        rcopy(far.at[c], far.at[c], 6, mate), rcopy(xqn.at[c], xqn.at[c], 7, mate),
        rcopy(far.at[2 + c], far.at[2 + c], S, mate), rcopy(rqn.at[c], rqn.at[c], 9, mate)]
    for k in range(2):
        direct[k].wait_recv()
        fwd[k].start()
    for cp in gcopies:
        cp.wait()

    tri = (lax.broadcasted_iota(jnp.int32, (NB, NB), 0) < lax.broadcasted_iota(jnp.int32, (NB, NB), 1)).astype(BF16)
    srow = lax.broadcasted_iota(jnp.int32, (S, NB), 0)
    tlan = lax.broadcasted_iota(jnp.int32, (S, NB), 1).astype(F32)
    for half in range(2):
        base = jnp.zeros((S, 1), F32)
        for k in range(Q):
            hd = dp if half == 0 else 1 - dp
            xx = xc if k < 2 else 1 - xc
            g = gt_s[hd * Q + xx * 2 + k % 2]
            m = g >= 0.0
            mf = m.astype(F32)
            pos = dot(mf.astype(BF16), tri) + base
            pos_s[half * Q + k] = jnp.where(m, pos, -1.0)
            base = base + jnp.sum(mf, axis=1, keepdims=True)
            g = jnp.where(m, g, 0.0)
            g1 = g.astype(BF16)
            e1 = g - g1.astype(F32)
            g2 = e1.astype(BF16)
            g3 = (e1 - g2.astype(F32)).astype(BF16)
            head = jnp.where(srow == 0, tlan, jnp.where(srow == 1, float(k), 0.0))
            v_s[half * Q + k] = jnp.concatenate([head, g1.astype(F32), g2.astype(F32), g3.astype(F32)], axis=0).astype(BF16)
        cnt_out[half] = jnp.broadcast_to(base, (S, L)).astype(jnp.int32)

    pio = lax.broadcasted_iota(jnp.int32, (NB, NB), 0).astype(F32)
    rio = lax.broadcasted_iota(jnp.int32, (32, NB), 0)
    lio = lax.broadcasted_iota(jnp.int32, (1, NB), 1)

    def list_body(he, carry):
        half = he // S
        e = he % S
        cnt_e = cnt_out[half, pl.ds(e, 1), 0:1]
        for pt in range(Q):
            acc = jnp.zeros((32, NB), F32)
            for k in range(pt, Q):
                prow = pos_s[half * Q + k, pl.ds(e, 1), :] - float(256 * pt)
                oh = (pio == prow).astype(F32).astype(BF16)
                acc = acc + dot(v_s[half * Q + k], oh, 1, 1)
            ids = (acc[0:1, :] + 256.0 * acc[1:2, :]).astype(jnp.int32)
            ids = jnp.where(lio + NB * pt < cnt_e, ids, HALF) + half * HALF
            gv = jnp.sum(jnp.where((rio >= S) & (rio % S == e), acc, 0.0), axis=0, keepdims=True)
            for q in range(2):
                idx_out[he, 2 * pt + q:2 * pt + q + 1, :] = ids[:, L * q:L * (q + 1)]
                gat_out[he, 2 * pt + q:2 * pt + q + 1, :] = gv[:, L * q:L * (q + 1)]
        return carry

    lax.fori_loop(0, 2 * S, list_body, 0)
    cnt_out[2] = jnp.full((S, L), dp, jnp.int32)
    cnt_out[3] = jnp.full((S, L), ep, jnp.int32)
    idx_out[2 * S] = jnp.zeros((S, L), jnp.int32)
    gat_out[2 * S] = jnp.zeros((S, L), F32)

    for k in range(2, Q):
        direct[k].wait_recv()
        fwd[k].start()
    for cp in local:
        cp.wait()
    direct[Q].wait_recv()
    direct[5].wait_recv()
    for cp in direct:
        cp.wait_send()
    for cp in fwd:
        cp.wait()


def load_tokens(pairs, x2, r2, tmp, sem, before, hook):
    srcs = []
    for i, (xa, ra, off) in enumerate(pairs):
        for c in range(2):
            srcs.append((xa.at[c], x2, (2 * i + c) * NB))
            srcs.append((ra.at[off + c], r2, (2 * i + c) * NB))
    copies = [pltpu.make_async_copy(src, tmp.at[i % SLOTS], sem.at[i % SLOTS]) for i, (src, _, _) in enumerate(srcs)]
    for i in range(SLOTS):
        copies[i].start()
    before()
    for i, (_, dst2, row) in enumerate(srcs):
        copies[i].wait()

        def body(b, carry, i=i, dst2=dst2, row=row):
            r0 = pl.multiple_of(b * 64, 64)
            for s in range(S):
                dst2[pl.ds((row + r0) * PT + s, 64, stride=PT), :] = tmp[i % SLOTS, pl.ds(r0, 64), L * s:L * (s + 1)].astype(F32)
            return carry

        lax.fori_loop(0, NB // 64, body, 0)
        if hook is not None and i % 2 == 0:
            hook(i // 2, tmp.at[i % SLOTS])
        if i + SLOTS < len(srcs):
            copies[i + SLOTS].start()
    for ref in (x2, r2):
        ref[row9(2 * len(pairs) * NB), :] = jnp.zeros((S, L), F32)


def strided(ref2, s):
    return ref2[pl.ds(s, T, stride=PT), :]


def zero_rows(ref2, n):
    step = n // 12

    def body(i, carry):
        ref2[pl.ds(pl.multiple_of(i * step, S), step), :] = jnp.zeros((step, L), F32)
        return carry
    lax.fori_loop(0, 12, body, 0)


def row9(t):
    return pl.ds(t * PT, S)


def row8(t):
    return pl.ds(pl.multiple_of(t * S, S), S)


def own_kernel(cnt, idx, gatv, xn, rn, far, w1, w3, w2,
               mine, mate, far_out, dgt_out,
               y_out, dx_out, x2, r2, ust, rsta, rstb, us, ds, o2a, o2b, d2a, d2b, dgsa, dgsb, dgd, gcs, tmp, prev, sem, osem):
    e = pl.program_id(0)
    lane1 = lax.broadcasted_iota(jnp.int32, (1, L), 1)

    def gate_column(base):
        for q in range(2):
            gcs[L * q:L * (q + 1), :] = jnp.transpose(jnp.broadcast_to(gatv[pl.ds(base // L + q, 1), :], (L, L)))

    rsts, o2s, d2s, dgss = (rsta, rstb), (o2a, o2b), (d2a, d2b), (dgsa, dgsb)

    def gather(base, r0, n, slot):
        for r in range(n):
            t = row9(idx[base + r])
            ust[row9(r0 + r), :] = x2[t, :]
            rsts[slot][row9(r0 + r), :] = r2[t, :]

    def scatter(base, r0, n, slot):
        o2, d2, dgs = o2s[slot], d2s[slot], dgss[slot]
        mine = lane1 == base // HALF
        for c in range(0, n, S):
            ts = [idx[base + c + j] for j in range(S)]
            ys = [y_out[row8(ts[j]), :] + o2[row9(r0 + c + j), :] for j in range(S)]
            dl = [dx_out[row8(ts[j]), :] + d2[row9(r0 + c + j), :] for j in range(S)]
            gd = [dgs[pl.ds(r0 + c + j, 1), :] for j in range(S)]
            for j in range(S):
                y_out[row8(ts[j]), :] = ys[j]
                dx_out[row8(ts[j]), :] = dl[j]
                pltpu.store(dgd.at[pl.ds(ts[j], 1), :], gd[j], mask=mine)

    @pl.when(e == 0)
    def _():
        def clear():
            zero_rows(y_out, R1)
            zero_rows(dx_out, R1)
            zero_rows(o2b, XT)
            zero_rows(d2b, XT)
            dgd[...] = jnp.zeros_like(dgd)
            dgsb[...] = jnp.zeros_like(dgsb)
            prev[0] = 0
            prev[1] = 0
            gate_column(0)

        load_tokens([(xn, rn, 0), (far, far, 2)], x2, r2, tmp, sem, clear, None)

        def first(c, carry):
            gather(c * 32, c * 32, 32, 0)
            return carry
        lax.fori_loop(0, T // 32, first, 0)

    n = cnt[0, e, 0]

    def tile(k, slot):
        base = k * T
        o2, d2, rst = o2s[slot], d2s[slot], rsts[slot]
        gcol = gcs[...]
        for s in range(S):
            cs = slice(L * s, L * (s + 1))
            us[:, cs] = strided(ust, s).astype(BF16)
            ds[:, cs] = (strided(rst, s) * gcol).astype(BF16)
        more = base + T < n
        nxt = jnp.where(more, e * HALF + base + T, jnp.minimum(e + 1, NE - 1) * HALF)
        gather(nxt, 0, T, 1 - slot)
        scatter(prev[0], 0, T, 1 - slot)
        u = us[...]
        h1 = dot(u, w1[0])
        h3 = dot(u, w3[0])
        sg = jax.nn.sigmoid(h1)
        sl = h1 * sg
        a = (sl * h3).astype(BF16)
        da = dot(ds[...], w2[0], 1, 1)
        o = dot(a, w2[0]).astype(BF16).astype(F32)
        dh1 = (da * h3 * sg * (1.0 + h1 * (1.0 - sg))).astype(BF16)
        dh3 = (da * sl).astype(BF16)
        dr = (dot(dh1, w1[0], 1, 1) + dot(dh3, w3[0], 1, 1)).astype(BF16).astype(F32)
        acc = jnp.zeros((T, L), F32)
        for s in range(S):
            cs = slice(L * s, L * (s + 1))
            o2[pl.ds(s, T, stride=PT), :] = o[:, cs] * gcol
            d2[pl.ds(s, T, stride=PT), :] = dr[:, cs]
            acc = acc + o[:, cs] * strided(rst, s)
        dgss[slot][...] = jnp.broadcast_to(jnp.sum(acc, axis=1, keepdims=True), (T, L))
        prev[0] = e * HALF + base
        prev[1] = 1 - slot
        gate_column(nxt)

    def tile_body(k, carry):
        par = prev[1]
        for slot in range(2):
            pl.when(par == slot)(functools.partial(tile, k, slot))
        return carry

    lax.fori_loop(0, jnp.maximum((n + T - 1) // T, 1), tile_body, 0)

    @pl.when(e == NE - 1)
    def _():
        def last(c, carry):
            for slot in range(2):
                pl.when(prev[1] != slot)(functools.partial(scatter, prev[0] + c * 32, c * 32, 32, slot))
            return carry
        lax.fori_loop(0, T // 32, last, 0)
        c = cnt[3, 0, 0] % 2
        outs = []
        for i, src in enumerate((y_out, dx_out)):
            for q, dst in enumerate((mine, mate)):
                row = pl.multiple_of((c if q == 0 else 1 - c) * NB * S, NB * S)
                outs.append(pltpu.make_async_copy(src.at[pl.ds(row, NB * S)], dst.at[i], osem.at[i, q]))
            outs.append(pltpu.make_async_copy(src.at[pl.ds(FF * S, FF * S)], far_out.at[i], osem.at[i, 2]))
        for cp in outs:
            cp.start()
        xc = cnt[3, 0, 0] // 2
        tr = jnp.transpose(dgd[0:HALF, :])
        dgt_out[:, pl.ds(pl.multiple_of(xc * FF, FF), FF)] = tr[0:S, 0:FF]
        dgt_out[:, pl.ds(pl.multiple_of(FF - xc * FF, FF), FF)] = tr[0:S, FF:HALF]
        for cp in outs:
            cp.wait()


def pair_kernel(fpart, dgt, gt, mate_in, far, dz_all, dz_own, mate_out, rbuf, obuf, dgb, dzb, ssem, rsem, lsem, wsem, gsend, grecv, zsend, zrecv):
    dp = lax.axis_index('dp')
    ep = lax.axis_index('ep')
    c = ep % 2
    me = dp * Q + ep
    mate = (dp, (ep // 2) * 2 + 1 - c)
    barrier_all(dp, ep)
    mine = pl.ds(pl.multiple_of(ep * S, S), S)
    gcopies = []
    for k in range(1, Q):
        other = (ep + k) % Q
        cp = pltpu.make_async_remote_copy(
            src_ref=dgt.at[:, pl.ds(pl.multiple_of(other * NB, NB), NB)], dst_ref=dgb.at[mine],
            send_sem=gsend.at[k - 1], recv_sem=grecv.at[k - 1], device_id=(dp, other), device_id_type=MESH)
        cp.start()
        gcopies.append(cp)
    sends, loads, stores = [], [], []
    for i in range(2):
        cp = pltpu.make_async_remote_copy(
            src_ref=fpart.at[i, pl.ds(pl.multiple_of((1 - c) * NB * S, NB * S), NB * S)], dst_ref=rbuf.at[i],
            send_sem=ssem.at[i], recv_sem=rsem.at[i], device_id=mate, device_id_type=MESH)
        cp.start()
        sends.append(cp)
        ld = pltpu.make_async_copy(fpart.at[i, pl.ds(pl.multiple_of(c * NB * S, NB * S), NB * S)], obuf.at[i], lsem.at[i])
        ld.start()
        loads.append(ld)
        stores.append(pltpu.make_async_copy(obuf.at[i], far.at[i], wsem.at[i]))
    dgb[mine, :] = dgt[:, pl.ds(pl.multiple_of(ep * NB, NB), NB)]
    for cp in gcopies:
        cp.wait()
    gm = jnp.maximum(gt[...], 0.0)
    dgv = dgb[...]
    dz = (gm * (dgv - jnp.sum(gm * dgv, axis=0, keepdims=True))).astype(BF16)
    dzb[me] = dz
    dz_own[...] = dz
    zcopies = []
    for k in range(1, S):
        dev = ((dp + k // Q) % 2, (ep + k % Q) % Q)
        cp = pltpu.make_async_remote_copy(src_ref=dzb.at[me], dst_ref=dzb.at[me], send_sem=zsend.at[k - 1], recv_sem=zrecv.at[k - 1], device_id=dev, device_id_type=MESH)
        cp.start()
        zcopies.append(cp)
    for i in range(2):
        loads[i].wait()
        sends[i].wait_recv()

        def body(b, carry, i=i):
            rows = pl.ds(pl.multiple_of(b * L, L), L)
            obuf[i, rows, :] = obuf[i, rows, :] + rbuf[i, rows, :]
            return carry

        lax.fori_loop(0, NB // 16, body, 0)
        stores[i].start()
    for cp in zcopies:
        cp.wait()
    dz_all[...] = dzb[...]
    for cp in sends:
        cp.wait_send()
    for cp in stores:
        cp.wait()


def grad_kernel(cnt, idx, gat, dz_all, xon, ron, far, xqn, rqn, qfar, w1, w3, w2,
                g1, g3, g2, dw_out, x2, r2, ust, dst, us, ds, uts, tmp, sem):
    e = pl.program_id(0)

    def gather(ne, nb, r0, n):
        n0 = cnt[0, ne, 0]
        a0 = ne * HALF
        a1 = NE * HALF + a0 - n0
        for r in range(n):
            q = nb + r
            q = q + jnp.where(q < n0, a0, a1)
            t = row9(idx[q])
            ust[row9(r0 + r), :] = x2[t, :]
            dst[row9(r0 + r), :] = r2[t, :] * gat[q]

    @pl.when(e == 0)
    def _():
        dp = cnt[2, 0, 0]
        ep = cnt[3, 0, 0]

        def clear():
            dw_out[...] = jnp.zeros_like(dw_out)

        def add_chunk(i, xc_ref):
            hd = dp if i < Q else 1 - dp
            xx = ep // 2 if i % Q < 2 else 1 - ep // 2
            dw_out[...] += dot(dz_all[hd * Q + xx * 2 + i % 2], xc_ref[...])

        load_tokens([(xon, ron, 0), (far, far, 2), (xqn, rqn, 0), (qfar, qfar, 2)], x2, r2, tmp, sem, clear, add_chunk)

        def first(c, carry):
            gather(0, c * 32, c * 32, 32)
            return carry
        lax.fori_loop(0, T // 32, first, 0)

    n = cnt[0, e, 0] + cnt[1, e, 0]
    rown = lax.broadcasted_iota(jnp.int32, (T, L), 0)

    def tile(k, first):
        base = k * T
        live = rown + base < n
        for s in range(S):
            cs = slice(L * s, L * (s + 1))
            us[:, cs] = strided(ust, s).astype(BF16)
            ds[:, cs] = jnp.where(live, strided(dst, s), 0.0).astype(BF16)
        more = base + T < n
        gather(jnp.where(more, e, jnp.minimum(e + 1, NE - 1)), jnp.where(more, base + T, 0), 0, T)
        u = us[...]
        do = ds[...]
        uts[...] = jnp.transpose(u)
        h1 = dot(u, w1[0])
        h3 = dot(u, w3[0])
        sg = jax.nn.sigmoid(h1)
        sl = h1 * sg
        a = (sl * h3).astype(BF16)
        da = dot(do, w2[0], 1, 1)
        dh1 = (da * h3 * sg * (1.0 + h1 * (1.0 - sg))).astype(BF16)
        dh3 = (da * sl).astype(BF16)
        if first:
            g2[0] = dot(a, do, 0, 0)
            g1[0] = dot(uts[...], dh1)
            g3[0] = dot(uts[...], dh3)
        else:
            g2[0] += dot(a, do, 0, 0)
            g1[0] += dot(uts[...], dh1)
            g3[0] += dot(uts[...], dh3)

    tile(0, True)

    def tile_body(k, carry):
        tile(k, False)
        return carry

    lax.fori_loop(1, (n + T - 1) // T, tile_body, 0)


def final_kernel(x, r, mine, mate, rec, dz, wr, after, y_out, dx_out):
    dxr = dot(dz[...], wr[...], 0, 0)
    for s in range(S):
        cs = slice(L * s, L * (s + 1))
        rows = pl.ds(s, L, stride=S)
        y_out[:, cs] = x[:, cs].astype(F32) + ((mine[0, rows, :] + mate[0, rows, :]) + rec[0, rows, :])
        dx_out[:, cs] = r[:, cs].astype(F32) + dxr[:, cs] + ((mine[1, rows, :] + mate[1, rows, :]) + rec[1, rows, :])


def solution(mesh):
    axes = ('dp', 'ep')
    sds = jax.ShapeDtypeStruct

    def local_step(tokens, w_router, w_gate, w_up, w_down, top_ids, r_proj):
        near = sds((2, NB, D), BF16)
        dma = pltpu.SemaphoreType.DMA
        xon, ron, far, xqn, rqn, gto, idx, gat, cnt = pl.pallas_call(
            gather_kernel,
            out_shape=[near] * 2 + [sds((Q, NB, D), BF16)] + [near] * 2 + [sds((32, NB), F32), sds((NL, S, L), jnp.int32), sds((NL, S, L), F32), sds((Q, S, L), jnp.int32)],
            in_specs=[vspec()] * Q,
            out_specs=[aspec()] * 5 + [vspec()] * Q,
            scratch_shapes=[pltpu.VMEM((S, S, NB), F32), pltpu.VMEM((S, S, NB), F32), pltpu.VMEM((S, 32, NB), BF16),
                            dma((10,)), dma((10,)), dma((2,)), dma((7,)), dma((7,))],
            compiler_params=pltpu.CompilerParams(collective_id=0, has_side_effects=True),
            name='k0_gather',
        )(tokens, r_proj, top_ids.T, w_router.T)

        idx1 = idx.reshape(-1)
        gat1 = gat.reshape(-1)
        xswap = [(0, 2), (2, 0), (1, 3), (3, 1)]
        qfar = lax.ppermute(far, 'dp', [(0, 1), (1, 0)])

        wspec = [pl.BlockSpec((1, D, FF), lambda e: (e, 0, 0)), pl.BlockSpec((1, D, FF), lambda e: (e, 0, 0)), pl.BlockSpec((1, FF, D), lambda e: (e, 0, 0))]
        quarter = sds((2, NB * S, L), F32)
        mine, mate, fpart, dgt = pl.pallas_call(
            own_kernel,
            grid=(NE,),
            out_shape=[quarter, quarter, sds((2, FF * S, L), F32), sds((S, HALF), F32)],
            in_specs=[sspec()] * 2 + [vspec()] + [aspec()] * 3 + wspec,
            out_specs=[aspec()] * 3 + [pl.BlockSpec((S, HALF), lambda e: (0, 0))],
            scratch_shapes=[pltpu.VMEM((R1, L), F32)] * 2 + [pltpu.VMEM((X1, L), F32)] * 2 + [pltpu.VMEM((XT, L), F32)] * 3 + [pltpu.VMEM((T, D), BF16)] * 2
            + [pltpu.VMEM((XT, L), F32)] * Q + [pltpu.VMEM((T, L), F32)] * 2 + [pltpu.VMEM((RB, L), F32), pltpu.VMEM((T, L), F32),
               pltpu.VMEM((SLOTS, NB, D), BF16), pltpu.SMEM((2,), jnp.int32), dma((SLOTS,)), dma((2, 3))],
            compiler_params=pltpu.CompilerParams(vmem_limit_bytes=VMEM_MAX, dimension_semantics=('arbitrary',)),
            cost_estimate=pl.CostEstimate(flops=20 * 10 ** 9, bytes_accessed=40 * 10 ** 6, transcendentals=0),
            name='k1_own',
        )(cnt, idx1, gat.reshape(NL * S, L), xon, ron, far, w_gate, w_up, w_down)

        farsum, dz_all, dz, mate = pl.pallas_call(
            pair_kernel,
            out_shape=[quarter, sds((S, 32, NB), BF16), sds((32, NB), BF16), quarter],
            in_specs=[aspec(), vspec(), vspec(), aspec()],
            out_specs=[aspec()] + [vspec()] * 2 + [aspec()],
            input_output_aliases={3: 3},
            scratch_shapes=[pltpu.VMEM((2, NB * S, L), F32), pltpu.VMEM((2, NB * S, L), F32), pltpu.VMEM((32, NB), F32), pltpu.VMEM((S, 32, NB), BF16),
                            dma((2,)), dma((2,)), dma((2,)), dma((2,)), dma((3,)), dma((3,)), dma((7,)), dma((7,))],
            compiler_params=pltpu.CompilerParams(collective_id=1, has_side_effects=True),
            name='k2_pair',
        )(fpart, dgt, gto, mate)
        matesum = lax.ppermute(mate, 'ep', [(0, 1), (1, 0), (2, 3), (3, 2)])
        rec = lax.ppermute(farsum, 'ep', xswap)

        gspec = [pl.BlockSpec((1, D, FF), lambda e: (e, 0, 0)), pl.BlockSpec((1, D, FF), lambda e: (e, 0, 0)), pl.BlockSpec((1, FF, D), lambda e: (e, 0, 0))]
        grad_gate, grad_up, grad_down, dwt = pl.pallas_call(
            grad_kernel,
            grid=(NE,),
            out_shape=[sds((NE, D, FF), F32), sds((NE, D, FF), F32), sds((NE, FF, D), F32), sds((32, D), F32)],
            in_specs=[sspec()] * 3 + [vspec()] + [aspec()] * 6 + wspec,
            out_specs=gspec + [pl.BlockSpec((32, D), lambda e: (0, 0))],
            scratch_shapes=[pltpu.VMEM((X2, L), F32)] * 2 + [pltpu.VMEM((XT, L), F32)] * 2 + [pltpu.VMEM((T, D), BF16)] * 2
            + [pltpu.VMEM((D, T), BF16), pltpu.VMEM((SLOTS, NB, D), BF16), dma((SLOTS,))],
            compiler_params=pltpu.CompilerParams(vmem_limit_bytes=VMEM_MAX, dimension_semantics=('arbitrary',)),
            cost_estimate=pl.CostEstimate(flops=30 * 10 ** 9, bytes_accessed=90 * 10 ** 6, transcendentals=0),
            name='k3_grad',
        )(cnt, idx1, gat1, dz_all, xon, ron, far, xqn, rqn, qfar, w_gate, w_up, w_down)

        rspec = pl.BlockSpec((L, D), lambda i: (i, 0))
        qspec = pl.BlockSpec((2, L * S, L), lambda i: (0, i, 0))
        y, dx = pl.pallas_call(
            final_kernel,
            grid=(2,),
            out_shape=[sds((NB, D), F32), sds((NB, D), F32)],
            in_specs=[rspec, rspec, qspec, qspec, qspec, pl.BlockSpec((32, L), lambda i: (0, i)), pl.BlockSpec((32, D), lambda i: (0, 0)), aspec()],
            out_specs=[rspec, rspec],
            compiler_params=pltpu.CompilerParams(vmem_limit_bytes=VMEM_MAX),
            name='k4_final',
        )(tokens, r_proj, mine, matesum, rec, dz, w_router.T, dwt)
        return y, dx, grad_gate, grad_up, grad_down, dwt.T

    tok_spec = P(axes, None)
    exp_spec = P('ep', None, None)
    return jax.shard_map(local_step, mesh=mesh, in_specs=(tok_spec, P(), exp_spec, exp_spec, exp_spec, tok_spec, tok_spec), out_specs=(tok_spec, tok_spec, exp_spec, exp_spec, exp_spec, P()), check_vma=False)
```
